64 devices in a mesh: dp: 4 (over x, y), ep: 16 (over z, core).
Axes of the slice: x: 2, y: 2, z: 8, core: 2. Of those that a mesh axis runs over, the one named last changes fastest.
The devices are a block of a 4x4x8 slice.
Arguments:
- tokens: bfloat16 [8192, 2048], P(('dp', 'ep')), parts along dimension 0
- topk_idx: int32 [8192, 8], P(('dp', 'ep')), parts along dimension 0
- topk_w: float32 [8192, 8], P(('dp', 'ep')), parts along dimension 0
- w_up: bfloat16 [16, 9, 2048, 768], P('ep')
- w_down: bfloat16 [16, 9, 768, 2048], P('ep')
- slot_expert: int32 [16, 9], replicated
Outputs:
- output: bfloat16 [8192, 2048], P(('dp', 'ep')), parts along dimension 0
There are 4 independent parts. The reference program is written for one: setup_inputs(seed, part) draws one part's arguments, and reference() takes and returns one part's arrays. A program takes and returns all parts, laid end to end along the dimension named above; an argument that names none is the same for every part.
All inputs are finite; a program needn't handle non-finite values.
Results may differ from the reference program's by a relative error of at most 0.0013.
Values are sent between devices in bfloat16 or wider.
A program may use at most 768 MiB of HBM per device.

```python
import jax
import jax.numpy as jnp
from jax import lax
import numpy as np

GROUP = 16
TOK_DEV = 128
D_MODEL = 2048
D_FF = 768
EXPERTS = 128
TOP = 8

PER_DEV = EXPERTS // GROUP
SLOTS = PER_DEV + 1
N_UNITS = GROUP * SLOTS
PAIRS_DEV = TOK_DEV * TOP
BASE_LOAD = PAIRS_DEV // N_UNITS
BLOCK = max(8, (GROUP * PAIRS_DEV) // N_UNITS)
N_BLOCKS = (GROUP * PAIRS_DEV) // BLOCK + EXPERTS


def base_table():
    dev_ids = np.arange(GROUP)
    hot_dev = (3 * (dev_ids // 3) + 3) % GROUP
    spare_exp = hot_dev * PER_DEV + PER_DEV - 1
    primary = np.arange(EXPERTS).reshape(GROUP, PER_DEV)
    return np.concatenate([primary, spare_exp[:, None]], axis=1).astype(np.int32)


def draw_table(key_tab):
    key_dev, key_col, key_lab = jax.random.split(key_tab, 3)
    relabel = jax.random.permutation(key_lab, EXPERTS).astype(jnp.int32)
    dev_perm = jax.random.permutation(key_dev, GROUP)
    col_perm = jax.random.permutation(key_col, SLOTS)
    slot_table = jnp.asarray(base_table())[dev_perm][:, col_perm]
    return relabel[slot_table], relabel


def draw_loads(key_load):
    key_perm, key_shift = jax.random.split(key_load)
    unit_order = 1 + jax.random.permutation(key_perm, N_UNITS - 1)
    shift_amt = jax.random.randint(key_shift, ((N_UNITS - 2) // 2,), 0, BASE_LOAD // 2 + 1, dtype=jnp.int32)
    spread = BASE_LOAD // 2 + 1
    unit_loads = jnp.full((N_UNITS,), BASE_LOAD, jnp.int32)
    unit_loads = unit_loads.at[0].add(spread).at[unit_order[0]].add(-spread)
    unit_loads = unit_loads.at[unit_order[1::2]].add(shift_amt).at[unit_order[2::2]].add(-shift_amt)
    return unit_loads.at[unit_order[:PAIRS_DEV - N_UNITS * BASE_LOAD]].add(1)


def draw_routing(key_src, unit_expert):
    key_load, key_tok = jax.random.split(key_src)
    counts = jax.ops.segment_sum(draw_loads(key_load), unit_expert, num_segments=EXPERTS)
    bounds = jnp.cumsum(counts)
    sorted_exp = jnp.searchsorted(bounds, jnp.arange(PAIRS_DEV, dtype=jnp.int32), side='right').astype(jnp.int32)
    routes = sorted_exp.reshape(TOP, TOK_DEV).T
    return routes[jax.random.permutation(key_tok, TOK_DEV)]


def setup_inputs(seed: int = 0, part: int = 0) -> dict:
    root_key = jax.random.key(seed)
    key_tab, key_up, key_down, key_part = jax.random.split(root_key, 4)
    slot_expert, relabel = draw_table(key_tab)
    unit_expert = relabel[jnp.asarray(base_table()).reshape(-1)]
    up_base = jax.random.normal(key_up, (EXPERTS, D_MODEL, D_FF), jnp.float32) * D_MODEL ** -0.5
    down_base = jax.random.normal(key_down, (EXPERTS, D_FF, D_MODEL), jnp.float32) * D_FF ** -0.5
    key_grp = jax.random.fold_in(key_part, part)
    key_tokens, key_gate, key_route = jax.random.split(key_grp, 3)
    tokens = jax.random.normal(key_tokens, (GROUP * TOK_DEV, D_MODEL), jnp.float32)
    topk_w = jax.random.uniform(key_gate, (GROUP * TOK_DEV, TOP), jnp.float32, 0.3, 1.0)
    src_keys = jax.random.split(key_route, GROUP)
    topk_idx = jax.vmap(draw_routing, in_axes=(0, None))(src_keys, unit_expert)
    return {'tokens': tokens.astype(jnp.bfloat16), 'topk_idx': topk_idx.reshape(GROUP * TOK_DEV, TOP), 'topk_w': topk_w, 'w_up': up_base.astype(jnp.bfloat16)[slot_expert], 'w_down': down_base.astype(jnp.bfloat16)[slot_expert], 'slot_expert': slot_expert}


def reference(tokens, topk_idx, topk_w, w_up, w_down, slot_expert):
    n_tok = tokens.shape[0]
    n_pairs = n_tok * TOP
    table_flat = slot_expert.reshape(-1)
    first_slot = jax.ops.segment_min(jnp.arange(N_UNITS, dtype=jnp.int32), table_flat, num_segments=EXPERTS)
    up_flat = w_up.reshape(N_UNITS, D_MODEL, D_FF)
    down_flat = w_down.reshape(N_UNITS, D_FF, D_MODEL)
    flat_exp = topk_idx.reshape(-1)
    flat_gate = topk_w.reshape(-1)
    pair_order = jnp.argsort(flat_exp, stable=True)
    counts = jnp.bincount(flat_exp, length=EXPERTS)
    starts = jnp.cumsum(counts) - counts
    exp_blocks = (counts + BLOCK - 1) // BLOCK
    block_end = jnp.cumsum(exp_blocks)
    block_start = block_end - exp_blocks
    lane_ids = jnp.arange(BLOCK)

    def block_step(acc_sum, block_id):
        exp_id = jnp.minimum(jnp.searchsorted(block_end, block_id, side='right'), EXPERTS - 1)
        offsets = (block_id - block_start[exp_id]) * BLOCK + lane_ids
        is_valid = (offsets < counts[exp_id]) & (block_id < block_end[EXPERTS - 1])
        pair_ids = pair_order[jnp.clip(starts[exp_id] + offsets, 0, n_pairs - 1)]
        tok_ids = pair_ids // TOP
        slot_id = first_slot[exp_id]
        pre_act = jnp.dot(tokens[tok_ids], up_flat[slot_id], preferred_element_type=jnp.float32)
        hidden = jax.nn.gelu(pre_act, approximate=True).astype(jnp.bfloat16)
        expert_out = jnp.dot(hidden, down_flat[slot_id], preferred_element_type=jnp.float32).astype(jnp.bfloat16)
        gate_vals = jnp.where(is_valid, flat_gate[pair_ids], 0.0)
        return acc_sum.at[tok_ids].add(gate_vals[:, None] * expert_out.astype(jnp.float32)), None

    acc_out, _ = lax.scan(block_step, jnp.zeros((n_tok, D_MODEL), jnp.float32), jnp.arange(N_BLOCKS))
    return acc_out.astype(jnp.bfloat16)
```

```python
import functools

import jax
import jax.numpy as jnp
from jax import lax
from jax.experimental import pallas as pl
from jax.experimental.pallas import tpu as pltpu
from jax.sharding import PartitionSpec as P

MESH = pl.DeviceIdType.MESH
F32 = jnp.float32
BF16 = jnp.bfloat16
CORES = 2
W_DEPTH = 3
AG_CHUNKS = 2
RS_CHUNKS = 4


def slot_bound(n_tok, n_top, n_dev, n_slot):
    base_load = (n_tok * n_top) // (n_dev * n_slot)
    return base_load + base_load // 2 + 1


def split3(x):
    hi = x.astype(BF16)
    rest = x - hi.astype(F32)
    mid = rest.astype(BF16)
    low = (rest - mid.astype(F32)).astype(BF16)
    return hi, mid, low


def layer_kernel(nz, tok_hbm, meta_hbm, slot_smem, slot_vmem, up_hbm, down_hbm, out_ref,
                 toks, metas, x_buf, o_sib, up_buf, down_buf, rs_buf, mix, pick, target,
                 in_sem, ag_send, ag_recv, sib_send, sib_recv, ms_send, ms_recv, mb_send, mb_recv,
                 w_sem, o_send, o_recv, rs_send, rs_recv):
    half = nz // 2
    n_tok, d_model = tok_hbm.shape
    n_top = meta_hbm.shape[0] // 2
    n_slot, cap = x_buf.shape[0], x_buf.shape[3]
    rows = n_slot * cap
    k_pad, n_exp = pick.shape
    ag_rows = n_tok // AG_CHUNKS
    rs_cols = d_model // RS_CHUNKS

    me = lax.axis_index("ep")
    z = me // CORES
    core = me % CORES
    other = 1 - core

    def ring(pos):
        return (pos + nz) % nz

    def device(pos, which):
        return {"ep": pos * CORES + which}

    def remote(src, dst, send, recv, dev):
        return pltpu.make_async_remote_copy(src_ref=src, dst_ref=dst, send_sem=send, recv_sem=recv,
                                            device_id=dev, device_id_type=MESH)

    def weight_copies(slot):
        buf = slot % W_DEPTH
        return (pltpu.make_async_copy(up_hbm.at[0, slot], up_buf.at[buf], w_sem.at[0, buf]),
                pltpu.make_async_copy(down_hbm.at[0, slot], down_buf.at[buf], w_sem.at[1, buf]))

    own_tok = pltpu.make_async_copy(tok_hbm, toks.at[core, z], in_sem.at[0])
    own_meta = pltpu.make_async_copy(meta_hbm, metas.at[core, z], in_sem.at[1])
    own_meta.start()
    own_tok.start()
    barrier = pltpu.get_barrier_semaphore()
    pl.semaphore_signal(barrier, inc=1, device_id=device(ring(z + 1), core), device_id_type=MESH)
    pl.semaphore_signal(barrier, inc=1, device_id=device(ring(z - 1), core), device_id_type=MESH)
    pl.semaphore_signal(barrier, inc=1, device_id=device(z, other), device_id_type=MESH)
    pl.semaphore_wait(barrier, 3)
    own_meta.wait()
    own_tok.wait()

    def ag_copy(d, hop, c):
        sign = 1 - 2 * d
        ref = toks.at[core, ring(z - sign * (hop - 1)), pl.ds(c * ag_rows, ag_rows)]
        return remote(ref, ref, ag_send.at[d, hop - 1, c], ag_recv.at[d, hop - 1, c], device(ring(z + sign), core))

    def ag_arrival(d, hop, c):
        sign = 1 - 2 * d
        ref = toks.at[core, ring(z - sign * hop), pl.ds(c * ag_rows, ag_rows)]
        return remote(ref, ref, ag_send.at[d, hop - 1, c], ag_recv.at[d, hop - 1, c], device(ring(z + sign), core))

    def sib_copy(d, hop, c, which):
        sign = 1 - 2 * d
        ref = toks.at[which, ring(z - sign * hop), pl.ds(c * ag_rows, ag_rows)]
        return remote(ref, ref, sib_send.at[d, hop, c], sib_recv.at[d, hop, c], device(z, other))

    def meta_copy(d, hop, back):
        sign = 1 - 2 * d
        ref = metas.at[core, ring(z - sign * (hop - 1 + back))]
        return remote(ref, ref, ms_send.at[d, hop - 1], ms_recv.at[d, hop - 1], device(ring(z + sign), core))

    def meta_sib(d, hop, which):
        sign = 1 - 2 * d
        ref = metas.at[which, ring(z - sign * hop)]
        return remote(ref, ref, mb_send.at[d, hop], mb_recv.at[d, hop], device(z, other))

    def chunk_order(d):
        return list(range(AG_CHUNKS)) if d == 0 else list(range(AG_CHUNKS))[::-1]

    def carried(d, hop):
        order = chunk_order(d)
        return order if hop < half else order[:AG_CHUNKS // 2]

    def meta_carried(d, hop):
        return hop < half or d == 0

    for d in range(2):
        meta_copy(d, 1, 0).start()
    for c in range(AG_CHUNKS):
        for d in range(2):
            ag_copy(d, 1, chunk_order(d)[c]).start()
    meta_sib(0, 0, core).start()
    for c in range(AG_CHUNKS):
        sib_copy(0, 0, c, core).start()
    for slot in range(W_DEPTH):
        for copy in weight_copies(slot):
            copy.start()

    lane = lax.broadcasted_iota(jnp.int32, (cap, n_exp), 1)
    row = lax.broadcasted_iota(jnp.int32, (cap, n_exp), 0).astype(F32)
    table = slot_vmem[...]
    place = lax.broadcasted_iota(jnp.int32, table.shape, 0) * n_slot + lax.broadcasted_iota(jnp.int32, table.shape, 1)
    for w in range(2):
        dev = me if w == 0 else z * CORES + other
        for s in range(n_slot):
            exp_id = slot_smem[dev, s]
            same = table == exp_id
            copies = jnp.sum(jnp.where(same, 1.0, 0.0))
            earlier = jnp.sum(jnp.where(same & (place < dev * n_slot + s), 1.0, 0.0))
            at = pl.ds(w * rows + s * cap, cap)
            pick[at, :] = jnp.where(lane == exp_id, 1.0, 0.0).astype(BF16)
            target[at, :] = row * copies + earlier
    if k_pad > 2 * rows:
        pick[2 * rows:, :] = jnp.zeros((k_pad - 2 * rows, n_exp), BF16)
        target[2 * rows:, :] = jnp.full((k_pad - 2 * rows, n_exp), -5.0, F32)

    def place_rows(which, pos, mine):
        info = metas[which, pos]
        exp_iota = lax.broadcasted_iota(jnp.int32, (n_exp, n_tok), 0).astype(F32)
        chosen = jnp.zeros((n_exp, n_tok), F32)
        gate = jnp.zeros((n_exp, n_tok), F32)
        for j in range(n_top):
            hit = exp_iota == info[j:j + 1, :]
            chosen = jnp.where(hit, 1.0, chosen)
            if mine:
                gate = jnp.where(hit, info[n_top + j:n_top + j + 1, :], gate)
        before = (lax.broadcasted_iota(jnp.int32, (n_tok, n_tok), 0)
                  < lax.broadcasted_iota(jnp.int32, (n_tok, n_tok), 1))
        rank = jnp.dot(chosen.astype(BF16), jnp.where(before, 1.0, 0.0).astype(BF16), preferred_element_type=F32)
        rank = jnp.where(chosen > 0.5, rank, -1.0).astype(BF16)
        n_rows = k_pad if mine else rows
        takes = jnp.dot(pick[:n_rows, :], rank, preferred_element_type=F32) == target[:n_rows, :]
        onehot = jnp.where(takes[:rows], 1.0, 0.0).astype(BF16)
        for c in range(RS_CHUNKS):
            cols = pl.ds(c * rs_cols, rs_cols)
            got = jnp.dot(onehot, toks[which, pos, :, cols], preferred_element_type=F32).astype(BF16)
            x_buf[:, which, pos, :, cols] = got.reshape(n_slot, cap, rs_cols)
        if mine:
            parts = [jnp.dot(pick[...], part, preferred_element_type=F32) for part in split3(gate)]
            picked = jnp.where(takes, parts[0] + parts[1] + parts[2], 0.0)
            for n, part in enumerate(split3(picked.T)):
                mix[pos, n * n_tok:(n + 1) * n_tok, :] = part

    place_rows(core, z, True)
    meta_sib(0, 0, other).wait_recv()
    for c in range(AG_CHUNKS):
        sib_copy(0, 0, c, other).wait_recv()
    place_rows(other, z, False)

    for hop in range(1, half + 1):
        for d in range(2):
            if meta_carried(d, hop):
                meta_copy(d, hop, 1).wait_recv()
                if hop < half and meta_carried(d, hop + 1):
                    meta_copy(d, hop + 1, 0).start()
                meta_sib(d, hop, core).start()
        for n in range(AG_CHUNKS):
            for d in range(2):
                if n < len(carried(d, hop)):
                    c = carried(d, hop)[n]
                    ag_arrival(d, hop, c).wait_recv()
                    if hop < half and c in carried(d, hop + 1):
                        ag_copy(d, hop + 1, c).start()
                    sib_copy(d, hop, c, core).start()
        n_dirs = 2 if hop < half else 1

        @pl.loop(0, n_dirs)
        def _(d):
            place_rows(core, ring(z - (1 - 2 * d) * hop), True)

        for d in range(2):
            if meta_carried(d, hop):
                meta_sib(d, hop, other).wait_recv()
            for c in carried(d, hop):
                sib_copy(d, hop, c, other).wait_recv()

        @pl.loop(0, n_dirs)
        def _(d):
            place_rows(other, ring(z - (1 - 2 * d) * hop), False)

    def o_copy(slot, which):
        return remote(x_buf.at[slot, which], o_sib.at[slot], o_send.at[slot], o_recv.at[slot], device(z, other))

    @pl.loop(0, n_slot)
    def _(slot):
        buf = slot % W_DEPTH
        for copy in weight_copies(slot):
            copy.wait()
        x = x_buf[slot].reshape(CORES * nz * cap, d_model)
        hidden = jax.nn.gelu(jnp.dot(x, up_buf[buf], preferred_element_type=F32), approximate=True).astype(BF16)
        for c in range(RS_CHUNKS):
            cols = pl.ds(c * rs_cols, rs_cols)
            o = jnp.dot(hidden, down_buf[buf, :, cols], preferred_element_type=F32).astype(BF16)
            x_buf[slot, :, :, :, cols] = o.reshape(CORES, nz, cap, rs_cols)
        o_copy(slot, other).start()

        @pl.when(slot + W_DEPTH < n_slot)
        def _():
            for copy in weight_copies(slot + W_DEPTH):
                copy.start()

    @pl.loop(0, n_slot)
    def _(slot):
        o_copy(slot, other).wait_recv()

    def own_sum(pos, c):
        cols = pl.ds(pl.multiple_of(c * rs_cols, rs_cols), rs_cols)
        parts = [x_buf[:, core, pos, :, cols].reshape(rows, rs_cols), o_sib[:, pos, :, cols].reshape(rows, rs_cols)]
        if k_pad > 2 * rows:
            parts.append(jnp.zeros((k_pad - 2 * rows, rs_cols), BF16))
        total = jnp.dot(mix[pos], jnp.concatenate(parts, axis=0), preferred_element_type=F32)
        return total[:n_tok] + total[n_tok:2 * n_tok] + total[2 * n_tok:]

    skip = RS_CHUNKS // 2
    items = half * RS_CHUNKS

    def rs_copy(d, n):
        sign = 1 - 2 * d
        return remote(rs_buf.at[d, n - skip], rs_buf.at[d, n - skip + RS_CHUNKS], rs_send.at[d, n],
                      rs_recv.at[d, n + RS_CHUNKS], device(ring(z + sign), core))

    def rs_arrival(d, n):
        sign = 1 - 2 * d
        return remote(rs_buf.at[d, n - skip], rs_buf.at[d, n - skip], rs_send.at[d, n], rs_recv.at[d, n],
                      device(ring(z + sign), core))

    def rs_chunk(d, n):
        c = n % RS_CHUNKS
        return (c + skip) % RS_CHUNKS if d == 0 else c

    @pl.loop(skip, items)
    def _(n):
        away = half - n // RS_CHUNKS
        for d in range(2):
            sign = 1 - 2 * d
            value = own_sum(ring(z + sign * away), rs_chunk(d, n))

            @pl.when(n < skip + RS_CHUNKS)
            def _():
                rs_buf[d, n - skip] = value

            @pl.when(n >= skip + RS_CHUNKS)
            def _():
                rs_arrival(d, n).wait_recv()
                rs_buf[d, n - skip] += value

            rs_copy(d, n).start()

    for c in range(RS_CHUNKS):
        value = own_sum(z, c)
        for d in range(2):
            n = items + ((c + skip) % RS_CHUNKS if d == 0 else c)
            rs_arrival(d, n).wait_recv()
            value += rs_buf[d, n - skip]
        out_ref[:, c * rs_cols:(c + 1) * rs_cols] = value.astype(BF16)

    for d in range(2):
        for hop in range(1, half + 1):
            if meta_carried(d, hop):
                meta_copy(d, hop, 0).wait_send()
                meta_sib(d, hop, core).wait_send()
            for c in carried(d, hop):
                ag_copy(d, hop, c).wait_send()
                sib_copy(d, hop, c, core).wait_send()
    meta_sib(0, 0, core).wait_send()
    for c in range(AG_CHUNKS):
        sib_copy(0, 0, c, core).wait_send()

    @pl.loop(0, n_slot)
    def _(slot):
        o_copy(slot, other).wait_send()

    @pl.loop(skip, items)
    def _(n):
        for d in range(2):
            rs_copy(d, n).wait_send()


def solution(mesh):
    n_dev = mesh.shape["ep"]
    nz = n_dev // CORES
    half = nz // 2

    def group_layer(tokens, topk_idx, topk_w, w_up, w_down, slot_expert):
        n_tok, d_model = tokens.shape
        n_top = topk_idx.shape[1]
        n_slot = slot_expert.shape[1]
        n_exp = n_dev * (n_slot - 1)
        d_ff = w_up.shape[3]
        cap = -(-slot_bound(n_tok, n_top, n_dev, n_slot) // 16) * 16
        k_pad = -(-2 * n_slot * cap // 128) * 128
        meta = jnp.concatenate([topk_idx.T.astype(F32), topk_w.T], axis=0)
        skip = RS_CHUNKS // 2
        dma = pltpu.SemaphoreType.DMA
        any_space = pl.BlockSpec(memory_space=pl.ANY)
        vmem = pl.BlockSpec(memory_space=pltpu.VMEM)
        return pl.pallas_call(
            functools.partial(layer_kernel, nz),
            out_shape=jax.ShapeDtypeStruct((n_tok, d_model), BF16),
            in_specs=[any_space, any_space, pl.BlockSpec(memory_space=pltpu.SMEM), vmem, any_space, any_space],
            out_specs=vmem,
            scratch_shapes=[
                pltpu.VMEM((CORES, nz, n_tok, d_model), BF16),
                pltpu.VMEM((CORES, nz, 2 * n_top, n_tok), F32),
                pltpu.VMEM((n_slot, CORES, nz, cap, d_model), BF16),
                pltpu.VMEM((n_slot, nz, cap, d_model), BF16),
                pltpu.VMEM((W_DEPTH, d_model, d_ff), BF16),
                pltpu.VMEM((W_DEPTH, d_ff, d_model), BF16),
                pltpu.VMEM((2, (half + 1) * RS_CHUNKS - skip, n_tok, d_model // RS_CHUNKS), F32),
                pltpu.VMEM((nz, 3 * n_tok, k_pad), BF16),
                pltpu.VMEM((k_pad, n_exp), BF16),
                pltpu.VMEM((k_pad, n_exp), F32),
                dma((2,)),
                dma((2, half, AG_CHUNKS)), dma((2, half, AG_CHUNKS)),
                dma((2, half + 1, AG_CHUNKS)), dma((2, half + 1, AG_CHUNKS)),
                dma((2, half)), dma((2, half)),
                dma((2, half + 1)), dma((2, half + 1)),
                dma((2, W_DEPTH)),
                dma((n_slot,)), dma((n_slot,)),
                dma((2, half * RS_CHUNKS)), dma((2, (half + 1) * RS_CHUNKS)),
            ],
            compiler_params=pltpu.CompilerParams(collective_id=0, has_side_effects=True,
                                                 vmem_limit_bytes=62 * 1024 * 1024),
        )(tokens, meta, slot_expert, slot_expert, w_up, w_down)

    row_spec = P(("dp", "ep"), None)
    weight_spec = P("ep", None, None, None)
    return jax.shard_map(group_layer, mesh=mesh,
                         in_specs=(row_spec, row_spec, row_spec, weight_spec, weight_spec, P(None, None)),
                         out_specs=row_spec, check_vma=False)
```

```python
import functools

import jax
import jax.numpy as jnp
from jax import lax
from jax.experimental import pallas as pl
from jax.experimental.pallas import tpu as pltpu
from jax.sharding import PartitionSpec as P

MESH = pl.DeviceIdType.MESH
F32 = jnp.float32
BF16 = jnp.bfloat16
CORES = 2
W_DEPTH = 3
AG_CHUNKS = 2
RS_CHUNKS = 4
AG2_HOP = 3
AG2_STEPS = ((1, 1, 0), (3, 1, 1), (4, 2, 0), (5, 2, 1), (7, 3, 0), (8, 3, 1))


def slot_bound(n_tok, n_top, n_dev, n_slot):
    base_load = (n_tok * n_top) // (n_dev * n_slot)
    return base_load + base_load // 2 + 1


def split3(x):
    hi = x.astype(BF16)
    rest = x - hi.astype(F32)
    mid = rest.astype(BF16)
    low = (rest - mid.astype(F32)).astype(BF16)
    return hi, mid, low


def layer_kernel(nz, tok_hbm, meta_hbm, slot_smem, slot_vmem, up_hbm, down_hbm, out_ref,
                 toks, metas, x_buf, o_sib, up_buf, down_buf, rs_buf, mix, pick, target,
                 in_sem, ag_send, ag_recv, sib_send, sib_recv, ms_send, ms_recv, mb_send, mb_recv,
                 w_sem, o_send, o_recv, rs_send, rs_recv):
    half = nz // 2
    n_tok, d_model = tok_hbm.shape
    n_top = meta_hbm.shape[0] // 2
    n_slot, cap = x_buf.shape[0], x_buf.shape[3]
    rows = n_slot * cap
    k_pad, n_exp = pick.shape
    ag_rows = n_tok // AG_CHUNKS
    rs_cols = d_model // RS_CHUNKS

    me = lax.axis_index("ep")
    z = me // CORES
    core = me % CORES
    other = 1 - core

    def ring(pos):
        return (pos + nz) % nz

    def device(pos, which):
        return {"ep": pos * CORES + which}

    def remote(src, dst, send, recv, dev):
        return pltpu.make_async_remote_copy(src_ref=src, dst_ref=dst, send_sem=send, recv_sem=recv,
                                            device_id=dev, device_id_type=MESH)

    def weight_copies(step):
        buf, slot = step % W_DEPTH, step % n_slot
        return (pltpu.make_async_copy(up_hbm.at[0, slot], up_buf.at[buf], w_sem.at[0, buf]),
                pltpu.make_async_copy(down_hbm.at[0, slot], down_buf.at[buf], w_sem.at[1, buf]))

    own_tok = pltpu.make_async_copy(tok_hbm, toks.at[core, z], in_sem.at[0])
    own_meta = pltpu.make_async_copy(meta_hbm, metas.at[core, z], in_sem.at[1])
    own_meta.start()
    own_tok.start()
    barrier = pltpu.get_barrier_semaphore()
    pl.semaphore_signal(barrier, inc=1, device_id=device(ring(z + 1), core), device_id_type=MESH)
    pl.semaphore_signal(barrier, inc=1, device_id=device(ring(z - 1), core), device_id_type=MESH)
    pl.semaphore_signal(barrier, inc=1, device_id=device(z, other), device_id_type=MESH)
    pl.semaphore_wait(barrier, 3)
    own_meta.wait()
    own_tok.wait()

    def ag_copy(d, hop, c):
        sign = 1 - 2 * d
        ref = toks.at[core, ring(z - sign * (hop - 1)), pl.ds(c * ag_rows, ag_rows)]
        return remote(ref, ref, ag_send.at[d, hop - 1, c], ag_recv.at[d, hop - 1, c], device(ring(z + sign), core))

    def ag_arrival(d, hop, c):
        sign = 1 - 2 * d
        ref = toks.at[core, ring(z - sign * hop), pl.ds(c * ag_rows, ag_rows)]
        return remote(ref, ref, ag_send.at[d, hop - 1, c], ag_recv.at[d, hop - 1, c], device(ring(z + sign), core))

    def sib_copy(d, hop, c, which):
        sign = 1 - 2 * d
        ref = toks.at[which, ring(z - sign * hop), pl.ds(c * ag_rows, ag_rows)]
        return remote(ref, ref, sib_send.at[d, hop, c], sib_recv.at[d, hop, c], device(z, other))

    def meta_copy(d, hop, back):
        sign = 1 - 2 * d
        ref = metas.at[core, ring(z - sign * (hop - 1 + back))]
        return remote(ref, ref, ms_send.at[d, hop - 1], ms_recv.at[d, hop - 1], device(ring(z + sign), core))

    def meta_sib(d, hop, which):
        sign = 1 - 2 * d
        ref = metas.at[which, ring(z - sign * hop)]
        return remote(ref, ref, mb_send.at[d, hop], mb_recv.at[d, hop], device(z, other))

    def chunk_order(d):
        return list(range(AG_CHUNKS)) if d == 0 else list(range(AG_CHUNKS))[::-1]

    def carried(d, hop):
        order = chunk_order(d)
        return order if hop < half else order[:AG_CHUNKS // 2]

    def meta_carried(d, hop):
        return hop < half or d == 0

    for d in range(2):
        meta_copy(d, 1, 0).start()
    meta_sib(0, 0, core).start()

    @pl.when(core == 0)
    def _():
        for c in range(AG_CHUNKS):
            for d in range(2):
                ag_copy(d, 1, chunk_order(d)[c]).start()
        for c in range(AG_CHUNKS):
            sib_copy(0, 0, c, core).start()

    for step in range(W_DEPTH):
        for copy in weight_copies(step):
            copy.start()

    lane = lax.broadcasted_iota(jnp.int32, (cap, n_exp), 1)
    row = lax.broadcasted_iota(jnp.int32, (cap, n_exp), 0).astype(F32)
    table = slot_vmem[...]
    place = lax.broadcasted_iota(jnp.int32, table.shape, 0) * n_slot + lax.broadcasted_iota(jnp.int32, table.shape, 1)
    for w in range(2):
        dev = me if w == 0 else z * CORES + other
        for s in range(n_slot):
            exp_id = slot_smem[dev, s]
            same = table == exp_id
            copies = jnp.sum(jnp.where(same, 1.0, 0.0))
            earlier = jnp.sum(jnp.where(same & (place < dev * n_slot + s), 1.0, 0.0))
            at = pl.ds(w * rows + s * cap, cap)
            pick[at, :] = jnp.where(lane == exp_id, 1.0, 0.0).astype(BF16)
            target[at, :] = row * copies + earlier
    if k_pad > 2 * rows:
        pick[2 * rows:, :] = jnp.zeros((k_pad - 2 * rows, n_exp), BF16)
        target[2 * rows:, :] = jnp.full((k_pad - 2 * rows, n_exp), -5.0, F32)

    def place_rows(which, pos):
        info = metas[which, pos]
        exp_iota = lax.broadcasted_iota(jnp.int32, (n_exp, n_tok), 0).astype(F32)
        chosen = jnp.zeros((n_exp, n_tok), F32)
        for j in range(n_top):
            chosen = jnp.where(exp_iota == info[j:j + 1, :], 1.0, chosen)
        before = (lax.broadcasted_iota(jnp.int32, (n_tok, n_tok), 0)
                  < lax.broadcasted_iota(jnp.int32, (n_tok, n_tok), 1))
        rank = jnp.dot(chosen.astype(BF16), jnp.where(before, 1.0, 0.0).astype(BF16), preferred_element_type=F32)
        rank = jnp.where(chosen > 0.5, rank, -1.0).astype(BF16)
        takes = jnp.dot(pick[:rows, :], rank, preferred_element_type=F32) == target[:rows, :]
        onehot = jnp.where(takes, 1.0, 0.0).astype(BF16)
        for c in range(RS_CHUNKS):
            cols = pl.ds(c * rs_cols, rs_cols)
            got = jnp.dot(onehot, toks[which, pos, :, cols], preferred_element_type=F32).astype(BF16)
            x_buf[:, which, pos, :, cols] = got.reshape(n_slot, cap, rs_cols)

        @pl.when(core == which)
        def _():
            gate = jnp.zeros((n_exp, n_tok), F32)
            for j in range(n_top):
                gate = jnp.where(exp_iota == info[j:j + 1, :], info[n_top + j:n_top + j + 1, :], gate)
            takes = jnp.dot(pick[...], rank, preferred_element_type=F32) == target[...]
            parts = [jnp.dot(pick[...], part, preferred_element_type=F32) for part in split3(gate)]
            picked = jnp.where(takes, parts[0] + parts[1] + parts[2], 0.0)
            for n, part in enumerate(split3(picked.T)):
                mix[pos, n * n_tok:(n + 1) * n_tok, :] = part

    def start_gather():
        for c in range(AG_CHUNKS):
            for d in range(2):
                ag_copy(d, 1, chunk_order(d)[c]).start()
        for c in range(AG_CHUNKS):
            sib_copy(0, 0, c, core).start()

    def pass_on(hop, n):
        for d in range(2):
            if n < len(carried(d, hop)):
                c = carried(d, hop)[n]
                ag_arrival(d, hop, c).wait_recv()
                if hop < half and c in carried(d, hop + 1):
                    ag_copy(d, hop + 1, c).start()
                sib_copy(d, hop, c, core).start()

    def from_sibling(hop):
        if hop == 0:
            for c in range(AG_CHUNKS):
                sib_copy(0, 0, c, other).wait_recv()
            return
        for d in range(2):
            for c in carried(d, hop):
                sib_copy(d, hop, c, other).wait_recv()

    def place_hop(which, hop):
        @pl.loop(0, 1 if hop in (0, half) else 2)
        def _(d):
            place_rows(which, ring(z - (1 - 2 * d) * hop))

    meta_sib(0, 0, other).wait_recv()
    for hop in range(half + 1):
        if hop > 0:
            for d in range(2):
                if meta_carried(d, hop):
                    meta_copy(d, hop, 1).wait_recv()
                    if hop < half and meta_carried(d, hop + 1):
                        meta_copy(d, hop + 1, 0).start()
                    meta_sib(d, hop, core).start()

        @pl.when(core == 0)
        def _():
            if hop > 0:
                for n in range(len(carried(0, hop))):
                    pass_on(hop, n)

        @pl.when(core == 1)
        def _():
            from_sibling(hop)
            if hop == AG2_HOP:
                start_gather()

        if hop > 0:
            for d in range(2):
                if meta_carried(d, hop):
                    meta_sib(d, hop, other).wait_recv()
        place_hop(0, hop)

    def o_copy(slot):
        return remote(x_buf.at[slot, other], o_sib.at[slot], o_send.at[slot], o_recv.at[slot], device(z, other))

    def experts(slot, batch):
        step = batch * n_slot + slot
        buf = step % W_DEPTH
        for copy in weight_copies(step):
            copy.wait()
        x = x_buf[slot, batch].reshape(nz * cap, d_model)
        hidden = jax.nn.gelu(jnp.dot(x, up_buf[buf], preferred_element_type=F32), approximate=True).astype(BF16)
        for c in range(RS_CHUNKS):
            cols = pl.ds(c * rs_cols, rs_cols)
            o = jnp.dot(hidden, down_buf[buf, :, cols], preferred_element_type=F32).astype(BF16)
            x_buf[slot, batch, :, :, cols] = o.reshape(nz, cap, rs_cols)

        @pl.when(core != batch)
        def _():
            o_copy(slot).start()

        @pl.when(step + W_DEPTH < 2 * n_slot)
        def _():
            for copy in weight_copies(step + W_DEPTH):
                copy.start()

    @pl.loop(0, n_slot)
    def _(slot):
        experts(slot, 0)
        for after, hop, n in AG2_STEPS:
            @pl.when((core == 1) & (slot == after))
            def _():
                pass_on(hop, n)

    def from_sibling_o():
        @pl.loop(0, n_slot)
        def _(slot):
            o_copy(slot).wait_recv()

    def own_sum(pos, c):
        cols = pl.ds(pl.multiple_of(c * rs_cols, rs_cols), rs_cols)
        parts = [x_buf[:, core, pos, :, cols].reshape(rows, rs_cols), o_sib[:, pos, :, cols].reshape(rows, rs_cols)]
        if k_pad > 2 * rows:
            parts.append(jnp.zeros((k_pad - 2 * rows, rs_cols), BF16))
        total = jnp.dot(mix[pos], jnp.concatenate(parts, axis=0), preferred_element_type=F32)
        return total[:n_tok] + total[n_tok:2 * n_tok] + total[2 * n_tok:]

    skip = RS_CHUNKS // 2
    items = half * RS_CHUNKS

    def rs_copy(d, n):
        sign = 1 - 2 * d
        return remote(rs_buf.at[d, n - skip], rs_buf.at[d, n - skip + RS_CHUNKS], rs_send.at[d, n],
                      rs_recv.at[d, n + RS_CHUNKS], device(ring(z + sign), core))

    def rs_arrival(d, n):
        sign = 1 - 2 * d
        return remote(rs_buf.at[d, n - skip], rs_buf.at[d, n - skip], rs_send.at[d, n], rs_recv.at[d, n],
                      device(ring(z + sign), core))

    def rs_chunk(d, n):
        c = n % RS_CHUNKS
        return (c + skip) % RS_CHUNKS if d == 0 else c

    def rs_item(n):
        away = half - n // RS_CHUNKS
        for d in range(2):
            sign = 1 - 2 * d
            value = own_sum(ring(z + sign * away), rs_chunk(d, n))

            @pl.when(n < skip + RS_CHUNKS)
            def _():
                rs_buf[d, n - skip] = value

            @pl.when(n >= skip + RS_CHUNKS)
            def _():
                rs_arrival(d, n).wait_recv()
                rs_buf[d, n - skip] += value

            rs_copy(d, n).start()

    @pl.when(core == 0)
    def _():
        from_sibling_o()
        pl.loop(skip, skip + RS_CHUNKS)(rs_item)

    @pl.when(core == 1)
    def _():
        for n in range(len(carried(0, half))):
            pass_on(half, n)

    for hop in range(half + 1):
        @pl.when(core == 0)
        def _():
            from_sibling(hop)

        place_hop(1, hop)

    @pl.loop(0, n_slot)
    def _(slot):
        experts(slot, 1)

        @pl.when(core == 0)
        def _():
            rs_item(skip + RS_CHUNKS + slot)

    @pl.when(core == 1)
    def _():
        from_sibling_o()

    pl.loop(jnp.where(core == 0, skip + RS_CHUNKS + n_slot, skip), items)(rs_item)

    for c in range(RS_CHUNKS):
        value = own_sum(z, c)
        for d in range(2):
            n = items + ((c + skip) % RS_CHUNKS if d == 0 else c)
            rs_arrival(d, n).wait_recv()
            value += rs_buf[d, n - skip]
        out_ref[:, c * rs_cols:(c + 1) * rs_cols] = value.astype(BF16)

    for d in range(2):
        for hop in range(1, half + 1):
            if meta_carried(d, hop):
                meta_copy(d, hop, 0).wait_send()
                meta_sib(d, hop, core).wait_send()
            for c in carried(d, hop):
                ag_copy(d, hop, c).wait_send()
                sib_copy(d, hop, c, core).wait_send()
    meta_sib(0, 0, core).wait_send()
    for c in range(AG_CHUNKS):
        sib_copy(0, 0, c, core).wait_send()

    @pl.loop(0, n_slot)
    def _(slot):
        o_copy(slot).wait_send()

    @pl.loop(skip, items)
    def _(n):
        for d in range(2):
            rs_copy(d, n).wait_send()


def solution(mesh):
    n_dev = mesh.shape["ep"]
    nz = n_dev // CORES
    half = nz // 2

    def group_layer(tokens, topk_idx, topk_w, w_up, w_down, slot_expert):
        n_tok, d_model = tokens.shape
        n_top = topk_idx.shape[1]
        n_slot = slot_expert.shape[1]
        n_exp = n_dev * (n_slot - 1)
        d_ff = w_up.shape[3]
        cap = -(-slot_bound(n_tok, n_top, n_dev, n_slot) // 16) * 16
        k_pad = -(-2 * n_slot * cap // 128) * 128
        meta = jnp.concatenate([topk_idx.T.astype(F32), topk_w.T], axis=0)
        skip = RS_CHUNKS // 2
        dma = pltpu.SemaphoreType.DMA
        any_space = pl.BlockSpec(memory_space=pl.ANY)
        vmem = pl.BlockSpec(memory_space=pltpu.VMEM)
        return pl.pallas_call(
            functools.partial(layer_kernel, nz),
            out_shape=jax.ShapeDtypeStruct((n_tok, d_model), BF16),
            in_specs=[any_space, any_space, pl.BlockSpec(memory_space=pltpu.SMEM), vmem, any_space, any_space],
            out_specs=vmem,
            scratch_shapes=[
                pltpu.VMEM((CORES, nz, n_tok, d_model), BF16),
                pltpu.VMEM((CORES, nz, 2 * n_top, n_tok), F32),
                pltpu.VMEM((n_slot, CORES, nz, cap, d_model), BF16),
                pltpu.VMEM((n_slot, nz, cap, d_model), BF16),
                pltpu.VMEM((W_DEPTH, d_model, d_ff), BF16),
                pltpu.VMEM((W_DEPTH, d_ff, d_model), BF16),
                pltpu.VMEM((2, (half + 1) * RS_CHUNKS - skip, n_tok, d_model // RS_CHUNKS), F32),
                pltpu.VMEM((nz, 3 * n_tok, k_pad), BF16),
                pltpu.VMEM((k_pad, n_exp), BF16),
                pltpu.VMEM((k_pad, n_exp), F32),
                dma((2,)),
                dma((2, half, AG_CHUNKS)), dma((2, half, AG_CHUNKS)),
                dma((2, half + 1, AG_CHUNKS)), dma((2, half + 1, AG_CHUNKS)),
                dma((2, half)), dma((2, half)),
                dma((2, half + 1)), dma((2, half + 1)),
                dma((2, W_DEPTH)),
                dma((n_slot,)), dma((n_slot,)),
                dma((2, half * RS_CHUNKS)), dma((2, (half + 1) * RS_CHUNKS)),
            ],
            compiler_params=pltpu.CompilerParams(collective_id=0, has_side_effects=True,
                                                 vmem_limit_bytes=62 * 1024 * 1024),
        )(tokens, meta, slot_expert, slot_expert, w_up, w_down)

    row_spec = P(("dp", "ep"), None)
    weight_spec = P("ep", None, None, None)
    return jax.shard_map(group_layer, mesh=mesh,
                         in_specs=(row_spec, row_spec, row_spec, weight_spec, weight_spec, P(None, None)),
                         out_specs=row_spec, check_vma=False)
```

```python
import functools

import jax
import jax.numpy as jnp
from jax import lax
from jax.experimental import pallas as pl
from jax.experimental.pallas import tpu as pltpu
from jax.sharding import PartitionSpec as P

MESH = pl.DeviceIdType.MESH
F32 = jnp.float32
BF16 = jnp.bfloat16
CORES = 2
W_DEPTH = 3
AG_CHUNKS = 2
RS_CHUNKS = 4
AG2_HOP = 3
AG2_STEPS = ((0, 1, 0), (2, 1, 1), (3, 2, 0), (5, 2, 1), (7, 3, 0), (8, 3, 1))


def slot_bound(n_tok, n_top, n_dev, n_slot):
    base_load = (n_tok * n_top) // (n_dev * n_slot)
    return base_load + base_load // 2 + 1


def round_up(n, unit):
    return -(-n // unit) * unit


def split3(x):
    hi = x.astype(BF16)
    rest = x - hi.astype(F32)
    mid = rest.astype(BF16)
    low = (rest - mid.astype(F32)).astype(BF16)
    return hi, mid, low


def layer_kernel(nz, bound, tok_hbm, idx_hbm, gate_hbm, slot_smem, slot_vmem, up_hbm, down_hbm, out_ref,
                 toks, idx_own, metas, x_buf, o_sib, up_buf, down_buf, rs_buf, first_out, first_in, total_buf,
                 mix, mix_up, pick, target, pick_up, target_up, pack,
                 in_sem, ag_send, ag_recv, sib_send, sib_recv, ms_send, ms_recv, mb_send, mb_recv,
                 w_sem, o_send, o_recv, rs_send, rs_recv):
    half = nz // 2
    n_tok, d_model = tok_hbm.shape
    n_top = idx_hbm.shape[0]
    n_slot, cap = x_buf.shape[0], x_buf.shape[3]
    rows = n_slot * cap
    k_pad, n_exp = pick.shape
    packed, packed_pad = first_out.shape[2], pack.shape[0]
    ag_rows = n_tok // AG_CHUNKS
    rs_cols = d_model // RS_CHUNKS

    me = lax.axis_index("ep")
    z = me // CORES
    core = me % CORES
    other = 1 - core

    def ring(pos):
        return (pos + nz) % nz

    def device(pos, which):
        return {"ep": pos * CORES + which}

    def remote(src, dst, send, recv, dev):
        return pltpu.make_async_remote_copy(src_ref=src, dst_ref=dst, send_sem=send, recv_sem=recv,
                                            device_id=dev, device_id_type=MESH)

    def weight_copies(step):
        buf, slot = step % W_DEPTH, step % n_slot
        return (pltpu.make_async_copy(up_hbm.at[0, slot], up_buf.at[buf], w_sem.at[0, buf]),
                pltpu.make_async_copy(down_hbm.at[0, slot], down_buf.at[buf], w_sem.at[1, buf]))

    own_tok = pltpu.make_async_copy(tok_hbm, toks.at[core, z], in_sem.at[0])
    own_idx = pltpu.make_async_copy(idx_hbm, idx_own, in_sem.at[1])
    own_gate = pltpu.make_async_copy(gate_hbm, metas.at[core, z, n_top:], in_sem.at[2])
    own_tok.start()
    own_idx.start()
    own_gate.start()
    barrier = pltpu.get_barrier_semaphore()
    pl.semaphore_signal(barrier, inc=1, device_id=device(ring(z + 1), core), device_id_type=MESH)
    pl.semaphore_signal(barrier, inc=1, device_id=device(ring(z - 1), core), device_id_type=MESH)
    pl.semaphore_signal(barrier, inc=1, device_id=device(z, other), device_id_type=MESH)
    own_idx.wait()
    metas[core, z, :n_top, :] = idx_own[...].astype(F32)
    own_gate.wait()
    own_tok.wait()
    pl.semaphore_wait(barrier, 3)

    def ag_copy(d, hop, c):
        sign = 1 - 2 * d
        ref = toks.at[core, ring(z - sign * (hop - 1)), pl.ds(c * ag_rows, ag_rows)]
        return remote(ref, ref, ag_send.at[d, hop - 1, c], ag_recv.at[d, hop - 1, c], device(ring(z + sign), core))

    def ag_arrival(d, hop, c):
        sign = 1 - 2 * d
        ref = toks.at[core, ring(z - sign * hop), pl.ds(c * ag_rows, ag_rows)]
        return remote(ref, ref, ag_send.at[d, hop - 1, c], ag_recv.at[d, hop - 1, c], device(ring(z + sign), core))

    def sib_copy(d, hop, c, which):
        sign = 1 - 2 * d
        ref = toks.at[which, ring(z - sign * hop), pl.ds(c * ag_rows, ag_rows)]
        return remote(ref, ref, sib_send.at[d, hop, c], sib_recv.at[d, hop, c], device(z, other))

    def meta_copy(d, hop, back):
        sign = 1 - 2 * d
        ref = metas.at[core, ring(z - sign * (hop - 1 + back))]
        return remote(ref, ref, ms_send.at[d, hop - 1], ms_recv.at[d, hop - 1], device(ring(z + sign), core))

    def meta_sib(d, hop, which):
        sign = 1 - 2 * d
        ref = metas.at[which, ring(z - sign * hop)]
        return remote(ref, ref, mb_send.at[d, hop], mb_recv.at[d, hop], device(z, other))

    def chunk_order(d):
        return list(range(AG_CHUNKS)) if d == 0 else list(range(AG_CHUNKS))[::-1]

    def carried(d, hop):
        order = chunk_order(d)
        return order if hop < half else order[:AG_CHUNKS // 2]

    def meta_carried(d, hop):
        return hop < half or d == 0

    @pl.when(core == 0)
    def _():
        for c in range(AG_CHUNKS):
            for d in range(2):
                ag_copy(d, 1, chunk_order(d)[c]).start()
        for c in range(AG_CHUNKS):
            sib_copy(0, 0, c, core).start()

    for d in range(2):
        meta_copy(d, 1, 0).start()
    meta_sib(0, 0, core).start()
    for step in range(W_DEPTH):
        for copy in weight_copies(step):
            copy.start()

    lane = lax.broadcasted_iota(jnp.int32, (cap, n_exp), 1)
    row = lax.broadcasted_iota(jnp.int32, (cap, n_exp), 0).astype(F32)
    table = slot_vmem[...]
    place = lax.broadcasted_iota(jnp.int32, table.shape, 0) * n_slot + lax.broadcasted_iota(jnp.int32, table.shape, 1)
    if k_pad > 2 * rows:
        pick[2 * rows:, :] = jnp.zeros((k_pad - 2 * rows, n_exp), BF16)
        target[2 * rows:, :] = jnp.full((k_pad - 2 * rows, n_exp), -1.0, F32)

    def slot_rows(pos):
        for w in range(2):
            dev = pos * CORES + (core if w == 0 else other)
            for s in range(n_slot):
                exp_id = slot_smem[dev, s]
                same = table == exp_id
                copies = jnp.sum(jnp.where(same, 1.0, 0.0))
                earlier = jnp.sum(jnp.where(same & (place < dev * n_slot + s), 1.0, 0.0))
                at = pl.ds(w * rows + s * cap, cap)
                pick[at, :] = jnp.where(lane == exp_id, 1.0, 0.0).astype(BF16)
                target[at, :] = row * copies + earlier

    column = lax.broadcasted_iota(jnp.int32, (packed_pad, k_pad), 1)
    side = jnp.where(column >= rows, 1, 0)
    in_side = column - side * rows
    in_slot = in_side % cap
    packed_row = side * (packed // 2) + (in_side // cap) * bound + in_slot
    used = (in_slot < bound) & (column < 2 * rows)
    pack[...] = jnp.where(used & (lax.broadcasted_iota(jnp.int32, (packed_pad, k_pad), 0) == packed_row),
                          1.0, 0.0).astype(BF16)
    for d in range(2):
        slot_rows(ring(z - (1 - 2 * d)))
        pick_up[d] = jnp.dot(pack[...], pick[...], preferred_element_type=F32).astype(BF16)
        target_up[d] = jnp.dot(pack[...], (target[...] + 1.0).astype(BF16), preferred_element_type=F32) - 1.0
    slot_rows(z)

    exp_iota = lax.broadcasted_iota(jnp.int32, (n_exp, n_tok), 0).astype(F32)

    def ranks(info):
        chosen = jnp.zeros((n_exp, n_tok), F32)
        for j in range(n_top):
            chosen = jnp.where(exp_iota == info[j:j + 1, :], 1.0, chosen)
        before = (lax.broadcasted_iota(jnp.int32, (n_tok, n_tok), 0)
                  < lax.broadcasted_iota(jnp.int32, (n_tok, n_tok), 1))
        rank = jnp.dot(chosen.astype(BF16), jnp.where(before, 1.0, 0.0).astype(BF16), preferred_element_type=F32)
        return jnp.where(chosen > 0.5, rank, -1.0).astype(BF16)

    def mixing(info, rank, picks, targets):
        gate = jnp.zeros((n_exp, n_tok), F32)
        for j in range(n_top):
            gate = jnp.where(exp_iota == info[j:j + 1, :], info[n_top + j:n_top + j + 1, :], gate)
        takes = jnp.dot(picks, rank, preferred_element_type=F32) == targets
        parts = [jnp.dot(picks, part, preferred_element_type=F32) for part in split3(gate)]
        return split3(jnp.where(takes, parts[0] + parts[1] + parts[2], 0.0).T)

    def mix_first_hop():
        @pl.loop(0, 4)
        def _(i):
            d, j = i // 2, i % 2
            info = metas[core, ring(z + (1 - 2 * d) * (half - 1 - j))]
            for n, part in enumerate(mixing(info, ranks(info), pick_up[d], target_up[d])):
                mix_up[d, j, n * n_tok:(n + 1) * n_tok, :] = part

    def place_rows(which, pos):
        info = metas[which, pos]
        rank = ranks(info)
        takes = jnp.dot(pick[:rows, :], rank, preferred_element_type=F32) == target[:rows, :]
        onehot = jnp.where(takes, 1.0, 0.0).astype(BF16)
        for c in range(RS_CHUNKS):
            cols = pl.ds(c * rs_cols, rs_cols)
            got = jnp.dot(onehot, toks[which, pos, :, cols], preferred_element_type=F32).astype(BF16)
            x_buf[:, which, pos, :, cols] = got.reshape(n_slot, cap, rs_cols)

        @pl.when(core == which)
        def _():
            for n, part in enumerate(mixing(info, rank, pick[...], target[...])):
                mix[pos, n * n_tok:(n + 1) * n_tok, :] = part

    def start_gather():
        for c in range(AG_CHUNKS):
            for d in range(2):
                ag_copy(d, 1, chunk_order(d)[c]).start()
        for c in range(AG_CHUNKS):
            sib_copy(0, 0, c, core).start()

    def pass_on(hop, n):
        for d in range(2):
            if n < len(carried(d, hop)):
                c = carried(d, hop)[n]
                ag_arrival(d, hop, c).wait_recv()
                if hop < half and c in carried(d, hop + 1):
                    ag_copy(d, hop + 1, c).start()
                sib_copy(d, hop, c, core).start()

    def from_sibling(hop):
        if hop == 0:
            for c in range(AG_CHUNKS):
                sib_copy(0, 0, c, other).wait_recv()
            return
        for d in range(2):
            for c in carried(d, hop):
                sib_copy(d, hop, c, other).wait_recv()

    def place_hop(which, hop):
        @pl.loop(0, 1 if hop in (0, half) else 2)
        def _(d):
            place_rows(which, ring(z - (1 - 2 * d) * hop))

    meta_sib(0, 0, other).wait_recv()
    for hop in range(half + 1):
        if hop > 0:
            for d in range(2):
                if meta_carried(d, hop):
                    meta_copy(d, hop, 1).wait_recv()
                    if hop < half and meta_carried(d, hop + 1):
                        meta_copy(d, hop + 1, 0).start()
                    meta_sib(d, hop, core).start()

        @pl.when(core == 0)
        def _():
            if hop > 0:
                for n in range(len(carried(0, hop))):
                    pass_on(hop, n)

        @pl.when(core == 1)
        def _():
            from_sibling(hop)
            if hop == AG2_HOP:
                start_gather()

        if hop > 0:
            for d in range(2):
                if meta_carried(d, hop):
                    meta_sib(d, hop, other).wait_recv()
        place_hop(0, hop)
        if hop == half - 1:
            @pl.when(core == 0)
            def _():
                mix_first_hop()

    def o_copy(slot):
        return remote(x_buf.at[slot, other], o_sib.at[slot], o_send.at[slot], o_recv.at[slot], device(z, other))

    def experts(slot, batch):
        step = batch * n_slot + slot
        buf = step % W_DEPTH
        for copy in weight_copies(step):
            copy.wait()
        x = x_buf[slot, batch].reshape(nz * cap, d_model)
        hidden = jax.nn.gelu(jnp.dot(x, up_buf[buf], preferred_element_type=F32), approximate=True).astype(BF16)
        for c in range(RS_CHUNKS):
            cols = pl.ds(c * rs_cols, rs_cols)
            o = jnp.dot(hidden, down_buf[buf, :, cols], preferred_element_type=F32).astype(BF16)
            x_buf[slot, batch, :, :, cols] = o.reshape(nz, cap, rs_cols)

        @pl.when(core != batch)
        def _():
            o_copy(slot).start()

        @pl.when(step + W_DEPTH < 2 * n_slot)
        def _():
            for copy in weight_copies(step + W_DEPTH):
                copy.start()

    @pl.loop(0, n_slot)
    def _(slot):
        experts(slot, 0)
        for after, hop, n in AG2_STEPS:
            @pl.when((core == 1) & (slot == after))
            def _():
                pass_on(hop, n)

    def from_sibling_o():
        @pl.loop(0, n_slot)
        def _(slot):
            o_copy(slot).wait_recv()

    def chip_rows(pos, c):
        cols = pl.ds(pl.multiple_of(c * rs_cols, rs_cols), rs_cols)
        parts = [x_buf[:, core, pos, :, cols].reshape(rows, rs_cols), o_sib[:, pos, :, cols].reshape(rows, rs_cols)]
        if k_pad > 2 * rows:
            parts.append(jnp.zeros((k_pad - 2 * rows, rs_cols), BF16))
        return jnp.concatenate(parts, axis=0)

    def mixed(weights, values):
        total = jnp.dot(weights, values, preferred_element_type=F32)
        return total[:n_tok] + total[n_tok:2 * n_tok] + total[2 * n_tok:]

    def own_sum(pos, c):
        return mixed(mix[pos], chip_rows(pos, c))

    skip = RS_CHUNKS // 2
    first = skip + RS_CHUNKS
    items = half * RS_CHUNKS

    def rs_chunk(d, n):
        c = n % RS_CHUNKS
        return (c + skip) % RS_CHUNKS if d == 0 else c

    def rs_dest(d, n):
        return ring(z + (1 - 2 * d) * (half - n // RS_CHUNKS))

    def first_copy(d, n):
        return remote(first_out.at[d, n - skip], first_in.at[d, n - skip], rs_send.at[d, n],
                      rs_recv.at[d, n + RS_CHUNKS], device(ring(z + (1 - 2 * d)), core))

    def first_arrival(d, n):
        return remote(first_out.at[d, n - first], first_in.at[d, n - first], rs_send.at[d, n],
                      rs_recv.at[d, n], device(ring(z + (1 - 2 * d)), core))

    def rs_copy(d, n):
        return remote(rs_buf.at[d, n - first], rs_buf.at[d, n - first + RS_CHUNKS], rs_send.at[d, n],
                      rs_recv.at[d, n + RS_CHUNKS], device(ring(z + (1 - 2 * d)), core))

    def rs_arrival(d, n):
        return remote(rs_buf.at[d, n - first], rs_buf.at[d, n - first], rs_send.at[d, n], rs_recv.at[d, n],
                      device(ring(z + (1 - 2 * d)), core))

    def first_item(n):
        for d in range(2):
            got = jnp.dot(pack[:packed, :], chip_rows(rs_dest(d, n), rs_chunk(d, n)), preferred_element_type=F32)
            first_out[d, n - skip] = got.astype(BF16)
            first_copy(d, n).start()

    def second_item(n):
        for d in range(2):
            value = own_sum(rs_dest(d, n), rs_chunk(d, n))
            first_arrival(d, n).wait_recv()
            rows_in = first_in[d, n - first]
            if packed_pad > packed:
                rows_in = jnp.concatenate([rows_in, jnp.zeros((packed_pad - packed, rs_cols), BF16)], axis=0)
            rs_buf[d, n - first] = value + mixed(mix_up[d, (n - first) // skip], rows_in)
            rs_copy(d, n).start()

    def later_item(n):
        for d in range(2):
            value = own_sum(rs_dest(d, n), rs_chunk(d, n))
            rs_arrival(d, n).wait_recv()
            rs_buf[d, n - first] += value
            rs_copy(d, n).start()

    def start_chains():
        from_sibling_o()
        pl.loop(skip, first)(first_item)

    @pl.when(core == 0)
    def _():
        start_chains()

    @pl.when(core == 1)
    def _():
        for n in range(len(carried(0, half))):
            pass_on(half, n)

    for hop in range(half + 1):
        @pl.when(core == 0)
        def _():
            from_sibling(hop)

        place_hop(1, hop)

    @pl.loop(0, n_slot)
    def _(slot):
        experts(slot, 1)

        @pl.when((core == 0) & (slot < RS_CHUNKS))
        def _():
            second_item(first + slot)

        @pl.when((core == 0) & (slot >= RS_CHUNKS))
        def _():
            later_item(first + slot)

    @pl.when(core == 1)
    def _():
        mix_first_hop()
        start_chains()
        pl.loop(first, first + RS_CHUNKS)(second_item)

    pl.loop(jnp.where(core == 0, first + n_slot, first + RS_CHUNKS), items)(later_item)

    for c in range(RS_CHUNKS):
        total_buf[c] = own_sum(z, c)
    for i in range(RS_CHUNKS):
        for d in range(2):
            rs_arrival(d, items + i).wait_recv()
        if i >= skip:
            for c in (i - skip, i):
                value = total_buf[c]
                for d in range(2):
                    value += rs_buf[d, items - first + ((c + skip) % RS_CHUNKS if d == 0 else c)]
                out_ref[:, c * rs_cols:(c + 1) * rs_cols] = value.astype(BF16)

    for d in range(2):
        for hop in range(1, half + 1):
            if meta_carried(d, hop):
                meta_copy(d, hop, 0).wait_send()
                meta_sib(d, hop, core).wait_send()
            for c in carried(d, hop):
                ag_copy(d, hop, c).wait_send()
                sib_copy(d, hop, c, core).wait_send()
    meta_sib(0, 0, core).wait_send()
    for c in range(AG_CHUNKS):
        sib_copy(0, 0, c, core).wait_send()

    @pl.loop(0, n_slot)
    def _(slot):
        o_copy(slot).wait_send()

    @pl.loop(skip, first)
    def _(n):
        for d in range(2):
            first_copy(d, n).wait_send()

    @pl.loop(first, items)
    def _(n):
        for d in range(2):
            rs_copy(d, n).wait_send()


def solution(mesh):
    n_dev = mesh.shape["ep"]
    nz = n_dev // CORES
    half = nz // 2

    def group_layer(tokens, topk_idx, topk_w, w_up, w_down, slot_expert):
        n_tok, d_model = tokens.shape
        n_top = topk_idx.shape[1]
        n_slot = slot_expert.shape[1]
        n_exp = n_dev * (n_slot - 1)
        d_ff = w_up.shape[3]
        bound = slot_bound(n_tok, n_top, n_dev, n_slot)
        cap = round_up(bound, 16)
        k_pad = round_up(2 * n_slot * cap, 128)
        packed = 2 * round_up(n_slot * bound, 8)
        packed_pad = round_up(packed, 128)
        rs_cols = d_model // RS_CHUNKS
        skip = RS_CHUNKS // 2
        dma = pltpu.SemaphoreType.DMA
        any_space = pl.BlockSpec(memory_space=pl.ANY)
        vmem = pl.BlockSpec(memory_space=pltpu.VMEM)
        return pl.pallas_call(
            functools.partial(layer_kernel, nz, bound),
            out_shape=jax.ShapeDtypeStruct((n_tok, d_model), BF16),
            in_specs=[any_space, any_space, any_space, pl.BlockSpec(memory_space=pltpu.SMEM), vmem, any_space, any_space],
            out_specs=vmem,
            scratch_shapes=[
                pltpu.VMEM((CORES, nz, n_tok, d_model), BF16),
                pltpu.VMEM((n_top, n_tok), jnp.int32),
                pltpu.VMEM((CORES, nz, 2 * n_top, n_tok), F32),
                pltpu.VMEM((n_slot, CORES, nz, cap, d_model), BF16),
                pltpu.VMEM((n_slot, nz, cap, d_model), BF16),
                pltpu.VMEM((W_DEPTH, d_model, d_ff), BF16),
                pltpu.VMEM((W_DEPTH, d_ff, d_model), BF16),
                pltpu.VMEM((2, half * RS_CHUNKS - skip, n_tok, rs_cols), F32),
                pltpu.VMEM((2, RS_CHUNKS, packed, rs_cols), BF16),
                pltpu.VMEM((2, RS_CHUNKS, packed, rs_cols), BF16),
                pltpu.VMEM((RS_CHUNKS, n_tok, rs_cols), F32),
                pltpu.VMEM((nz, 3 * n_tok, k_pad), BF16),
                pltpu.VMEM((2, 2, 3 * n_tok, packed_pad), BF16),
                pltpu.VMEM((k_pad, n_exp), BF16),
                pltpu.VMEM((k_pad, n_exp), F32),
                pltpu.VMEM((2, packed_pad, n_exp), BF16),
                pltpu.VMEM((2, packed_pad, n_exp), F32),
                pltpu.VMEM((packed_pad, k_pad), BF16),
                dma((3,)),
                dma((2, half, AG_CHUNKS)), dma((2, half, AG_CHUNKS)),
                dma((2, half + 1, AG_CHUNKS)), dma((2, half + 1, AG_CHUNKS)),
                dma((2, half)), dma((2, half)),
                dma((2, half + 1)), dma((2, half + 1)),
                dma((2, W_DEPTH)),
                dma((n_slot,)), dma((n_slot,)),
                dma((2, half * RS_CHUNKS)), dma((2, (half + 1) * RS_CHUNKS)),
            ],
            compiler_params=pltpu.CompilerParams(collective_id=0, has_side_effects=True,
                                                 vmem_limit_bytes=62 * 1024 * 1024),
        )(tokens, topk_idx.T, topk_w.T, slot_expert, slot_expert, w_up, w_down)

    row_spec = P(("dp", "ep"), None)
    weight_spec = P("ep", None, None, None)
    return jax.shard_map(group_layer, mesh=mesh,
                         in_specs=(row_spec, row_spec, row_spec, weight_spec, weight_spec, P(None, None)),
                         out_specs=row_spec, check_vma=False)
```

```python
import functools

import jax
import jax.numpy as jnp
from jax import lax
from jax.experimental import pallas as pl
from jax.experimental.pallas import tpu as pltpu
from jax.sharding import PartitionSpec as P

MESH = pl.DeviceIdType.MESH
F32 = jnp.float32
BF16 = jnp.bfloat16
CORES = 2
W_DEPTH = 3
AG_CHUNKS = 2
RS_CHUNKS = 4
AG2_HOP = 3
AG2_STEPS = ((0, 1, 0), (2, 1, 1), (3, 2, 0), (5, 2, 1), (7, 3, 0), (8, 3, 1))


def slot_bound(n_tok, n_top, n_dev, n_slot):
    base_load = (n_tok * n_top) // (n_dev * n_slot)
    return base_load + base_load // 2 + 1


def round_up(n, unit):
    return -(-n // unit) * unit


def split3(x):
    hi = x.astype(BF16)
    rest = x - hi.astype(F32)
    mid = rest.astype(BF16)
    low = (rest - mid.astype(F32)).astype(BF16)
    return hi, mid, low


def layer_kernel(nz, bound, tok_hbm, idx_hbm, gate_hbm, slot_smem, slot_vmem, up_hbm, down_hbm, out_ref,
                 toks, idx_own, metas, x_buf, o_sib, up_buf, down_buf, rs_buf, first_out, first_in, total_buf,
                 mix, mix_up, pick, target, pick_up, target_up, pack,
                 in_sem, ag_send, ag_recv, sib_send, sib_recv, ms_send, ms_recv, mb_send, mb_recv,
                 w_sem, o_send, o_recv, rs_send, rs_recv):
    half = nz // 2
    n_tok, d_model = tok_hbm.shape
    n_top = idx_hbm.shape[0]
    n_slot, cap = x_buf.shape[0], x_buf.shape[3]
    rows = n_slot * cap
    k_pad, n_exp = pick.shape
    packed, packed_pad = first_out.shape[2], pack.shape[0]
    ag_rows = n_tok // AG_CHUNKS
    rs_cols = d_model // RS_CHUNKS

    me = lax.axis_index("ep")
    z = me // CORES
    core = me % CORES
    other = 1 - core

    def ring(pos):
        return (pos + nz) % nz

    def device(pos, which):
        return {"ep": pos * CORES + which}

    def remote(src, dst, send, recv, dev):
        return pltpu.make_async_remote_copy(src_ref=src, dst_ref=dst, send_sem=send, recv_sem=recv,
                                            device_id=dev, device_id_type=MESH)

    def weight_copies(step):
        buf, slot = step % W_DEPTH, step % n_slot
        return (pltpu.make_async_copy(up_hbm.at[0, slot], up_buf.at[buf], w_sem.at[0, buf]),
                pltpu.make_async_copy(down_hbm.at[0, slot], down_buf.at[buf], w_sem.at[1, buf]))

    own_tok = pltpu.make_async_copy(tok_hbm, toks.at[core, z], in_sem.at[0])
    own_idx = pltpu.make_async_copy(idx_hbm, idx_own, in_sem.at[1])
    own_gate = pltpu.make_async_copy(gate_hbm, metas.at[core, z, n_top:], in_sem.at[2])
    own_tok.start()
    own_idx.start()
    own_gate.start()
    barrier = pltpu.get_barrier_semaphore()
    pl.semaphore_signal(barrier, inc=1, device_id=device(ring(z + 1), core), device_id_type=MESH)
    pl.semaphore_signal(barrier, inc=1, device_id=device(ring(z - 1), core), device_id_type=MESH)
    pl.semaphore_signal(barrier, inc=1, device_id=device(z, other), device_id_type=MESH)
    own_idx.wait()
    metas[core, z, :n_top, :] = idx_own[...].astype(F32)
    own_gate.wait()
    own_tok.wait()
    pl.semaphore_wait(barrier, 3)

    def ag_copy(d, hop, c):
        sign = 1 - 2 * d
        ref = toks.at[core, ring(z - sign * (hop - 1)), pl.ds(c * ag_rows, ag_rows)]
        return remote(ref, ref, ag_send.at[d, hop - 1, c], ag_recv.at[d, hop - 1, c], device(ring(z + sign), core))

    def ag_arrival(d, hop, c):
        sign = 1 - 2 * d
        ref = toks.at[core, ring(z - sign * hop), pl.ds(c * ag_rows, ag_rows)]
        return remote(ref, ref, ag_send.at[d, hop - 1, c], ag_recv.at[d, hop - 1, c], device(ring(z + sign), core))

    def sib_copy(d, hop, c, which):
        sign = 1 - 2 * d
        ref = toks.at[which, ring(z - sign * hop), pl.ds(c * ag_rows, ag_rows)]
        return remote(ref, ref, sib_send.at[d, hop, c], sib_recv.at[d, hop, c], device(z, other))

    def meta_copy(d, hop, back):
        sign = 1 - 2 * d
        ref = metas.at[core, ring(z - sign * (hop - 1 + back))]
        return remote(ref, ref, ms_send.at[d, hop - 1], ms_recv.at[d, hop - 1], device(ring(z + sign), core))

    def meta_sib(d, hop, which):
        sign = 1 - 2 * d
        ref = metas.at[which, ring(z - sign * hop)]
        return remote(ref, ref, mb_send.at[d, hop], mb_recv.at[d, hop], device(z, other))

    def chunk_order(d):
        return list(range(AG_CHUNKS)) if d == 0 else list(range(AG_CHUNKS))[::-1]

    def carried(d, hop):
        order = chunk_order(d)
        return order if hop < half else order[:AG_CHUNKS // 2]

    def meta_carried(d, hop):
        return hop < half or d == 0

    for d in range(2):
        meta_copy(d, 1, 0).start()
    meta_sib(0, 0, core).start()

    @pl.when(core == 0)
    def _():
        for c in range(AG_CHUNKS):
            for d in range(2):
                ag_copy(d, 1, chunk_order(d)[c]).start()
        for c in range(AG_CHUNKS):
            sib_copy(0, 0, c, core).start()

    for step in range(W_DEPTH):
        for copy in weight_copies(step):
            copy.start()

    lane = lax.broadcasted_iota(jnp.int32, (cap, n_exp), 1)
    row = lax.broadcasted_iota(jnp.int32, (cap, n_exp), 0).astype(F32)
    table = slot_vmem[...]
    place = lax.broadcasted_iota(jnp.int32, table.shape, 0) * n_slot + lax.broadcasted_iota(jnp.int32, table.shape, 1)
    if k_pad > 2 * rows:
        pick[2 * rows:, :] = jnp.zeros((k_pad - 2 * rows, n_exp), BF16)
        target[2 * rows:, :] = jnp.full((k_pad - 2 * rows, n_exp), -1.0, F32)

    def slot_rows(pos):
        for w in range(2):
            dev = pos * CORES + (core if w == 0 else other)
            for s in range(n_slot):
                exp_id = slot_smem[dev, s]
                same = table == exp_id
                copies = jnp.sum(jnp.where(same, 1.0, 0.0))
                earlier = jnp.sum(jnp.where(same & (place < dev * n_slot + s), 1.0, 0.0))
                at = pl.ds(w * rows + s * cap, cap)
                pick[at, :] = jnp.where(lane == exp_id, 1.0, 0.0).astype(BF16)
                target[at, :] = row * copies + earlier

    column = lax.broadcasted_iota(jnp.int32, (packed_pad, k_pad), 1)
    side = jnp.where(column >= rows, 1, 0)
    in_side = column - side * rows
    in_slot = in_side % cap
    packed_row = side * (packed // 2) + (in_side // cap) * bound + in_slot
    used = (in_slot < bound) & (column < 2 * rows)
    pack[...] = jnp.where(used & (lax.broadcasted_iota(jnp.int32, (packed_pad, k_pad), 0) == packed_row),
                          1.0, 0.0).astype(BF16)
    for d in range(2):
        slot_rows(ring(z - (1 - 2 * d)))
        pick_up[d] = jnp.dot(pack[...], pick[...], preferred_element_type=F32).astype(BF16)
        target_up[d] = jnp.dot(pack[...], (target[...] + 1.0).astype(BF16), preferred_element_type=F32) - 1.0
    slot_rows(z)

    exp_iota = lax.broadcasted_iota(jnp.int32, (n_exp, n_tok), 0).astype(F32)

    def ranks(info):
        chosen = jnp.zeros((n_exp, n_tok), F32)
        for j in range(n_top):
            chosen = jnp.where(exp_iota == info[j:j + 1, :], 1.0, chosen)
        before = (lax.broadcasted_iota(jnp.int32, (n_tok, n_tok), 0)
                  < lax.broadcasted_iota(jnp.int32, (n_tok, n_tok), 1))
        rank = jnp.dot(chosen.astype(BF16), jnp.where(before, 1.0, 0.0).astype(BF16), preferred_element_type=F32)
        return jnp.where(chosen > 0.5, rank, -1.0).astype(BF16)

    def mixing(info, rank, picks, targets):
        gate = jnp.zeros((n_exp, n_tok), F32)
        for j in range(n_top):
            gate = jnp.where(exp_iota == info[j:j + 1, :], info[n_top + j:n_top + j + 1, :], gate)
        takes = jnp.dot(picks, rank, preferred_element_type=F32) == targets
        parts = [jnp.dot(picks, part, preferred_element_type=F32) for part in split3(gate)]
        return split3(jnp.where(takes, parts[0] + parts[1] + parts[2], 0.0).T)

    def mix_first_hop():
        @pl.loop(0, 4)
        def _(i):
            d, j = i // 2, i % 2
            info = metas[core, ring(z + (1 - 2 * d) * (half - 1 - j))]
            for n, part in enumerate(mixing(info, ranks(info), pick_up[d], target_up[d])):
                mix_up[d, j, n * n_tok:(n + 1) * n_tok, :] = part

    def place_rows(which, pos):
        info = metas[which, pos]
        rank = ranks(info)
        takes = jnp.dot(pick[:rows, :], rank, preferred_element_type=F32) == target[:rows, :]
        onehot = jnp.where(takes, 1.0, 0.0).astype(BF16)
        for c in range(RS_CHUNKS):
            cols = pl.ds(c * rs_cols, rs_cols)
            got = jnp.dot(onehot, toks[which, pos, :, cols], preferred_element_type=F32).astype(BF16)
            x_buf[:, which, pos, :, cols] = got.reshape(n_slot, cap, rs_cols)

        @pl.when(core == which)
        def _():
            for n, part in enumerate(mixing(info, rank, pick[...], target[...])):
                mix[pos, n * n_tok:(n + 1) * n_tok, :] = part

    def start_gather():
        for c in range(AG_CHUNKS):
            for d in range(2):
                ag_copy(d, 1, chunk_order(d)[c]).start()
        for c in range(AG_CHUNKS):
            sib_copy(0, 0, c, core).start()

    def pass_on(hop, n):
        for d in range(2):
            if n < len(carried(d, hop)):
                c = carried(d, hop)[n]
                ag_arrival(d, hop, c).wait_recv()
                if hop < half and c in carried(d, hop + 1):
                    ag_copy(d, hop + 1, c).start()
                sib_copy(d, hop, c, core).start()

    def from_sibling(hop):
        if hop == 0:
            for c in range(AG_CHUNKS):
                sib_copy(0, 0, c, other).wait_recv()
            return
        for d in range(2):
            for c in carried(d, hop):
                sib_copy(d, hop, c, other).wait_recv()

    def place_hop(which, hop):
        @pl.loop(0, 1 if hop in (0, half) else 2)
        def _(d):
            place_rows(which, ring(z - (1 - 2 * d) * hop))

    def meta_from_sibling(hop):
        for d in range(2):
            if (hop == 0 and d == 0) or (hop > 0 and meta_carried(d, hop)):
                meta_sib(d, hop, other).wait_recv()

    for hop in range(half + 1):
        if hop > 0:
            for d in range(2):
                if meta_carried(d, hop):
                    meta_copy(d, hop, 1).wait_recv()
                    if hop < half and meta_carried(d, hop + 1):
                        meta_copy(d, hop + 1, 0).start()
                    meta_sib(d, hop, core).start()

        @pl.when(core == 0)
        def _():
            if hop > 0:
                for n in range(len(carried(0, hop))):
                    pass_on(hop, n)

        @pl.when(core == 1)
        def _():
            meta_from_sibling(hop)
            from_sibling(hop)
            if hop == AG2_HOP:
                start_gather()

        place_hop(0, hop)
        if hop == half - 1:
            @pl.when(core == 0)
            def _():
                mix_first_hop()

    def o_copy(slot):
        return remote(x_buf.at[slot, other], o_sib.at[slot], o_send.at[slot], o_recv.at[slot], device(z, other))

    def experts(slot, batch):
        step = batch * n_slot + slot
        buf = step % W_DEPTH
        for copy in weight_copies(step):
            copy.wait()
        x = x_buf[slot, batch].reshape(nz * cap, d_model)
        hidden = jax.nn.gelu(jnp.dot(x, up_buf[buf], preferred_element_type=F32), approximate=True).astype(BF16)
        for c in range(RS_CHUNKS):
            cols = pl.ds(c * rs_cols, rs_cols)
            o = jnp.dot(hidden, down_buf[buf, :, cols], preferred_element_type=F32).astype(BF16)
            x_buf[slot, batch, :, :, cols] = o.reshape(nz, cap, rs_cols)

        @pl.when(core != batch)
        def _():
            o_copy(slot).start()

        @pl.when(step + W_DEPTH < 2 * n_slot)
        def _():
            for copy in weight_copies(step + W_DEPTH):
                copy.start()

    @pl.loop(0, n_slot)
    def _(slot):
        experts(slot, 0)
        for after, hop, n in AG2_STEPS:
            @pl.when((core == 1) & (slot == after))
            def _():
                pass_on(hop, n)

    def from_sibling_o():
        @pl.loop(0, n_slot)
        def _(slot):
            o_copy(slot).wait_recv()

    def chip_rows(pos, c):
        cols = pl.ds(pl.multiple_of(c * rs_cols, rs_cols), rs_cols)
        parts = [x_buf[:, core, pos, :, cols].reshape(rows, rs_cols), o_sib[:, pos, :, cols].reshape(rows, rs_cols)]
        if k_pad > 2 * rows:
            parts.append(jnp.zeros((k_pad - 2 * rows, rs_cols), BF16))
        return jnp.concatenate(parts, axis=0)

    def mixed(weights, values):
        total = jnp.dot(weights, values, preferred_element_type=F32)
        return total[:n_tok] + total[n_tok:2 * n_tok] + total[2 * n_tok:]

    def own_sum(pos, c):
        return mixed(mix[pos], chip_rows(pos, c))

    skip = RS_CHUNKS // 2
    first = skip + RS_CHUNKS
    items = half * RS_CHUNKS

    def rs_chunk(d, n):
        c = n % RS_CHUNKS
        return (c + skip) % RS_CHUNKS if d == 0 else c

    def rs_dest(d, n):
        return ring(z + (1 - 2 * d) * (half - n // RS_CHUNKS))

    def first_copy(d, n):
        return remote(first_out.at[d, n - skip], first_in.at[d, n - skip], rs_send.at[d, n],
                      rs_recv.at[d, n + RS_CHUNKS], device(ring(z + (1 - 2 * d)), core))

    def first_arrival(d, n):
        return remote(first_out.at[d, n - first], first_in.at[d, n - first], rs_send.at[d, n],
                      rs_recv.at[d, n], device(ring(z + (1 - 2 * d)), core))

    def rs_copy(d, n):
        return remote(rs_buf.at[d, n - first], rs_buf.at[d, n - first + RS_CHUNKS], rs_send.at[d, n],
                      rs_recv.at[d, n + RS_CHUNKS], device(ring(z + (1 - 2 * d)), core))

    def rs_arrival(d, n):
        return remote(rs_buf.at[d, n - first], rs_buf.at[d, n - first], rs_send.at[d, n], rs_recv.at[d, n],
                      device(ring(z + (1 - 2 * d)), core))

    def first_item(n):
        for d in range(2):
            got = jnp.dot(pack[:packed, :], chip_rows(rs_dest(d, n), rs_chunk(d, n)), preferred_element_type=F32)
            first_out[d, n - skip] = got.astype(BF16)
            first_copy(d, n).start()

    def second_item(n):
        for d in range(2):
            value = own_sum(rs_dest(d, n), rs_chunk(d, n))
            first_arrival(d, n).wait_recv()
            rows_in = first_in[d, n - first]
            if packed_pad > packed:
                rows_in = jnp.concatenate([rows_in, jnp.zeros((packed_pad - packed, rs_cols), BF16)], axis=0)
            rs_buf[d, n - first] = value + mixed(mix_up[d, (n - first) // skip], rows_in)
            rs_copy(d, n).start()

    def later_item(n):
        for d in range(2):
            value = own_sum(rs_dest(d, n), rs_chunk(d, n))
            rs_arrival(d, n).wait_recv()
            rs_buf[d, n - first] += value
            rs_copy(d, n).start()

    def start_chains():
        from_sibling_o()
        pl.loop(skip, first)(first_item)

    @pl.when(core == 0)
    def _():
        start_chains()

    @pl.when(core == 1)
    def _():
        for n in range(len(carried(0, half))):
            pass_on(half, n)

    for hop in range(half + 1):
        @pl.when(core == 0)
        def _():
            meta_from_sibling(hop)
            from_sibling(hop)

        place_hop(1, hop)

    @pl.loop(0, n_slot)
    def _(slot):
        experts(slot, 1)

        @pl.when((core == 0) & (slot < RS_CHUNKS))
        def _():
            second_item(first + slot)

        @pl.when((core == 0) & (slot >= RS_CHUNKS))
        def _():
            later_item(first + slot)

    @pl.when(core == 1)
    def _():
        mix_first_hop()
        start_chains()
        pl.loop(first, first + RS_CHUNKS)(second_item)

    pl.loop(jnp.where(core == 0, first + n_slot, first + RS_CHUNKS), items)(later_item)

    for c in range(RS_CHUNKS):
        total_buf[c] = own_sum(z, c)
    for i in range(RS_CHUNKS):
        for d in range(2):
            rs_arrival(d, items + i).wait_recv()
        if i >= skip:
            for c in (i - skip, i):
                value = total_buf[c]
                for d in range(2):
                    value += rs_buf[d, items - first + ((c + skip) % RS_CHUNKS if d == 0 else c)]
                out_ref[:, c * rs_cols:(c + 1) * rs_cols] = value.astype(BF16)

    for d in range(2):
        for hop in range(1, half + 1):
            if meta_carried(d, hop):
                meta_copy(d, hop, 0).wait_send()
                meta_sib(d, hop, core).wait_send()
            for c in carried(d, hop):
                ag_copy(d, hop, c).wait_send()
                sib_copy(d, hop, c, core).wait_send()
    meta_sib(0, 0, core).wait_send()
    for c in range(AG_CHUNKS):
        sib_copy(0, 0, c, core).wait_send()

    @pl.loop(0, n_slot)
    def _(slot):
        o_copy(slot).wait_send()

    @pl.loop(skip, first)
    def _(n):
        for d in range(2):
            first_copy(d, n).wait_send()

    @pl.loop(first, items)
    def _(n):
        for d in range(2):
            rs_copy(d, n).wait_send()


def solution(mesh):
    n_dev = mesh.shape["ep"]
    nz = n_dev // CORES
    half = nz // 2

    def group_layer(tokens, topk_idx, topk_w, w_up, w_down, slot_expert):
        n_tok, d_model = tokens.shape
        n_top = topk_idx.shape[1]
        n_slot = slot_expert.shape[1]
        n_exp = n_dev * (n_slot - 1)
        d_ff = w_up.shape[3]
        bound = slot_bound(n_tok, n_top, n_dev, n_slot)
        cap = round_up(bound, 16)
        k_pad = round_up(2 * n_slot * cap, 128)
        packed = 2 * round_up(n_slot * bound, 8)
        packed_pad = round_up(packed, 128)
        rs_cols = d_model // RS_CHUNKS
        skip = RS_CHUNKS // 2
        dma = pltpu.SemaphoreType.DMA
        any_space = pl.BlockSpec(memory_space=pl.ANY)
        vmem = pl.BlockSpec(memory_space=pltpu.VMEM)
        return pl.pallas_call(
            functools.partial(layer_kernel, nz, bound),
            out_shape=jax.ShapeDtypeStruct((n_tok, d_model), BF16),
            in_specs=[any_space, any_space, any_space, pl.BlockSpec(memory_space=pltpu.SMEM), vmem, any_space, any_space],
            out_specs=vmem,
            scratch_shapes=[
                pltpu.VMEM((CORES, nz, n_tok, d_model), BF16),
                pltpu.VMEM((n_top, n_tok), jnp.int32),
                pltpu.VMEM((CORES, nz, 2 * n_top, n_tok), F32),
                pltpu.VMEM((n_slot, CORES, nz, cap, d_model), BF16),
                pltpu.VMEM((n_slot, nz, cap, d_model), BF16),
                pltpu.VMEM((W_DEPTH, d_model, d_ff), BF16),
                pltpu.VMEM((W_DEPTH, d_ff, d_model), BF16),
                pltpu.VMEM((2, half * RS_CHUNKS - skip, n_tok, rs_cols), F32),
                pltpu.VMEM((2, RS_CHUNKS, packed, rs_cols), BF16),
                pltpu.VMEM((2, RS_CHUNKS, packed, rs_cols), BF16),
                pltpu.VMEM((RS_CHUNKS, n_tok, rs_cols), F32),
                pltpu.VMEM((nz, 3 * n_tok, k_pad), BF16),
                pltpu.VMEM((2, 2, 3 * n_tok, packed_pad), BF16),
                pltpu.VMEM((k_pad, n_exp), BF16),
                pltpu.VMEM((k_pad, n_exp), F32),
                pltpu.VMEM((2, packed_pad, n_exp), BF16),
                pltpu.VMEM((2, packed_pad, n_exp), F32),
                pltpu.VMEM((packed_pad, k_pad), BF16),
                dma((3,)),
                dma((2, half, AG_CHUNKS)), dma((2, half, AG_CHUNKS)),
                dma((2, half + 1, AG_CHUNKS)), dma((2, half + 1, AG_CHUNKS)),
                dma((2, half)), dma((2, half)),
                dma((2, half + 1)), dma((2, half + 1)),
                dma((2, W_DEPTH)),
                dma((n_slot,)), dma((n_slot,)),
                dma((2, half * RS_CHUNKS)), dma((2, (half + 1) * RS_CHUNKS)),
            ],
            compiler_params=pltpu.CompilerParams(collective_id=0, has_side_effects=True,
                                                 vmem_limit_bytes=62 * 1024 * 1024),
        )(tokens, topk_idx.T, topk_w.T, slot_expert, slot_expert, w_up, w_down)

    row_spec = P(("dp", "ep"), None)
    weight_spec = P("ep", None, None, None)
    return jax.shard_map(group_layer, mesh=mesh,
                         in_specs=(row_spec, row_spec, row_spec, weight_spec, weight_spec, P(None, None)),
                         out_specs=row_spec, check_vma=False)
```

```python
import functools

import jax
import jax.numpy as jnp
from jax import lax
from jax.experimental import pallas as pl
from jax.experimental.pallas import tpu as pltpu
from jax.sharding import PartitionSpec as P

MESH = pl.DeviceIdType.MESH
F32 = jnp.float32
BF16 = jnp.bfloat16
CORES = 2
W_DEPTH = 4
AG_CHUNKS = 4
RS_CHUNKS = 4
AG2_LATE = (((3, 0), (3, 1)), ((3, 2), (3, 3)), ((4, 0), (4, 1)), (), ())
AG2_HOP = 3


def slot_bound(n_tok, n_top, n_dev, n_slot):
    base_load = (n_tok * n_top) // (n_dev * n_slot)
    return base_load + base_load // 2 + 1


def round_up(n, unit):
    return -(-n // unit) * unit


def split3(x):
    hi = x.astype(BF16)
    rest = x - hi.astype(F32)
    mid = rest.astype(BF16)
    low = (rest - mid.astype(F32)).astype(BF16)
    return hi, mid, low


def layer_kernel(nz, bound, tok_hbm, idx_hbm, gate_hbm, slot_hbm, up_hbm, down_hbm, out_ref,
                 toks, idx_own, slot_smem, slot_vmem, metas, x_buf, o_sib, up_buf, down_buf, rs_buf, first_out, first_in, total_buf,
                 mix, mix_up, pick, target, pick_up, target_up, pack,
                 in_sem, ag_send, ag_recv, sib_send, sib_recv, ms_send, ms_recv, mb_send, mb_recv,
                 w_sem, o_send, o_recv, rs_send, rs_recv):
    half = nz // 2
    n_tok, d_model = tok_hbm.shape
    n_top = idx_hbm.shape[0]
    n_slot, cap = x_buf.shape[0], x_buf.shape[3]
    rows = n_slot * cap
    k_pad, n_exp = pick.shape
    packed, packed_pad = first_out.shape[2], pack.shape[0]
    ag_rows = n_tok // AG_CHUNKS
    rs_cols = d_model // RS_CHUNKS

    me = lax.axis_index("ep")
    z = me // CORES
    core = me % CORES
    other = 1 - core

    def ring(pos):
        return (pos + nz) % nz

    def device(pos, which):
        return {"ep": pos * CORES + which}

    def remote(src, dst, send, recv, dev):
        return pltpu.make_async_remote_copy(src_ref=src, dst_ref=dst, send_sem=send, recv_sem=recv,
                                            device_id=dev, device_id_type=MESH)

    def weight_copies(step):
        buf, slot = step % W_DEPTH, step % n_slot
        return (pltpu.make_async_copy(up_hbm.at[0, slot], up_buf.at[buf], w_sem.at[0, buf]),
                pltpu.make_async_copy(down_hbm.at[0, slot], down_buf.at[buf], w_sem.at[1, buf]))

    own_tok = pltpu.make_async_copy(tok_hbm, toks.at[core, z], in_sem.at[0])
    own_idx = pltpu.make_async_copy(idx_hbm, idx_own, in_sem.at[1])
    own_gate = pltpu.make_async_copy(gate_hbm, metas.at[core, z, n_top:], in_sem.at[2])
    tables = [pltpu.make_async_copy(slot_hbm, ref, in_sem.at[3 + n]) for n, ref in enumerate((slot_smem, slot_vmem))]
    own_tok.start()
    own_idx.start()
    own_gate.start()
    for copy in tables:
        copy.start()
    barrier = pltpu.get_barrier_semaphore()
    pl.semaphore_signal(barrier, inc=1, device_id=device(ring(z + 1), core), device_id_type=MESH)
    pl.semaphore_signal(barrier, inc=1, device_id=device(ring(z - 1), core), device_id_type=MESH)
    pl.semaphore_signal(barrier, inc=1, device_id=device(z, other), device_id_type=MESH)
    own_idx.wait()
    metas[core, z, :n_top, :] = idx_own[...].astype(F32)
    own_gate.wait()
    own_tok.wait()
    pl.semaphore_wait(barrier, 3)

    def ag_copy(d, hop, c):
        sign = 1 - 2 * d
        ref = toks.at[core, ring(z - sign * (hop - 1)), pl.ds(c * ag_rows, ag_rows)]
        return remote(ref, ref, ag_send.at[d, hop - 1, c], ag_recv.at[d, hop - 1, c], device(ring(z + sign), core))

    def ag_arrival(d, hop, c):
        sign = 1 - 2 * d
        ref = toks.at[core, ring(z - sign * hop), pl.ds(c * ag_rows, ag_rows)]
        return remote(ref, ref, ag_send.at[d, hop - 1, c], ag_recv.at[d, hop - 1, c], device(ring(z + sign), core))

    def sib_copy(d, hop, c, which):
        sign = 1 - 2 * d
        ref = toks.at[which, ring(z - sign * hop), pl.ds(c * ag_rows, ag_rows)]
        return remote(ref, ref, sib_send.at[d, hop, c], sib_recv.at[d, hop, c], device(z, other))

    def meta_copy(d, hop, back):
        sign = 1 - 2 * d
        ref = metas.at[core, ring(z - sign * (hop - 1 + back))]
        return remote(ref, ref, ms_send.at[d, hop - 1], ms_recv.at[d, hop - 1], device(ring(z + sign), core))

    def meta_sib(d, hop, which):
        sign = 1 - 2 * d
        ref = metas.at[which, ring(z - sign * hop)]
        return remote(ref, ref, mb_send.at[d, hop], mb_recv.at[d, hop], device(z, other))

    def chunk_order(d):
        return list(range(AG_CHUNKS)) if d == 0 else list(range(AG_CHUNKS))[::-1]

    def carried(d, hop):
        order = chunk_order(d)
        return order if hop < half else order[:AG_CHUNKS // 2]

    def meta_carried(d, hop):
        return hop < half or d == 0

    for d in range(2):
        meta_copy(d, 1, 0).start()
    meta_sib(0, 0, core).start()

    @pl.when(core == 0)
    def _():
        for c in range(AG_CHUNKS):
            for d in range(2):
                ag_copy(d, 1, chunk_order(d)[c]).start()
        for c in range(AG_CHUNKS):
            sib_copy(0, 0, c, core).start()

    for step in range(W_DEPTH):
        for copy in weight_copies(step):
            copy.start()

    lane = lax.broadcasted_iota(jnp.int32, (cap, n_exp), 1)
    row = lax.broadcasted_iota(jnp.int32, (cap, n_exp), 0).astype(F32)
    for copy in tables:
        copy.wait()
    table = slot_vmem[...]
    place = lax.broadcasted_iota(jnp.int32, table.shape, 0) * n_slot + lax.broadcasted_iota(jnp.int32, table.shape, 1)
    if k_pad > 2 * rows:
        pick[2 * rows:, :] = jnp.zeros((k_pad - 2 * rows, n_exp), BF16)
        target[2 * rows:, :] = jnp.full((k_pad - 2 * rows, n_exp), -1.0, F32)

    def slot_rows(pos):
        for w in range(2):
            dev = pos * CORES + (core if w == 0 else other)
            for s in range(n_slot):
                exp_id = slot_smem[dev, s]
                same = table == exp_id
                copies = jnp.sum(jnp.where(same, 1.0, 0.0))
                earlier = jnp.sum(jnp.where(same & (place < dev * n_slot + s), 1.0, 0.0))
                at = pl.ds(w * rows + s * cap, cap)
                pick[at, :] = jnp.where(lane == exp_id, 1.0, 0.0).astype(BF16)
                target[at, :] = row * copies + earlier

    column = lax.broadcasted_iota(jnp.int32, (packed_pad, k_pad), 1)
    side = jnp.where(column >= rows, 1, 0)
    in_side = column - side * rows
    in_slot = in_side % cap
    packed_row = side * (packed // 2) + (in_side // cap) * bound + in_slot
    used = (in_slot < bound) & (column < 2 * rows)
    pack[...] = jnp.where(used & (lax.broadcasted_iota(jnp.int32, (packed_pad, k_pad), 0) == packed_row),
                          1.0, 0.0).astype(BF16)
    for d in range(2):
        slot_rows(ring(z - (1 - 2 * d)))
        pick_up[d] = jnp.dot(pack[...], pick[...], preferred_element_type=F32).astype(BF16)
        target_up[d] = jnp.dot(pack[...], (target[...] + 1.0).astype(BF16), preferred_element_type=F32) - 1.0
    slot_rows(z)

    exp_iota = lax.broadcasted_iota(jnp.int32, (n_exp, n_tok), 0).astype(F32)

    def ranks(info):
        chosen = jnp.zeros((n_exp, n_tok), F32)
        for j in range(n_top):
            chosen = jnp.where(exp_iota == info[j:j + 1, :], 1.0, chosen)
        before = (lax.broadcasted_iota(jnp.int32, (n_tok, n_tok), 0)
                  < lax.broadcasted_iota(jnp.int32, (n_tok, n_tok), 1))
        rank = jnp.dot(chosen.astype(BF16), jnp.where(before, 1.0, 0.0).astype(BF16), preferred_element_type=F32)
        return jnp.where(chosen > 0.5, rank, -1.0).astype(BF16)

    def mixing(info, rank, picks, targets):
        gate = jnp.zeros((n_exp, n_tok), F32)
        for j in range(n_top):
            gate = jnp.where(exp_iota == info[j:j + 1, :], info[n_top + j:n_top + j + 1, :], gate)
        takes = jnp.dot(picks, rank, preferred_element_type=F32) == targets
        parts = [jnp.dot(picks, part, preferred_element_type=F32) for part in split3(gate)]
        return split3(jnp.where(takes, parts[0] + parts[1] + parts[2], 0.0).T)

    def mix_first_hop():
        @pl.loop(0, 4)
        def _(i):
            d, j = i // 2, i % 2
            info = metas[core, ring(z + (1 - 2 * d) * (half - 1 - j))]
            for n, part in enumerate(mixing(info, ranks(info), pick_up[d], target_up[d])):
                mix_up[d, j, n * n_tok:(n + 1) * n_tok, :] = part

    def place_rows(which, pos):
        info = metas[which, pos]
        rank = ranks(info)
        takes = jnp.dot(pick[:rows, :], rank, preferred_element_type=F32) == target[:rows, :]
        onehot = jnp.where(takes, 1.0, 0.0).astype(BF16)
        for c in range(RS_CHUNKS):
            cols = pl.ds(c * rs_cols, rs_cols)
            got = jnp.dot(onehot, toks[which, pos, :, cols], preferred_element_type=F32).astype(BF16)
            x_buf[:, which, pos, :, cols] = got.reshape(n_slot, cap, rs_cols)

        @pl.when(core == which)
        def _():
            for n, part in enumerate(mixing(info, rank, pick[...], target[...])):
                mix[pos, n * n_tok:(n + 1) * n_tok, :] = part

    def start_gather():
        for c in range(AG_CHUNKS):
            for d in range(2):
                ag_copy(d, 1, chunk_order(d)[c]).start()
        for c in range(AG_CHUNKS):
            sib_copy(0, 0, c, core).start()

    def pass_on(hop, n):
        for d in range(2):
            if n < len(carried(d, hop)):
                c = carried(d, hop)[n]
                ag_arrival(d, hop, c).wait_recv()
                if hop < half and c in carried(d, hop + 1):
                    ag_copy(d, hop + 1, c).start()
                sib_copy(d, hop, c, core).start()

    def from_sibling(hop):
        if hop == 0:
            for c in range(AG_CHUNKS):
                sib_copy(0, 0, c, other).wait_recv()
            return
        for d in range(2):
            for c in carried(d, hop):
                sib_copy(d, hop, c, other).wait_recv()

    def place_hop(which, hop):
        @pl.loop(0, 1 if hop in (0, half) else 2)
        def _(d):
            place_rows(which, ring(z - (1 - 2 * d) * hop))

    def meta_from_sibling(hop):
        for d in range(2):
            if (hop == 0 and d == 0) or (hop > 0 and meta_carried(d, hop)):
                meta_sib(d, hop, other).wait_recv()

    for hop in range(half + 1):
        if hop > 0:
            for d in range(2):
                if meta_carried(d, hop):
                    meta_copy(d, hop, 1).wait_recv()
                    if hop < half and meta_carried(d, hop + 1):
                        meta_copy(d, hop + 1, 0).start()
                    meta_sib(d, hop, core).start()

        @pl.when(core == 0)
        def _():
            if hop > 0:
                for n in range(len(carried(0, hop))):
                    pass_on(hop, n)

        @pl.when(core == 1)
        def _():
            meta_from_sibling(hop)
            from_sibling(hop)
            if hop == AG2_HOP:
                start_gather()

        place_hop(0, hop)
        if hop == half - 1:
            @pl.when(core == 0)
            def _():
                mix_first_hop()

    def o_copy(slot):
        return remote(x_buf.at[slot, other], o_sib.at[slot], o_send.at[slot], o_recv.at[slot], device(z, other))

    def experts(slot, batch):
        step = batch * n_slot + slot
        buf = step % W_DEPTH
        for copy in weight_copies(step):
            copy.wait()
        x = x_buf[slot, batch].reshape(nz * cap, d_model)
        hidden = jax.nn.gelu(jnp.dot(x, up_buf[buf], preferred_element_type=F32), approximate=True).astype(BF16)
        for c in range(RS_CHUNKS):
            cols = pl.ds(c * rs_cols, rs_cols)
            o = jnp.dot(hidden, down_buf[buf, :, cols], preferred_element_type=F32).astype(BF16)
            x_buf[slot, batch, :, :, cols] = o.reshape(nz, cap, rs_cols)

        @pl.when(core != batch)
        def _():
            o_copy(slot).start()

        @pl.when(step + W_DEPTH < 2 * n_slot)
        def _():
            for copy in weight_copies(step + W_DEPTH):
                copy.start()

    @pl.loop(0, n_slot)
    def _(slot):
        experts(slot, 0)

        @pl.when((core == 1) & (slot < 2 * AG_CHUNKS))
        def _():
            hop, n = 1 + slot // AG_CHUNKS, slot % AG_CHUNKS
            for d in range(2):
                c = n if d == 0 else AG_CHUNKS - 1 - n
                ag_arrival(d, hop, c).wait_recv()
                ag_copy(d, hop + 1, c).start()
                sib_copy(d, hop, c, core).start()

    def from_sibling_o():
        @pl.loop(0, n_slot)
        def _(slot):
            o_copy(slot).wait_recv()

    def chip_rows(pos, c):
        cols = pl.ds(pl.multiple_of(c * rs_cols, rs_cols), rs_cols)
        parts = [x_buf[:, core, pos, :, cols].reshape(rows, rs_cols), o_sib[:, pos, :, cols].reshape(rows, rs_cols)]
        if k_pad > 2 * rows:
            parts.append(jnp.zeros((k_pad - 2 * rows, rs_cols), BF16))
        return jnp.concatenate(parts, axis=0)

    def mixed(weights, values):
        total = jnp.dot(weights, values, preferred_element_type=F32)
        return total[:n_tok] + total[n_tok:2 * n_tok] + total[2 * n_tok:]

    def own_sum(pos, c):
        return mixed(mix[pos], chip_rows(pos, c))

    skip = RS_CHUNKS // 2
    first = skip + RS_CHUNKS
    items = half * RS_CHUNKS

    def rs_chunk(d, n):
        c = n % RS_CHUNKS
        return (c + skip) % RS_CHUNKS if d == 0 else c

    def rs_dest(d, n):
        return ring(z + (1 - 2 * d) * (half - n // RS_CHUNKS))

    def first_copy(d, n):
        return remote(first_out.at[d, n - skip], first_in.at[d, n - skip], rs_send.at[d, n],
                      rs_recv.at[d, n + RS_CHUNKS], device(ring(z + (1 - 2 * d)), core))

    def first_arrival(d, n):
        return remote(first_out.at[d, n - first], first_in.at[d, n - first], rs_send.at[d, n],
                      rs_recv.at[d, n], device(ring(z + (1 - 2 * d)), core))

    def rs_copy(d, n):
        return remote(rs_buf.at[d, n - first], rs_buf.at[d, n - first + RS_CHUNKS], rs_send.at[d, n],
                      rs_recv.at[d, n + RS_CHUNKS], device(ring(z + (1 - 2 * d)), core))

    def rs_arrival(d, n):
        return remote(rs_buf.at[d, n - first], rs_buf.at[d, n - first], rs_send.at[d, n], rs_recv.at[d, n],
                      device(ring(z + (1 - 2 * d)), core))

    def first_item(n):
        for d in range(2):
            got = jnp.dot(pack[:packed, :], chip_rows(rs_dest(d, n), rs_chunk(d, n)), preferred_element_type=F32)
            first_out[d, n - skip] = got.astype(BF16)
            first_copy(d, n).start()

    def second_item(n):
        for d in range(2):
            value = own_sum(rs_dest(d, n), rs_chunk(d, n))
            first_arrival(d, n).wait_recv()
            rows_in = first_in[d, n - first]
            if packed_pad > packed:
                rows_in = jnp.concatenate([rows_in, jnp.zeros((packed_pad - packed, rs_cols), BF16)], axis=0)
            rs_buf[d, n - first] = value + mixed(mix_up[d, (n - first) // skip], rows_in)
            rs_copy(d, n).start()

    def later_item(n):
        for d in range(2):
            value = own_sum(rs_dest(d, n), rs_chunk(d, n))
            rs_arrival(d, n).wait_recv()
            rs_buf[d, n - first] += value
            rs_copy(d, n).start()

    def start_chains():
        from_sibling_o()
        pl.loop(skip, first)(first_item)

    @pl.when(core == 0)
    def _():
        start_chains()

    for hop in range(half + 1):
        @pl.when(core == 0)
        def _():
            meta_from_sibling(hop)
            from_sibling(hop)

        @pl.when(core == 1)
        def _():
            for late, n in AG2_LATE[hop]:
                pass_on(late, n)

        place_hop(1, hop)

    @pl.loop(0, n_slot)
    def _(slot):
        experts(slot, 1)

        @pl.when((core == 0) & (slot < RS_CHUNKS))
        def _():
            second_item(first + slot)

        @pl.when((core == 0) & (slot >= RS_CHUNKS))
        def _():
            later_item(first + slot)

    @pl.when(core == 1)
    def _():
        mix_first_hop()
        start_chains()
        pl.loop(first, first + RS_CHUNKS)(second_item)

    pl.loop(jnp.where(core == 0, first + n_slot, first + RS_CHUNKS), items)(later_item)

    for c in range(RS_CHUNKS):
        total_buf[c] = own_sum(z, c)
    for i in range(RS_CHUNKS):
        for d in range(2):
            rs_arrival(d, items + i).wait_recv()
        if i >= skip:
            for c in (i - skip, i):
                value = total_buf[c]
                for d in range(2):
                    value += rs_buf[d, items - first + ((c + skip) % RS_CHUNKS if d == 0 else c)]
                out_ref[:, c * rs_cols:(c + 1) * rs_cols] = value.astype(BF16)

    for d in range(2):
        for hop in range(1, half + 1):
            if meta_carried(d, hop):
                meta_copy(d, hop, 0).wait_send()
                meta_sib(d, hop, core).wait_send()
            for c in carried(d, hop):
                ag_copy(d, hop, c).wait_send()
                sib_copy(d, hop, c, core).wait_send()
    meta_sib(0, 0, core).wait_send()
    for c in range(AG_CHUNKS):
        sib_copy(0, 0, c, core).wait_send()

    @pl.loop(0, n_slot)
    def _(slot):
        o_copy(slot).wait_send()

    @pl.loop(skip, first)
    def _(n):
        for d in range(2):
            first_copy(d, n).wait_send()

    @pl.loop(first, items)
    def _(n):
        for d in range(2):
            rs_copy(d, n).wait_send()


def solution(mesh):
    n_dev = mesh.shape["ep"]
    nz = n_dev // CORES
    half = nz // 2

    def group_layer(tokens, topk_idx, topk_w, w_up, w_down, slot_expert):
        n_tok, d_model = tokens.shape
        n_top = topk_idx.shape[1]
        n_slot = slot_expert.shape[1]
        n_exp = n_dev * (n_slot - 1)
        d_ff = w_up.shape[3]
        bound = slot_bound(n_tok, n_top, n_dev, n_slot)
        cap = round_up(bound, 16)
        k_pad = round_up(2 * n_slot * cap, 128)
        packed = 2 * round_up(n_slot * bound, 8)
        packed_pad = round_up(packed, 128)
        rs_cols = d_model // RS_CHUNKS
        skip = RS_CHUNKS // 2
        dma = pltpu.SemaphoreType.DMA
        any_space = pl.BlockSpec(memory_space=pl.ANY)
        vmem = pl.BlockSpec(memory_space=pltpu.VMEM)
        return pl.pallas_call(
            functools.partial(layer_kernel, nz, bound),
            out_shape=jax.ShapeDtypeStruct((n_tok, d_model), BF16),
            in_specs=[any_space] * 6,
            out_specs=vmem,
            scratch_shapes=[
                pltpu.VMEM((CORES, nz, n_tok, d_model), BF16),
                pltpu.VMEM((n_top, n_tok), jnp.int32),
                pltpu.SMEM(slot_expert.shape, jnp.int32),
                pltpu.VMEM(slot_expert.shape, jnp.int32),
                pltpu.VMEM((CORES, nz, 2 * n_top, n_tok), F32),
                pltpu.VMEM((n_slot, CORES, nz, cap, d_model), BF16),
                pltpu.VMEM((n_slot, nz, cap, d_model), BF16),
                pltpu.VMEM((W_DEPTH, d_model, d_ff), BF16),
                pltpu.VMEM((W_DEPTH, d_ff, d_model), BF16),
                pltpu.VMEM((2, half * RS_CHUNKS - skip, n_tok, rs_cols), F32),
                pltpu.VMEM((2, RS_CHUNKS, packed, rs_cols), BF16),
                pltpu.VMEM((2, RS_CHUNKS, packed, rs_cols), BF16),
                pltpu.VMEM((RS_CHUNKS, n_tok, rs_cols), F32),
                pltpu.VMEM((nz, 3 * n_tok, k_pad), BF16),
                pltpu.VMEM((2, 2, 3 * n_tok, packed_pad), BF16),
                pltpu.VMEM((k_pad, n_exp), BF16),
                pltpu.VMEM((k_pad, n_exp), F32),
                pltpu.VMEM((2, packed_pad, n_exp), BF16),
                pltpu.VMEM((2, packed_pad, n_exp), F32),
                pltpu.VMEM((packed_pad, k_pad), BF16),
                dma((5,)),
                dma((2, half, AG_CHUNKS)), dma((2, half, AG_CHUNKS)),
                dma((2, half + 1, AG_CHUNKS)), dma((2, half + 1, AG_CHUNKS)),
                dma((2, half)), dma((2, half)),
                dma((2, half + 1)), dma((2, half + 1)),
                dma((2, W_DEPTH)),
                dma((n_slot,)), dma((n_slot,)),
                dma((2, half * RS_CHUNKS)), dma((2, (half + 1) * RS_CHUNKS)),
            ],
            compiler_params=pltpu.CompilerParams(collective_id=0, has_side_effects=True,
                                                 vmem_limit_bytes=67043328),
        )(tokens, topk_idx.T, topk_w.T, slot_expert, w_up, w_down)

    row_spec = P(("dp", "ep"), None)
    weight_spec = P("ep", None, None, None)
    return jax.shard_map(group_layer, mesh=mesh,
                         in_specs=(row_spec, row_spec, row_spec, weight_spec, weight_spec, P(None, None)),
                         out_specs=row_spec, check_vma=False)
```

```python
import functools

import jax
import jax.numpy as jnp
from jax import lax
from jax.experimental import pallas as pl
from jax.experimental.pallas import tpu as pltpu
from jax.sharding import PartitionSpec as P

MESH = pl.DeviceIdType.MESH
F32 = jnp.float32
BF16 = jnp.bfloat16
CORES = 2
W_DEPTH = 4
AG_CHUNKS = 4
RS_CHUNKS = 4
AG2_LATE = (((3, 0), (3, 1)), ((3, 2), (3, 3)), ((4, 0), (4, 1)), (), ())
AG2_HOP = 3


def slot_bound(n_tok, n_top, n_dev, n_slot):
    base_load = (n_tok * n_top) // (n_dev * n_slot)
    return base_load + base_load // 2 + 1


def round_up(n, unit):
    return -(-n // unit) * unit


def split3(x):
    hi = x.astype(BF16)
    rest = x - hi.astype(F32)
    mid = rest.astype(BF16)
    low = (rest - mid.astype(F32)).astype(BF16)
    return hi, mid, low


def layer_kernel(nz, bound, tok_hbm, idx_hbm, gate_hbm, slot_hbm, up_hbm, down_hbm, out_ref,
                 toks, idx_own, slot_smem, slot_vmem, metas, x_buf, o_sib, up_buf, down_buf, rs_buf, first_out, first_in, total_buf,
                 mix, mix_up, pick, target, pick_up, target_up, pack,
                 in_sem, ag_send, ag_recv, sib_send, sib_recv, ms_send, ms_recv, mb_send, mb_recv,
                 w_sem, o_send, o_recv, rs_send, rs_recv):
    half = nz // 2
    n_tok, d_model = tok_hbm.shape
    n_top = idx_hbm.shape[0]
    n_slot, cap = x_buf.shape[0], x_buf.shape[3]
    rows = n_slot * cap
    k_pad, n_exp = pick.shape
    packed, packed_pad = first_out.shape[2], pack.shape[0]
    ag_rows = n_tok // AG_CHUNKS
    rs_cols = d_model // RS_CHUNKS

    me = lax.axis_index("ep")
    z = me // CORES
    core = me % CORES
    other = 1 - core

    def ring(pos):
        return (pos + nz) % nz

    def device(pos, which):
        return {"ep": pos * CORES + which}

    def remote(src, dst, send, recv, dev):
        return pltpu.make_async_remote_copy(src_ref=src, dst_ref=dst, send_sem=send, recv_sem=recv,
                                            device_id=dev, device_id_type=MESH)

    def weight_copies(step):
        buf, slot = step % W_DEPTH, step % n_slot
        return (pltpu.make_async_copy(up_hbm.at[0, slot], up_buf.at[buf], w_sem.at[0, buf]),
                pltpu.make_async_copy(down_hbm.at[0, slot], down_buf.at[buf], w_sem.at[1, buf]))

    own_tok = pltpu.make_async_copy(tok_hbm, toks.at[core, z], in_sem.at[0])
    own_idx = pltpu.make_async_copy(idx_hbm, idx_own, in_sem.at[1])
    own_gate = pltpu.make_async_copy(gate_hbm, metas.at[core, z, n_top:], in_sem.at[2])
    tables = [pltpu.make_async_copy(slot_hbm, ref, in_sem.at[3 + n]) for n, ref in enumerate((slot_smem, slot_vmem))]
    own_tok.start()
    own_idx.start()
    own_gate.start()
    for copy in tables:
        copy.start()
    barrier = pltpu.get_barrier_semaphore()
    pl.semaphore_signal(barrier, inc=1, device_id=device(ring(z + 1), core), device_id_type=MESH)
    pl.semaphore_signal(barrier, inc=1, device_id=device(ring(z - 1), core), device_id_type=MESH)
    pl.semaphore_signal(barrier, inc=1, device_id=device(z, other), device_id_type=MESH)
    own_idx.wait()
    metas[core, z, :n_top, :] = idx_own[...].astype(F32)
    own_gate.wait()
    own_tok.wait()
    pl.semaphore_wait(barrier, 3)

    def ag_copy(d, hop, c):
        sign = 1 - 2 * d
        ref = toks.at[core, ring(z - sign * (hop - 1)), pl.ds(c * ag_rows, ag_rows)]
        return remote(ref, ref, ag_send.at[d, hop - 1, c], ag_recv.at[d, hop - 1, c], device(ring(z + sign), core))

    def ag_arrival(d, hop, c):
        sign = 1 - 2 * d
        ref = toks.at[core, ring(z - sign * hop), pl.ds(c * ag_rows, ag_rows)]
        return remote(ref, ref, ag_send.at[d, hop - 1, c], ag_recv.at[d, hop - 1, c], device(ring(z + sign), core))

    def sib_copy(d, hop, c, which):
        sign = 1 - 2 * d
        ref = toks.at[which, ring(z - sign * hop), pl.ds(c * ag_rows, ag_rows)]
        return remote(ref, ref, sib_send.at[d, hop, c], sib_recv.at[d, hop, c], device(z, other))

    def meta_copy(d, hop, back):
        sign = 1 - 2 * d
        ref = metas.at[core, ring(z - sign * (hop - 1 + back))]
        return remote(ref, ref, ms_send.at[d, hop - 1], ms_recv.at[d, hop - 1], device(ring(z + sign), core))

    def meta_sib(d, hop, which):
        sign = 1 - 2 * d
        ref = metas.at[which, ring(z - sign * hop)]
        return remote(ref, ref, mb_send.at[d, hop], mb_recv.at[d, hop], device(z, other))

    def chunk_order(d):
        return list(range(AG_CHUNKS)) if d == 0 else list(range(AG_CHUNKS))[::-1]

    def carried(d, hop):
        order = chunk_order(d)
        return order if hop < half else order[:AG_CHUNKS // 2]

    def meta_carried(d, hop):
        return hop < half or d == 0

    for d in range(2):
        meta_copy(d, 1, 0).start()
    meta_sib(0, 0, core).start()

    @pl.when(core == 0)
    def _():
        for c in range(AG_CHUNKS):
            for d in range(2):
                ag_copy(d, 1, chunk_order(d)[c]).start()
        for c in range(AG_CHUNKS):
            sib_copy(0, 0, c, core).start()

    for step in range(W_DEPTH):
        for copy in weight_copies(step):
            copy.start()

    lane = lax.broadcasted_iota(jnp.int32, (cap, n_exp), 1)
    row = lax.broadcasted_iota(jnp.int32, (cap, n_exp), 0).astype(F32)
    for copy in tables:
        copy.wait()
    table = slot_vmem[...]
    place = lax.broadcasted_iota(jnp.int32, table.shape, 0) * n_slot + lax.broadcasted_iota(jnp.int32, table.shape, 1)
    if k_pad > 2 * rows:
        pick[2 * rows:, :] = jnp.zeros((k_pad - 2 * rows, n_exp), BF16)
        target[2 * rows:, :] = jnp.full((k_pad - 2 * rows, n_exp), -1.0, F32)

    def slot_rows(pos):
        for w in range(2):
            dev = pos * CORES + (core if w == 0 else other)
            for s in range(n_slot):
                exp_id = slot_smem[dev, s]
                same = table == exp_id
                copies = jnp.sum(jnp.where(same, 1.0, 0.0))
                earlier = jnp.sum(jnp.where(same & (place < dev * n_slot + s), 1.0, 0.0))
                at = pl.ds(w * rows + s * cap, cap)
                pick[at, :] = jnp.where(lane == exp_id, 1.0, 0.0).astype(BF16)
                target[at, :] = row * copies + earlier

    column = lax.broadcasted_iota(jnp.int32, (packed_pad, k_pad), 1)
    side = jnp.where(column >= rows, 1, 0)
    in_side = column - side * rows
    in_slot = in_side % cap
    packed_row = side * (packed // 2) + (in_side // cap) * bound + in_slot
    used = (in_slot < bound) & (column < 2 * rows)
    pack[...] = jnp.where(used & (lax.broadcasted_iota(jnp.int32, (packed_pad, k_pad), 0) == packed_row),
                          1.0, 0.0).astype(BF16)
    for d in range(2):
        slot_rows(ring(z - (1 - 2 * d)))
        pick_up[d] = jnp.dot(pack[...], pick[...], preferred_element_type=F32).astype(BF16)
        target_up[d] = jnp.dot(pack[...], (target[...] + 1.0).astype(BF16), preferred_element_type=F32) - 1.0
    slot_rows(z)

    exp_iota = lax.broadcasted_iota(jnp.int32, (n_exp, n_tok), 0).astype(F32)

    def ranks(info):
        chosen = jnp.zeros((n_exp, n_tok), F32)
        for j in range(n_top):
            chosen = jnp.where(exp_iota == info[j:j + 1, :], 1.0, chosen)
        before = (lax.broadcasted_iota(jnp.int32, (n_tok, n_tok), 0)
                  < lax.broadcasted_iota(jnp.int32, (n_tok, n_tok), 1))
        rank = jnp.dot(chosen.astype(BF16), jnp.where(before, 1.0, 0.0).astype(BF16), preferred_element_type=F32)
        return jnp.where(chosen > 0.5, rank, -1.0).astype(BF16)

    def mixing(info, rank, picks, targets):
        gate = jnp.zeros((n_exp, n_tok), F32)
        for j in range(n_top):
            gate = jnp.where(exp_iota == info[j:j + 1, :], info[n_top + j:n_top + j + 1, :], gate)
        takes = jnp.dot(picks, rank, preferred_element_type=F32) == targets
        parts = [jnp.dot(picks, part, preferred_element_type=F32) for part in split3(gate)]
        return split3(jnp.where(takes, parts[0] + parts[1] + parts[2], 0.0).T)

    def mix_first_hop():
        @pl.loop(0, 4)
        def _(i):
            d, j = i // 2, i % 2
            info = metas[core, ring(z + (1 - 2 * d) * (half - 1 - j))]
            for n, part in enumerate(mixing(info, ranks(info), pick_up[d], target_up[d])):
                mix_up[d, j, n * n_tok:(n + 1) * n_tok, :] = part

    def place_rows(which, pos):
        info = metas[which, pos]
        rank = ranks(info)
        takes = jnp.dot(pick[:rows, :], rank, preferred_element_type=F32) == target[:rows, :]
        onehot = jnp.where(takes, 1.0, 0.0).astype(BF16)
        for c in range(RS_CHUNKS):
            cols = pl.ds(c * rs_cols, rs_cols)
            got = jnp.dot(onehot, toks[which, pos, :, cols], preferred_element_type=F32).astype(BF16)
            x_buf[:, which, pos, :, cols] = got.reshape(n_slot, cap, rs_cols)

        @pl.when(core == which)
        def _():
            for n, part in enumerate(mixing(info, rank, pick[...], target[...])):
                mix[pos, n * n_tok:(n + 1) * n_tok, :] = part

    def start_gather():
        for c in range(AG_CHUNKS):
            for d in range(2):
                ag_copy(d, 1, chunk_order(d)[c]).start()
        for c in range(AG_CHUNKS):
            sib_copy(0, 0, c, core).start()

    def pass_on(hop, n):
        for d in range(2):
            if n < len(carried(d, hop)):
                c = carried(d, hop)[n]
                ag_arrival(d, hop, c).wait_recv()
                if hop < half and c in carried(d, hop + 1):
                    ag_copy(d, hop + 1, c).start()
                sib_copy(d, hop, c, core).start()

    def from_sibling(hop):
        if hop == 0:
            for c in range(AG_CHUNKS):
                sib_copy(0, 0, c, other).wait_recv()
            return
        for d in range(2):
            for c in carried(d, hop):
                sib_copy(d, hop, c, other).wait_recv()

    def place_hop(which, hop):
        @pl.loop(0, 1 if hop in (0, half) else 2)
        def _(d):
            place_rows(which, ring(z - (1 - 2 * d) * hop))

    def meta_from_sibling(hop):
        for d in range(2):
            if (hop == 0 and d == 0) or (hop > 0 and meta_carried(d, hop)):
                meta_sib(d, hop, other).wait_recv()

    for hop in range(half + 1):
        if hop > 0:
            for d in range(2):
                if meta_carried(d, hop):
                    meta_copy(d, hop, 1).wait_recv()
                    if hop < half and meta_carried(d, hop + 1):
                        meta_copy(d, hop + 1, 0).start()
                    meta_sib(d, hop, core).start()

        @pl.when(core == 0)
        def _():
            if hop > 0:
                for n in range(len(carried(0, hop))):
                    pass_on(hop, n)

        @pl.when(core == 1)
        def _():
            meta_from_sibling(hop)
            from_sibling(hop)
            if hop == AG2_HOP:
                start_gather()

        place_hop(0, hop)
        if hop == half - 1:
            @pl.when(core == 0)
            def _():
                mix_first_hop()

    def o_copy(slot):
        return remote(x_buf.at[slot, other], o_sib.at[slot], o_send.at[slot], o_recv.at[slot], device(z, other))

    def experts(slot, batch):
        step = batch * n_slot + slot
        buf = step % W_DEPTH
        for copy in weight_copies(step):
            copy.wait()
        x = x_buf[slot, batch].reshape(nz * cap, d_model)
        hidden = jax.nn.gelu(jnp.dot(x, up_buf[buf], preferred_element_type=F32), approximate=True).astype(BF16)
        for c in range(RS_CHUNKS):
            cols = pl.ds(c * rs_cols, rs_cols)
            o = jnp.dot(hidden, down_buf[buf, :, cols], preferred_element_type=F32).astype(BF16)
            x_buf[slot, batch, :, :, cols] = o.reshape(nz, cap, rs_cols)

        @pl.when(core != batch)
        def _():
            o_copy(slot).start()

        @pl.when(step + W_DEPTH < 2 * n_slot)
        def _():
            for copy in weight_copies(step + W_DEPTH):
                copy.start()

    @pl.loop(0, n_slot)
    def _(slot):
        experts(slot, 0)

        @pl.when((core == 1) & (slot < 2 * AG_CHUNKS))
        def _():
            hop, n = 1 + slot // AG_CHUNKS, slot % AG_CHUNKS
            for d in range(2):
                c = n if d == 0 else AG_CHUNKS - 1 - n
                ag_arrival(d, hop, c).wait_recv()
                ag_copy(d, hop + 1, c).start()
                sib_copy(d, hop, c, core).start()

    def from_sibling_o():
        @pl.loop(0, n_slot)
        def _(slot):
            o_copy(slot).wait_recv()

    def chip_rows(pos, c):
        cols = pl.ds(pl.multiple_of(c * rs_cols, rs_cols), rs_cols)
        parts = [x_buf[:, core, pos, :, cols].reshape(rows, rs_cols), o_sib[:, pos, :, cols].reshape(rows, rs_cols)]
        if k_pad > 2 * rows:
            parts.append(jnp.zeros((k_pad - 2 * rows, rs_cols), BF16))
        return jnp.concatenate(parts, axis=0)

    def mixed(weights, values):
        total = jnp.dot(weights, values, preferred_element_type=F32)
        return total[:n_tok] + total[n_tok:2 * n_tok] + total[2 * n_tok:]

    def own_sum(pos, c):
        return mixed(mix[pos], chip_rows(pos, c))

    skip = RS_CHUNKS // 2
    first = skip + RS_CHUNKS
    items = half * RS_CHUNKS

    def rs_chunk(d, n):
        c = n % RS_CHUNKS
        return (c + skip) % RS_CHUNKS if d == 0 else c

    def rs_dest(d, n):
        return ring(z + (1 - 2 * d) * (half - n // RS_CHUNKS))

    def first_copy(d, n):
        return remote(first_out.at[d, n - skip], first_in.at[d, n - skip], rs_send.at[d, n],
                      rs_recv.at[d, n + RS_CHUNKS], device(ring(z + (1 - 2 * d)), core))

    def first_arrival(d, n):
        return remote(first_out.at[d, n - first], first_in.at[d, n - first], rs_send.at[d, n],
                      rs_recv.at[d, n], device(ring(z + (1 - 2 * d)), core))

    def rs_copy(d, n):
        return remote(rs_buf.at[d, n - first], rs_buf.at[d, n - first + RS_CHUNKS], rs_send.at[d, n],
                      rs_recv.at[d, n + RS_CHUNKS], device(ring(z + (1 - 2 * d)), core))

    def rs_arrival(d, n):
        return remote(rs_buf.at[d, n - first], rs_buf.at[d, n - first], rs_send.at[d, n], rs_recv.at[d, n],
                      device(ring(z + (1 - 2 * d)), core))

    def first_item(n):
        for d in range(2):
            got = jnp.dot(pack[:packed, :], chip_rows(rs_dest(d, n), rs_chunk(d, n)), preferred_element_type=F32)
            first_out[d, n - skip] = got.astype(BF16)
            first_copy(d, n).start()

    def second_item(n):
        for d in range(2):
            value = own_sum(rs_dest(d, n), rs_chunk(d, n))
            first_arrival(d, n).wait_recv()
            rows_in = first_in[d, n - first]
            if packed_pad > packed:
                rows_in = jnp.concatenate([rows_in, jnp.zeros((packed_pad - packed, rs_cols), BF16)], axis=0)
            rs_buf[d, n - first] = value + mixed(mix_up[d, (n - first) // skip], rows_in)
            rs_copy(d, n).start()

    def later_item(n):
        for d in range(2):
            value = own_sum(rs_dest(d, n), rs_chunk(d, n))
            rs_arrival(d, n).wait_recv()
            rs_buf[d, n - first] += value
            rs_copy(d, n).start()

    def start_chains():
        from_sibling_o()
        pl.loop(skip, first)(first_item)

    @pl.when(core == 0)
    def _():
        start_chains()

    for hop in range(half + 1):
        @pl.when(core == 0)
        def _():
            meta_from_sibling(hop)
            from_sibling(hop)

        @pl.when(core == 1)
        def _():
            for late, n in AG2_LATE[hop]:
                pass_on(late, n)

        place_hop(1, hop)
        if hop > 0:
            @pl.when(core == 0)
            def _():
                second_item(first + hop - 1)

    @pl.loop(0, n_slot)
    def _(slot):
        experts(slot, 1)

        @pl.when((core == 0) & (slot < items - first - RS_CHUNKS))
        def _():
            later_item(first + RS_CHUNKS + slot)

    @pl.when(core == 1)
    def _():
        mix_first_hop()
        start_chains()
        pl.loop(first, first + RS_CHUNKS)(second_item)
        pl.loop(first + RS_CHUNKS, items)(later_item)

    for c in range(RS_CHUNKS):
        total_buf[c] = own_sum(z, c)
    for i in range(RS_CHUNKS):
        for d in range(2):
            rs_arrival(d, items + i).wait_recv()
        if i >= skip:
            for c in (i - skip, i):
                value = total_buf[c]
                for d in range(2):
                    value += rs_buf[d, items - first + ((c + skip) % RS_CHUNKS if d == 0 else c)]
                out_ref[:, c * rs_cols:(c + 1) * rs_cols] = value.astype(BF16)

    for d in range(2):
        for hop in range(1, half + 1):
            if meta_carried(d, hop):
                meta_copy(d, hop, 0).wait_send()
                meta_sib(d, hop, core).wait_send()
            for c in carried(d, hop):
                ag_copy(d, hop, c).wait_send()
                sib_copy(d, hop, c, core).wait_send()
    meta_sib(0, 0, core).wait_send()
    for c in range(AG_CHUNKS):
        sib_copy(0, 0, c, core).wait_send()

    @pl.loop(0, n_slot)
    def _(slot):
        o_copy(slot).wait_send()

    @pl.loop(skip, first)
    def _(n):
        for d in range(2):
            first_copy(d, n).wait_send()

    @pl.loop(first, items)
    def _(n):
        for d in range(2):
            rs_copy(d, n).wait_send()


def solution(mesh):
    n_dev = mesh.shape["ep"]
    nz = n_dev // CORES
    half = nz // 2

    def group_layer(tokens, topk_idx, topk_w, w_up, w_down, slot_expert):
        n_tok, d_model = tokens.shape
        n_top = topk_idx.shape[1]
        n_slot = slot_expert.shape[1]
        n_exp = n_dev * (n_slot - 1)
        d_ff = w_up.shape[3]
        bound = slot_bound(n_tok, n_top, n_dev, n_slot)
        cap = round_up(bound, 16)
        k_pad = round_up(2 * n_slot * cap, 128)
        packed = 2 * round_up(n_slot * bound, 8)
        packed_pad = round_up(packed, 128)
        rs_cols = d_model // RS_CHUNKS
        skip = RS_CHUNKS // 2
        dma = pltpu.SemaphoreType.DMA
        any_space = pl.BlockSpec(memory_space=pl.ANY)
        vmem = pl.BlockSpec(memory_space=pltpu.VMEM)
        return pl.pallas_call(
            functools.partial(layer_kernel, nz, bound),
            out_shape=jax.ShapeDtypeStruct((n_tok, d_model), BF16),
            in_specs=[any_space] * 6,
            out_specs=vmem,
            scratch_shapes=[
                pltpu.VMEM((CORES, nz, n_tok, d_model), BF16),
                pltpu.VMEM((n_top, n_tok), jnp.int32),
                pltpu.SMEM(slot_expert.shape, jnp.int32),
                pltpu.VMEM(slot_expert.shape, jnp.int32),
                pltpu.VMEM((CORES, nz, 2 * n_top, n_tok), F32),
                pltpu.VMEM((n_slot, CORES, nz, cap, d_model), BF16),
                pltpu.VMEM((n_slot, nz, cap, d_model), BF16),
                pltpu.VMEM((W_DEPTH, d_model, d_ff), BF16),
                pltpu.VMEM((W_DEPTH, d_ff, d_model), BF16),
                pltpu.VMEM((2, half * RS_CHUNKS - skip, n_tok, rs_cols), F32),
                pltpu.VMEM((2, RS_CHUNKS, packed, rs_cols), BF16),
                pltpu.VMEM((2, RS_CHUNKS, packed, rs_cols), BF16),
                pltpu.VMEM((RS_CHUNKS, n_tok, rs_cols), F32),
                pltpu.VMEM((nz, 3 * n_tok, k_pad), BF16),
                pltpu.VMEM((2, 2, 3 * n_tok, packed_pad), BF16),
                pltpu.VMEM((k_pad, n_exp), BF16),
                pltpu.VMEM((k_pad, n_exp), F32),
                pltpu.VMEM((2, packed_pad, n_exp), BF16),
                pltpu.VMEM((2, packed_pad, n_exp), F32),
                pltpu.VMEM((packed_pad, k_pad), BF16),
                dma((5,)),
                dma((2, half, AG_CHUNKS)), dma((2, half, AG_CHUNKS)),
                dma((2, half + 1, AG_CHUNKS)), dma((2, half + 1, AG_CHUNKS)),
                dma((2, half)), dma((2, half)),
                dma((2, half + 1)), dma((2, half + 1)),
                dma((2, W_DEPTH)),
                dma((n_slot,)), dma((n_slot,)),
                dma((2, half * RS_CHUNKS)), dma((2, (half + 1) * RS_CHUNKS)),
            ],
            compiler_params=pltpu.CompilerParams(collective_id=0, has_side_effects=True,
                                                 vmem_limit_bytes=67043328),
        )(tokens, topk_idx.T, topk_w.T, slot_expert, w_up, w_down)

    row_spec = P(("dp", "ep"), None)
    weight_spec = P("ep", None, None, None)
    return jax.shard_map(group_layer, mesh=mesh,
                         in_specs=(row_spec, row_spec, row_spec, weight_spec, weight_spec, P(None, None)),
                         out_specs=row_spec, check_vma=False)
```

```python
import functools

import jax
import jax.numpy as jnp
from jax import lax
from jax.experimental import pallas as pl
from jax.experimental.pallas import tpu as pltpu
from jax.sharding import PartitionSpec as P

MESH = pl.DeviceIdType.MESH
F32 = jnp.float32
BF16 = jnp.bfloat16
CORES = 2
W_DEPTH = 4
AG_CHUNKS = 4
RS_CHUNKS = 4
AG2_LATE = (((3, 0), (3, 1)), ((3, 2), (3, 3)), ((4, 0), (4, 1)), (), ())
AG2_HOP = 3


def slot_bound(n_tok, n_top, n_dev, n_slot):
    base_load = (n_tok * n_top) // (n_dev * n_slot)
    return base_load + base_load // 2 + 1


def round_up(n, unit):
    return -(-n // unit) * unit


def split3(x):
    hi = x.astype(BF16)
    rest = x - hi.astype(F32)
    mid = rest.astype(BF16)
    low = (rest - mid.astype(F32)).astype(BF16)
    return hi, mid, low


def layer_kernel(nz, bound, tok_hbm, idx_hbm, gate_hbm, slot_hbm, up_hbm, down_hbm, out_ref,
                 toks, idx_own, slot_smem, slot_vmem, metas, x_buf, o_sib, up_buf, down_buf, rs_buf, first_out, first_in, total_buf,
                 mix, mix_up, pick, target, pick_up, target_up, pack,
                 in_sem, ag_send, ag_recv, sib_send, sib_recv, ms_send, ms_recv, mb_send, mb_recv,
                 w_sem, o_send, o_recv, first_send, first_recv, rs_send, rs_recv):
    half = nz // 2
    n_tok, d_model = tok_hbm.shape
    n_top = idx_hbm.shape[0]
    n_slot, cap = x_buf.shape[0], x_buf.shape[3]
    rows = n_slot * cap
    k_pad, n_exp = pick.shape
    packed, packed_pad = first_out.shape[3], pack.shape[0]
    ag_rows = n_tok // AG_CHUNKS
    rs_cols = d_model // RS_CHUNKS

    me = lax.axis_index("ep")
    z = me // CORES
    core = me % CORES
    other = 1 - core

    def ring(pos):
        return (pos + nz) % nz

    def device(pos, which):
        return {"ep": pos * CORES + which}

    def remote(src, dst, send, recv, dev):
        return pltpu.make_async_remote_copy(src_ref=src, dst_ref=dst, send_sem=send, recv_sem=recv,
                                            device_id=dev, device_id_type=MESH)

    def weight_copies(step):
        buf, slot = step % W_DEPTH, step % n_slot
        return (pltpu.make_async_copy(up_hbm.at[0, slot], up_buf.at[buf], w_sem.at[0, buf]),
                pltpu.make_async_copy(down_hbm.at[0, slot], down_buf.at[buf], w_sem.at[1, buf]))

    own_tok = pltpu.make_async_copy(tok_hbm, toks.at[core, z], in_sem.at[0])
    own_idx = pltpu.make_async_copy(idx_hbm, idx_own, in_sem.at[1])
    own_gate = pltpu.make_async_copy(gate_hbm, metas.at[core, z, n_top:], in_sem.at[2])
    tables = [pltpu.make_async_copy(slot_hbm, ref, in_sem.at[3 + n]) for n, ref in enumerate((slot_smem, slot_vmem))]
    own_tok.start()
    own_idx.start()
    own_gate.start()
    for copy in tables:
        copy.start()
    barrier = pltpu.get_barrier_semaphore()
    pl.semaphore_signal(barrier, inc=1, device_id=device(ring(z + 1), core), device_id_type=MESH)
    pl.semaphore_signal(barrier, inc=1, device_id=device(ring(z - 1), core), device_id_type=MESH)
    pl.semaphore_signal(barrier, inc=1, device_id=device(z, other), device_id_type=MESH)
    pl.semaphore_signal(barrier, inc=1, device_id=device(ring(z + 1), other), device_id_type=MESH)
    pl.semaphore_signal(barrier, inc=1, device_id=device(ring(z - 1), other), device_id_type=MESH)
    own_idx.wait()
    metas[core, z, :n_top, :] = idx_own[...].astype(F32)
    own_gate.wait()
    own_tok.wait()
    pl.semaphore_wait(barrier, 5)

    def ag_copy(d, hop, c):
        sign = 1 - 2 * d
        ref = toks.at[core, ring(z - sign * (hop - 1)), pl.ds(c * ag_rows, ag_rows)]
        return remote(ref, ref, ag_send.at[d, hop - 1, c], ag_recv.at[d, hop - 1, c], device(ring(z + sign), core))

    def ag_arrival(d, hop, c):
        sign = 1 - 2 * d
        ref = toks.at[core, ring(z - sign * hop), pl.ds(c * ag_rows, ag_rows)]
        return remote(ref, ref, ag_send.at[d, hop - 1, c], ag_recv.at[d, hop - 1, c], device(ring(z + sign), core))

    def sib_copy(d, hop, c, which):
        sign = 1 - 2 * d
        ref = toks.at[which, ring(z - sign * hop), pl.ds(c * ag_rows, ag_rows)]
        return remote(ref, ref, sib_send.at[d, hop, c], sib_recv.at[d, hop, c], device(z, other))

    def meta_copy(d, hop, back):
        sign = 1 - 2 * d
        ref = metas.at[core, ring(z - sign * (hop - 1 + back))]
        return remote(ref, ref, ms_send.at[d, hop - 1], ms_recv.at[d, hop - 1], device(ring(z + sign), core))

    def meta_sib(d, hop, which):
        sign = 1 - 2 * d
        ref = metas.at[which, ring(z - sign * hop)]
        return remote(ref, ref, mb_send.at[d, hop], mb_recv.at[d, hop], device(z, other))

    def chunk_order(d):
        return list(range(AG_CHUNKS)) if d == 0 else list(range(AG_CHUNKS))[::-1]

    def carried(d, hop):
        order = chunk_order(d)
        return order if hop < half else order[:AG_CHUNKS // 2]

    def meta_carried(d, hop):
        return hop < half or d == 0

    for d in range(2):
        meta_copy(d, 1, 0).start()
    meta_sib(0, 0, core).start()

    @pl.when(core == 0)
    def _():
        for c in range(AG_CHUNKS):
            for d in range(2):
                ag_copy(d, 1, chunk_order(d)[c]).start()
        for c in range(AG_CHUNKS):
            sib_copy(0, 0, c, core).start()

    for step in range(W_DEPTH):
        for copy in weight_copies(step):
            copy.start()

    lane = lax.broadcasted_iota(jnp.int32, (cap, n_exp), 1)
    row = lax.broadcasted_iota(jnp.int32, (cap, n_exp), 0).astype(F32)
    for copy in tables:
        copy.wait()
    table = slot_vmem[...]
    place = lax.broadcasted_iota(jnp.int32, table.shape, 0) * n_slot + lax.broadcasted_iota(jnp.int32, table.shape, 1)
    if k_pad > 2 * rows:
        pick[2 * rows:, :] = jnp.zeros((k_pad - 2 * rows, n_exp), BF16)
        target[2 * rows:, :] = jnp.full((k_pad - 2 * rows, n_exp), -1.0, F32)

    def slot_rows(pos):
        for w in range(2):
            dev = pos * CORES + (core if w == 0 else other)
            for s in range(n_slot):
                exp_id = slot_smem[dev, s]
                same = table == exp_id
                copies = jnp.sum(jnp.where(same, 1.0, 0.0))
                earlier = jnp.sum(jnp.where(same & (place < dev * n_slot + s), 1.0, 0.0))
                at = pl.ds(w * rows + s * cap, cap)
                pick[at, :] = jnp.where(lane == exp_id, 1.0, 0.0).astype(BF16)
                target[at, :] = row * copies + earlier

    column = lax.broadcasted_iota(jnp.int32, (packed_pad, k_pad), 1)
    side = jnp.where(column >= rows, 1, 0)
    in_side = column - side * rows
    in_slot = in_side % cap
    packed_row = side * (packed // 2) + (in_side // cap) * bound + in_slot
    used = (in_slot < bound) & (column < 2 * rows)
    pack[...] = jnp.where(used & (lax.broadcasted_iota(jnp.int32, (packed_pad, k_pad), 0) == packed_row),
                          1.0, 0.0).astype(BF16)
    for d in range(2):
        slot_rows(ring(z - (1 - 2 * d)))
        pick_up[d] = jnp.dot(pack[...], pick[...], preferred_element_type=F32).astype(BF16)
        target_up[d] = jnp.dot(pack[...], (target[...] + 1.0).astype(BF16), preferred_element_type=F32) - 1.0
    slot_rows(z)

    exp_iota = lax.broadcasted_iota(jnp.int32, (n_exp, n_tok), 0).astype(F32)

    def ranks(info):
        chosen = jnp.zeros((n_exp, n_tok), F32)
        for j in range(n_top):
            chosen = jnp.where(exp_iota == info[j:j + 1, :], 1.0, chosen)
        before = (lax.broadcasted_iota(jnp.int32, (n_tok, n_tok), 0)
                  < lax.broadcasted_iota(jnp.int32, (n_tok, n_tok), 1))
        rank = jnp.dot(chosen.astype(BF16), jnp.where(before, 1.0, 0.0).astype(BF16), preferred_element_type=F32)
        return jnp.where(chosen > 0.5, rank, -1.0).astype(BF16)

    def mixing(info, rank, picks, targets):
        gate = jnp.zeros((n_exp, n_tok), F32)
        for j in range(n_top):
            gate = jnp.where(exp_iota == info[j:j + 1, :], info[n_top + j:n_top + j + 1, :], gate)
        takes = jnp.dot(picks, rank, preferred_element_type=F32) == targets
        parts = [jnp.dot(picks, part, preferred_element_type=F32) for part in split3(gate)]
        return split3(jnp.where(takes, parts[0] + parts[1] + parts[2], 0.0).T)

    def mix_first_hop():
        @pl.loop(0, 4)
        def _(i):
            d, j = i // 2, i % 2
            info = metas[core, ring(z + (1 - 2 * d) * (half - 1 - j))]
            for n, part in enumerate(mixing(info, ranks(info), pick_up[d], target_up[d])):
                mix_up[d, j, n * n_tok:(n + 1) * n_tok, :] = part

    def place_rows(which, pos):
        info = metas[which, pos]
        rank = ranks(info)
        takes = jnp.dot(pick[:rows, :], rank, preferred_element_type=F32) == target[:rows, :]
        onehot = jnp.where(takes, 1.0, 0.0).astype(BF16)
        for c in range(RS_CHUNKS):
            cols = pl.ds(c * rs_cols, rs_cols)
            got = jnp.dot(onehot, toks[which, pos, :, cols], preferred_element_type=F32).astype(BF16)
            x_buf[:, which, pos, :, cols] = got.reshape(n_slot, cap, rs_cols)

        @pl.when(core == which)
        def _():
            for n, part in enumerate(mixing(info, rank, pick[...], target[...])):
                mix[pos, n * n_tok:(n + 1) * n_tok, :] = part

    def start_gather():
        for c in range(AG_CHUNKS):
            for d in range(2):
                ag_copy(d, 1, chunk_order(d)[c]).start()
        for c in range(AG_CHUNKS):
            sib_copy(0, 0, c, core).start()

    def pass_on(hop, n):
        for d in range(2):
            if n < len(carried(d, hop)):
                c = carried(d, hop)[n]
                ag_arrival(d, hop, c).wait_recv()
                if hop < half and c in carried(d, hop + 1):
                    ag_copy(d, hop + 1, c).start()
                sib_copy(d, hop, c, core).start()

    def from_sibling(hop):
        if hop == 0:
            for c in range(AG_CHUNKS):
                sib_copy(0, 0, c, other).wait_recv()
            return
        for d in range(2):
            for c in carried(d, hop):
                sib_copy(d, hop, c, other).wait_recv()

    def place_hop(which, hop):
        @pl.loop(0, 1 if hop in (0, half) else 2)
        def _(d):
            place_rows(which, ring(z - (1 - 2 * d) * hop))

    def meta_from_sibling(hop):
        for d in range(2):
            if (hop == 0 and d == 0) or (hop > 0 and meta_carried(d, hop)):
                meta_sib(d, hop, other).wait_recv()

    for hop in range(half + 1):
        if hop > 0:
            for d in range(2):
                if meta_carried(d, hop):
                    meta_copy(d, hop, 1).wait_recv()
                    if hop < half and meta_carried(d, hop + 1):
                        meta_copy(d, hop + 1, 0).start()
                    meta_sib(d, hop, core).start()

        @pl.when(core == 0)
        def _():
            if hop > 0:
                for n in range(len(carried(0, hop))):
                    pass_on(hop, n)

        @pl.when(core == 1)
        def _():
            meta_from_sibling(hop)
            from_sibling(hop)
            if hop == AG2_HOP:
                start_gather()

        place_hop(0, hop)
        if hop == half - 1:
            @pl.when(core == 0)
            def _():
                mix_first_hop()

    def o_copy(slot):
        return remote(x_buf.at[slot, other], o_sib.at[slot], o_send.at[slot], o_recv.at[slot], device(z, other))

    def experts(slot, batch):
        step = batch * n_slot + slot
        buf = step % W_DEPTH
        for copy in weight_copies(step):
            copy.wait()
        x = x_buf[slot, batch].reshape(nz * cap, d_model)
        hidden = jax.nn.gelu(jnp.dot(x, up_buf[buf], preferred_element_type=F32), approximate=True).astype(BF16)
        for c in range(RS_CHUNKS):
            cols = pl.ds(c * rs_cols, rs_cols)
            o = jnp.dot(hidden, down_buf[buf, :, cols], preferred_element_type=F32).astype(BF16)
            x_buf[slot, batch, :, :, cols] = o.reshape(nz, cap, rs_cols)

        @pl.when(core != batch)
        def _():
            o_copy(slot).start()

        @pl.when(step + W_DEPTH < 2 * n_slot)
        def _():
            for copy in weight_copies(step + W_DEPTH):
                copy.start()

    @pl.loop(0, n_slot)
    def _(slot):
        experts(slot, 0)

        @pl.when((core == 1) & (slot < 2 * AG_CHUNKS))
        def _():
            hop, n = 1 + slot // AG_CHUNKS, slot % AG_CHUNKS
            for d in range(2):
                c = n if d == 0 else AG_CHUNKS - 1 - n
                ag_arrival(d, hop, c).wait_recv()
                ag_copy(d, hop + 1, c).start()
                sib_copy(d, hop, c, core).start()

    def from_sibling_o():
        @pl.loop(0, n_slot)
        def _(slot):
            o_copy(slot).wait_recv()

    def chip_rows(pos, c):
        cols = pl.ds(pl.multiple_of(c * rs_cols, rs_cols), rs_cols)
        parts = [x_buf[:, core, pos, :, cols].reshape(rows, rs_cols), o_sib[:, pos, :, cols].reshape(rows, rs_cols)]
        if k_pad > 2 * rows:
            parts.append(jnp.zeros((k_pad - 2 * rows, rs_cols), BF16))
        return jnp.concatenate(parts, axis=0)

    def mixed(weights, values):
        total = jnp.dot(weights, values, preferred_element_type=F32)
        return total[:n_tok] + total[n_tok:2 * n_tok] + total[2 * n_tok:]

    def own_sum(pos, c):
        return mixed(mix[pos], chip_rows(pos, c))

    skip = RS_CHUNKS // 2
    first = skip + RS_CHUNKS
    items = half * RS_CHUNKS

    def rs_chunk(d, n):
        c = n % RS_CHUNKS
        return (c + skip) % RS_CHUNKS if d == 0 else c

    def rs_dest(d, n):
        return ring(z + (1 - 2 * d) * (half - n // RS_CHUNKS))

    def first_copy(batch, d, j):
        side = jnp.where(core == batch, 0, 1)
        return remote(first_out.at[batch, d, j], first_in.at[side, d, j], first_send.at[batch, d, j],
                      first_recv.at[side, d, j], device(ring(z + (1 - 2 * d)), batch))

    def first_arrival(side, d, j):
        return remote(first_out.at[0, d, j], first_in.at[side, d, j], first_send.at[0, d, j],
                      first_recv.at[side, d, j], device(ring(z + (1 - 2 * d)), core))

    def rs_copy(d, n):
        return remote(rs_buf.at[d, n - first], rs_buf.at[d, n - first + RS_CHUNKS], rs_send.at[d, n],
                      rs_recv.at[d, n + RS_CHUNKS], device(ring(z + (1 - 2 * d)), core))

    def rs_arrival(d, n):
        return remote(rs_buf.at[d, n - first], rs_buf.at[d, n - first], rs_send.at[d, n], rs_recv.at[d, n],
                      device(ring(z + (1 - 2 * d)), core))

    def start_chains(batch):
        k_own = round_up(rows, 128)
        for j in range(2):
            for d in range(2):
                got = []
                for n in (skip + 2 * j, skip + 2 * j + 1):
                    cols = pl.ds(rs_chunk(d, n) * rs_cols, rs_cols)
                    parts = [x_buf[:, batch, rs_dest(d, n), :, cols].reshape(rows, rs_cols)]
                    if k_own > rows:
                        parts.append(jnp.zeros((k_own - rows, rs_cols), BF16))
                    got.append(jnp.dot(pack[:round_up(packed // 2, 16), :k_own], jnp.concatenate(parts, axis=0),
                                       preferred_element_type=F32)[:packed // 2])
                first_out[batch, d, j] = jnp.concatenate(got, axis=0).astype(BF16)
                first_copy(batch, d, j).start()

    def second_pair(j):
        for d in range(2):
            for side in range(2):
                first_arrival(side, d, j).wait_recv()
            sides = [first_in[side, d, j].astype(F32) for side in range(2)]
            for i in range(2):
                n = first + 2 * j + i
                parts = [part[i * (packed // 2):(i + 1) * (packed // 2)] for part in sides]
                if packed_pad > packed:
                    parts.append(jnp.zeros((packed_pad - packed, rs_cols), F32))
                rows_in = jnp.concatenate(parts, axis=0).astype(BF16)
                rs_buf[d, n - first] = own_sum(rs_dest(d, n), rs_chunk(d, n)) + mixed(mix_up[d, j], rows_in)
                rs_copy(d, n).start()

    def later_item(n):
        for d in range(2):
            value = own_sum(rs_dest(d, n), rs_chunk(d, n))
            rs_arrival(d, n).wait_recv()
            rs_buf[d, n - first] += value
            rs_copy(d, n).start()

    start_chains(0)

    @pl.when(core == 0)
    def _():
        from_sibling_o()

    for hop in range(half + 1):
        @pl.when(core == 0)
        def _():
            meta_from_sibling(hop)
            from_sibling(hop)

        @pl.when(core == 1)
        def _():
            for late, n in AG2_LATE[hop]:
                pass_on(late, n)

        place_hop(1, hop)
        if hop in (1, 2):
            @pl.when(core == 0)
            def _():
                second_pair(hop - 1)

    @pl.loop(0, n_slot)
    def _(slot):
        experts(slot, 1)

        @pl.when((core == 0) & (slot < items - first - RS_CHUNKS))
        def _():
            later_item(first + RS_CHUNKS + slot)

    start_chains(1)

    @pl.when(core == 1)
    def _():
        mix_first_hop()
        from_sibling_o()
        for j in range(2):
            second_pair(j)
        pl.loop(first + RS_CHUNKS, items)(later_item)

    for c in range(RS_CHUNKS):
        total_buf[c] = own_sum(z, c)
    for i in range(RS_CHUNKS):
        for d in range(2):
            rs_arrival(d, items + i).wait_recv()
        if i >= skip:
            for c in (i - skip, i):
                value = total_buf[c]
                for d in range(2):
                    value += rs_buf[d, items - first + ((c + skip) % RS_CHUNKS if d == 0 else c)]
                out_ref[:, c * rs_cols:(c + 1) * rs_cols] = value.astype(BF16)

    for d in range(2):
        for hop in range(1, half + 1):
            if meta_carried(d, hop):
                meta_copy(d, hop, 0).wait_send()
                meta_sib(d, hop, core).wait_send()
            for c in carried(d, hop):
                ag_copy(d, hop, c).wait_send()
                sib_copy(d, hop, c, core).wait_send()
    meta_sib(0, 0, core).wait_send()
    for c in range(AG_CHUNKS):
        sib_copy(0, 0, c, core).wait_send()

    @pl.loop(0, n_slot)
    def _(slot):
        o_copy(slot).wait_send()

    for batch in range(2):
        for d in range(2):
            for j in range(2):
                first_copy(batch, d, j).wait_send()

    @pl.loop(first, items)
    def _(n):
        for d in range(2):
            rs_copy(d, n).wait_send()


def solution(mesh):
    n_dev = mesh.shape["ep"]
    nz = n_dev // CORES
    half = nz // 2

    def group_layer(tokens, topk_idx, topk_w, w_up, w_down, slot_expert):
        n_tok, d_model = tokens.shape
        n_top = topk_idx.shape[1]
        n_slot = slot_expert.shape[1]
        n_exp = n_dev * (n_slot - 1)
        d_ff = w_up.shape[3]
        bound = slot_bound(n_tok, n_top, n_dev, n_slot)
        cap = round_up(bound, 16)
        k_pad = round_up(2 * n_slot * cap, 128)
        packed = 2 * round_up(n_slot * bound, 8)
        packed_pad = round_up(packed, 128)
        rs_cols = d_model // RS_CHUNKS
        skip = RS_CHUNKS // 2
        dma = pltpu.SemaphoreType.DMA
        any_space = pl.BlockSpec(memory_space=pl.ANY)
        vmem = pl.BlockSpec(memory_space=pltpu.VMEM)
        return pl.pallas_call(
            functools.partial(layer_kernel, nz, bound),
            out_shape=jax.ShapeDtypeStruct((n_tok, d_model), BF16),
            in_specs=[any_space] * 6,
            out_specs=vmem,
            scratch_shapes=[
                pltpu.VMEM((CORES, nz, n_tok, d_model), BF16),
                pltpu.VMEM((n_top, n_tok), jnp.int32),
                pltpu.SMEM(slot_expert.shape, jnp.int32),
                pltpu.VMEM(slot_expert.shape, jnp.int32),
                pltpu.VMEM((CORES, nz, 2 * n_top, n_tok), F32),
                pltpu.VMEM((n_slot, CORES, nz, cap, d_model), BF16),
                pltpu.VMEM((n_slot, nz, cap, d_model), BF16),
                pltpu.VMEM((W_DEPTH, d_model, d_ff), BF16),
                pltpu.VMEM((W_DEPTH, d_ff, d_model), BF16),
                pltpu.VMEM((2, half * RS_CHUNKS - skip, n_tok, rs_cols), F32),
                pltpu.VMEM((2, 2, 2, packed, rs_cols), BF16),
                pltpu.VMEM((2, 2, 2, packed, rs_cols), BF16),
                pltpu.VMEM((RS_CHUNKS, n_tok, rs_cols), F32),
                pltpu.VMEM((nz, 3 * n_tok, k_pad), BF16),
                pltpu.VMEM((2, 2, 3 * n_tok, packed_pad), BF16),
                pltpu.VMEM((k_pad, n_exp), BF16),
                pltpu.VMEM((k_pad, n_exp), F32),
                pltpu.VMEM((2, packed_pad, n_exp), BF16),
                pltpu.VMEM((2, packed_pad, n_exp), F32),
                pltpu.VMEM((packed_pad, k_pad), BF16),
                dma((5,)),
                dma((2, half, AG_CHUNKS)), dma((2, half, AG_CHUNKS)),
                dma((2, half + 1, AG_CHUNKS)), dma((2, half + 1, AG_CHUNKS)),
                dma((2, half)), dma((2, half)),
                dma((2, half + 1)), dma((2, half + 1)),
                dma((2, W_DEPTH)),
                dma((n_slot,)), dma((n_slot,)),
                dma((2, 2, 2)), dma((2, 2, 2)),
                dma((2, half * RS_CHUNKS)), dma((2, (half + 1) * RS_CHUNKS)),
            ],
            compiler_params=pltpu.CompilerParams(collective_id=0, has_side_effects=True,
                                                 vmem_limit_bytes=67043328),
        )(tokens, topk_idx.T, topk_w.T, slot_expert, w_up, w_down)

    row_spec = P(("dp", "ep"), None)
    weight_spec = P("ep", None, None, None)
    return jax.shard_map(group_layer, mesh=mesh,
                         in_specs=(row_spec, row_spec, row_spec, weight_spec, weight_spec, P(None, None)),
                         out_specs=row_spec, check_vma=False)
```

```python
import functools

import jax
import jax.numpy as jnp
from jax import lax
from jax.experimental import pallas as pl
from jax.experimental.pallas import tpu as pltpu
from jax.sharding import PartitionSpec as P

MESH = pl.DeviceIdType.MESH
F32 = jnp.float32
BF16 = jnp.bfloat16
CORES = 2
W_DEPTH = 4
AG_CHUNKS = 4
RS_CHUNKS = 4
AG2_LATE = (((3, 0), (3, 1)), ((3, 2), (3, 3)), ((4, 0), (4, 1)), (), ())
AG2_HOP = 3


def slot_bound(n_tok, n_top, n_dev, n_slot):
    base_load = (n_tok * n_top) // (n_dev * n_slot)
    return base_load + base_load // 2 + 1


def round_up(n, unit):
    return -(-n // unit) * unit


def split3(x):
    hi = x.astype(BF16)
    rest = x - hi.astype(F32)
    mid = rest.astype(BF16)
    low = (rest - mid.astype(F32)).astype(BF16)
    return hi, mid, low


def layer_kernel(nz, bound, tok_hbm, idx_hbm, gate_hbm, slot_hbm, up_hbm, down_hbm, out_ref,
                 toks, idx_own, slot_smem, slot_vmem, metas, x_buf, o_sib, up_buf, down_buf, rs_buf, first_out, first_in, total_buf,
                 mix, mix_up, pick, target, pick_up, target_up, pack,
                 in_sem, ag_send, ag_recv, sib_send, sib_recv, ms_send, ms_recv, mb_send, mb_recv,
                 w_sem, o_send, o_recv, first_send, first_recv, rs_send, rs_recv):
    half = nz // 2
    n_tok, d_model = tok_hbm.shape
    n_top = idx_hbm.shape[0]
    n_slot, cap = x_buf.shape[0], x_buf.shape[3]
    rows = n_slot * cap
    k_pad, n_exp = pick.shape
    packed, packed_pad = first_out.shape[3], pack.shape[0]
    ag_rows = n_tok // AG_CHUNKS
    rs_cols = d_model // RS_CHUNKS

    me = lax.axis_index("ep")
    z = me // CORES
    core = me % CORES
    other = 1 - core

    def ring(pos):
        return (pos + nz) % nz

    def device(pos, which):
        return {"ep": pos * CORES + which}

    def remote(src, dst, send, recv, dev):
        return pltpu.make_async_remote_copy(src_ref=src, dst_ref=dst, send_sem=send, recv_sem=recv,
                                            device_id=dev, device_id_type=MESH)

    def weight_copies(step):
        buf, slot = step % W_DEPTH, step % n_slot
        return (pltpu.make_async_copy(up_hbm.at[0, slot], up_buf.at[buf], w_sem.at[0, buf]),
                pltpu.make_async_copy(down_hbm.at[0, slot], down_buf.at[buf], w_sem.at[1, buf]))

    own_tok = pltpu.make_async_copy(tok_hbm, toks.at[core, z], in_sem.at[0])
    own_idx = pltpu.make_async_copy(idx_hbm, idx_own, in_sem.at[1])
    own_gate = pltpu.make_async_copy(gate_hbm, metas.at[core, z, n_top:], in_sem.at[2])
    tables = [pltpu.make_async_copy(slot_hbm, ref, in_sem.at[3 + n]) for n, ref in enumerate((slot_smem, slot_vmem))]
    own_tok.start()
    own_idx.start()
    own_gate.start()
    for copy in tables:
        copy.start()
    barrier = pltpu.get_barrier_semaphore()
    pl.semaphore_signal(barrier, inc=1, device_id=device(ring(z + 1), core), device_id_type=MESH)
    pl.semaphore_signal(barrier, inc=1, device_id=device(ring(z - 1), core), device_id_type=MESH)
    pl.semaphore_signal(barrier, inc=1, device_id=device(z, other), device_id_type=MESH)
    pl.semaphore_signal(barrier, inc=1, device_id=device(ring(z + 1), other), device_id_type=MESH)
    pl.semaphore_signal(barrier, inc=1, device_id=device(ring(z - 1), other), device_id_type=MESH)
    own_idx.wait()
    metas[core, z, :n_top, :] = idx_own[...].astype(F32)
    own_gate.wait()
    own_tok.wait()
    pl.semaphore_wait(barrier, 5)

    def ag_copy(d, hop, c):
        sign = 1 - 2 * d
        ref = toks.at[core, ring(z - sign * (hop - 1)), pl.ds(c * ag_rows, ag_rows)]
        return remote(ref, ref, ag_send.at[d, hop - 1, c], ag_recv.at[d, hop - 1, c], device(ring(z + sign), core))

    def ag_arrival(d, hop, c):
        sign = 1 - 2 * d
        ref = toks.at[core, ring(z - sign * hop), pl.ds(c * ag_rows, ag_rows)]
        return remote(ref, ref, ag_send.at[d, hop - 1, c], ag_recv.at[d, hop - 1, c], device(ring(z + sign), core))

    def sib_copy(d, hop, c, which):
        sign = 1 - 2 * d
        ref = toks.at[which, ring(z - sign * hop), pl.ds(c * ag_rows, ag_rows)]
        return remote(ref, ref, sib_send.at[d, hop, c], sib_recv.at[d, hop, c], device(z, other))

    def meta_copy(d, hop, back):
        sign = 1 - 2 * d
        ref = metas.at[core, ring(z - sign * (hop - 1 + back))]
        return remote(ref, ref, ms_send.at[d, hop - 1], ms_recv.at[d, hop - 1], device(ring(z + sign), core))

    def meta_sib(d, hop, which):
        sign = 1 - 2 * d
        ref = metas.at[which, ring(z - sign * hop)]
        return remote(ref, ref, mb_send.at[d, hop], mb_recv.at[d, hop], device(z, other))

    def chunk_order(d):
        return list(range(AG_CHUNKS)) if d == 0 else list(range(AG_CHUNKS))[::-1]

    def carried(d, hop):
        order = chunk_order(d)
        return order if hop < half else order[:AG_CHUNKS // 2]

    def meta_carried(d, hop):
        return hop < half or d == 0

    for d in range(2):
        meta_copy(d, 1, 0).start()
    meta_sib(0, 0, core).start()

    @pl.when(core == 0)
    def _():
        for c in range(AG_CHUNKS):
            for d in range(2):
                ag_copy(d, 1, chunk_order(d)[c]).start()
        for c in range(AG_CHUNKS):
            sib_copy(0, 0, c, core).start()

    for step in range(W_DEPTH):
        for copy in weight_copies(step):
            copy.start()

    lane = lax.broadcasted_iota(jnp.int32, (cap, n_exp), 1)
    row = lax.broadcasted_iota(jnp.int32, (cap, n_exp), 0).astype(F32)
    for copy in tables:
        copy.wait()
    table = slot_vmem[...]
    place = lax.broadcasted_iota(jnp.int32, table.shape, 0) * n_slot + lax.broadcasted_iota(jnp.int32, table.shape, 1)
    if k_pad > 2 * rows:
        pick[2 * rows:, :] = jnp.zeros((k_pad - 2 * rows, n_exp), BF16)
        target[2 * rows:, :] = jnp.full((k_pad - 2 * rows, n_exp), -1.0, F32)

    def slot_rows(pos):
        for w in range(2):
            dev = pos * CORES + (core if w == 0 else other)
            for s in range(n_slot):
                exp_id = slot_smem[dev, s]
                same = table == exp_id
                copies = jnp.sum(jnp.where(same, 1.0, 0.0))
                earlier = jnp.sum(jnp.where(same & (place < dev * n_slot + s), 1.0, 0.0))
                at = pl.ds(w * rows + s * cap, cap)
                pick[at, :] = jnp.where(lane == exp_id, 1.0, 0.0).astype(BF16)
                target[at, :] = row * copies + earlier

    column = lax.broadcasted_iota(jnp.int32, (packed_pad, k_pad), 1)
    side = jnp.where(column >= rows, 1, 0)
    in_side = column - side * rows
    in_slot = in_side % cap
    packed_row = side * (packed // 2) + (in_side // cap) * bound + in_slot
    used = (in_slot < bound) & (column < 2 * rows)
    pack[...] = jnp.where(used & (lax.broadcasted_iota(jnp.int32, (packed_pad, k_pad), 0) == packed_row),
                          1.0, 0.0).astype(BF16)
    for d in range(2):
        slot_rows(ring(z - (1 - 2 * d)))
        pick_up[d] = jnp.dot(pack[...], pick[...], preferred_element_type=F32).astype(BF16)
        target_up[d] = jnp.dot(pack[...], (target[...] + 1.0).astype(BF16), preferred_element_type=F32) - 1.0
    slot_rows(z)

    exp_iota = lax.broadcasted_iota(jnp.int32, (n_exp, n_tok), 0).astype(F32)

    def ranks(info):
        chosen = jnp.zeros((n_exp, n_tok), F32)
        for j in range(n_top):
            chosen = jnp.where(exp_iota == info[j:j + 1, :], 1.0, chosen)
        before = (lax.broadcasted_iota(jnp.int32, (n_tok, n_tok), 0)
                  < lax.broadcasted_iota(jnp.int32, (n_tok, n_tok), 1))
        rank = jnp.dot(chosen.astype(BF16), jnp.where(before, 1.0, 0.0).astype(BF16), preferred_element_type=F32)
        return jnp.where(chosen > 0.5, rank, -1.0).astype(BF16)

    def mixing(info, rank, picks, targets):
        gate = jnp.zeros((n_exp, n_tok), F32)
        for j in range(n_top):
            gate = jnp.where(exp_iota == info[j:j + 1, :], info[n_top + j:n_top + j + 1, :], gate)
        takes = jnp.dot(picks, rank, preferred_element_type=F32) == targets
        parts = [jnp.dot(picks, part, preferred_element_type=F32) for part in split3(gate)]
        return split3(jnp.where(takes, parts[0] + parts[1] + parts[2], 0.0).T)

    def mix_first_hop():
        @pl.loop(0, 4)
        def _(i):
            d, j = i // 2, i % 2
            info = metas[core, ring(z + (1 - 2 * d) * (half - 1 - j))]
            for n, part in enumerate(mixing(info, ranks(info), pick_up[d], target_up[d])):
                mix_up[d, j, n * n_tok:(n + 1) * n_tok, :] = part

    def place_rows(which, pos):
        info = metas[which, pos]
        rank = ranks(info)
        takes = jnp.dot(pick[:rows, :], rank, preferred_element_type=F32) == target[:rows, :]
        onehot = jnp.where(takes, 1.0, 0.0).astype(BF16)
        for c in range(RS_CHUNKS):
            cols = pl.ds(c * rs_cols, rs_cols)
            got = jnp.dot(onehot, toks[which, pos, :, cols], preferred_element_type=F32).astype(BF16)
            x_buf[:, which, pos, :, cols] = got.reshape(n_slot, cap, rs_cols)

        @pl.when(core == which)
        def _():
            for n, part in enumerate(mixing(info, rank, pick[...], target[...])):
                mix[pos, n * n_tok:(n + 1) * n_tok, :] = part

    def start_gather():
        for c in range(AG_CHUNKS):
            for d in range(2):
                ag_copy(d, 1, chunk_order(d)[c]).start()
        for c in range(AG_CHUNKS):
            sib_copy(0, 0, c, core).start()

    def pass_on(hop, n):
        for d in range(2):
            if n < len(carried(d, hop)):
                c = carried(d, hop)[n]
                ag_arrival(d, hop, c).wait_recv()
                if hop < half and c in carried(d, hop + 1):
                    ag_copy(d, hop + 1, c).start()
                sib_copy(d, hop, c, core).start()

    def from_sibling(hop):
        if hop == 0:
            for c in range(AG_CHUNKS):
                sib_copy(0, 0, c, other).wait_recv()
            return
        for d in range(2):
            for c in carried(d, hop):
                sib_copy(d, hop, c, other).wait_recv()

    def place_hop(which, hop):
        @pl.loop(0, 1 if hop in (0, half) else 2)
        def _(d):
            place_rows(which, ring(z - (1 - 2 * d) * hop))

    def meta_from_sibling(hop):
        for d in range(2):
            if (hop == 0 and d == 0) or (hop > 0 and meta_carried(d, hop)):
                meta_sib(d, hop, other).wait_recv()

    for hop in range(half + 1):
        if hop > 0:
            for d in range(2):
                if meta_carried(d, hop):
                    meta_copy(d, hop, 1).wait_recv()
                    if hop < half and meta_carried(d, hop + 1):
                        meta_copy(d, hop + 1, 0).start()
                    meta_sib(d, hop, core).start()

        @pl.when(core == 0)
        def _():
            if hop > 0:
                for n in range(len(carried(0, hop))):
                    pass_on(hop, n)

        @pl.when(core == 1)
        def _():
            meta_from_sibling(hop)
            from_sibling(hop)
            if hop == AG2_HOP:
                start_gather()

        place_hop(0, hop)
        if hop == half - 1:
            @pl.when(core == 0)
            def _():
                mix_first_hop()

    def o_copy(slot):
        return remote(x_buf.at[slot, other], o_sib.at[slot], o_send.at[slot], o_recv.at[slot], device(z, other))

    def experts(slot, batch):
        step = batch * n_slot + slot
        buf = step % W_DEPTH
        for copy in weight_copies(step):
            copy.wait()
        x = x_buf[slot, batch].reshape(nz * cap, d_model)
        hidden = jax.nn.gelu(jnp.dot(x, up_buf[buf], preferred_element_type=F32), approximate=True).astype(BF16)
        for c in range(RS_CHUNKS):
            cols = pl.ds(c * rs_cols, rs_cols)
            o = jnp.dot(hidden, down_buf[buf, :, cols], preferred_element_type=F32).astype(BF16)
            x_buf[slot, batch, :, :, cols] = o.reshape(nz, cap, rs_cols)

        @pl.when(core != batch)
        def _():
            o_copy(slot).start()

        @pl.when(step + W_DEPTH < 2 * n_slot)
        def _():
            for copy in weight_copies(step + W_DEPTH):
                copy.start()

    @pl.loop(0, n_slot)
    def _(slot):
        experts(slot, 0)

        @pl.when((core == 1) & (slot < 2 * AG_CHUNKS))
        def _():
            hop, n = 1 + slot // AG_CHUNKS, slot % AG_CHUNKS
            for d in range(2):
                c = n if d == 0 else AG_CHUNKS - 1 - n
                ag_arrival(d, hop, c).wait_recv()
                ag_copy(d, hop + 1, c).start()
                sib_copy(d, hop, c, core).start()

    def from_sibling_o():
        @pl.loop(0, n_slot)
        def _(slot):
            o_copy(slot).wait_recv()

    def chip_rows(pos, c):
        cols = pl.ds(pl.multiple_of(c * rs_cols, rs_cols), rs_cols)
        parts = [x_buf[:, core, pos, :, cols].reshape(rows, rs_cols), o_sib[:, pos, :, cols].reshape(rows, rs_cols)]
        if k_pad > 2 * rows:
            parts.append(jnp.zeros((k_pad - 2 * rows, rs_cols), BF16))
        return jnp.concatenate(parts, axis=0)

    def mixed(weights, values):
        total = jnp.dot(weights, values, preferred_element_type=F32)
        return total[:n_tok] + total[n_tok:2 * n_tok] + total[2 * n_tok:]

    def own_sum(pos, c):
        return mixed(mix[pos], chip_rows(pos, c))

    skip = RS_CHUNKS // 2
    first = skip + RS_CHUNKS
    items = half * RS_CHUNKS

    def rs_chunk(d, n):
        c = n % RS_CHUNKS
        return (c + skip) % RS_CHUNKS if d == 0 else c

    def rs_dest(d, n):
        return ring(z + (1 - 2 * d) * (half - n // RS_CHUNKS))

    def first_copy(batch, d, j):
        side = jnp.where(core == batch, 0, 1)
        return remote(first_out.at[batch, d, j], first_in.at[side, d, j], first_send.at[batch, d, j],
                      first_recv.at[side, d, j], device(ring(z + (1 - 2 * d)), batch))

    def first_arrival(side, d, j):
        return remote(first_out.at[0, d, j], first_in.at[side, d, j], first_send.at[0, d, j],
                      first_recv.at[side, d, j], device(ring(z + (1 - 2 * d)), core))

    def rs_copy(d, n):
        return remote(rs_buf.at[d, n - first], rs_buf.at[d, n - first + RS_CHUNKS], rs_send.at[d, n],
                      rs_recv.at[d, n + RS_CHUNKS], device(ring(z + (1 - 2 * d)), core))

    def rs_arrival(d, n):
        return remote(rs_buf.at[d, n - first], rs_buf.at[d, n - first], rs_send.at[d, n], rs_recv.at[d, n],
                      device(ring(z + (1 - 2 * d)), core))

    def start_chains(batch):
        k_own = round_up(rows, 128)
        for j in range(2):
            for d in range(2):
                got = []
                for n in (skip + 2 * j, skip + 2 * j + 1):
                    cols = pl.ds(rs_chunk(d, n) * rs_cols, rs_cols)
                    parts = [x_buf[:, batch, rs_dest(d, n), :, cols].reshape(rows, rs_cols)]
                    if k_own > rows:
                        parts.append(jnp.zeros((k_own - rows, rs_cols), BF16))
                    got.append(jnp.dot(pack[:round_up(packed // 2, 16), :k_own], jnp.concatenate(parts, axis=0),
                                       preferred_element_type=F32)[:packed // 2])
                first_out[batch, d, j] = jnp.concatenate(got, axis=0).astype(BF16)
                first_copy(batch, d, j).start()

    def second_pair(j):
        for d in range(2):
            for side in range(2):
                first_arrival(side, d, j).wait_recv()
            sides = [first_in[side, d, j].astype(F32) for side in range(2)]
            for i in range(2):
                n = first + 2 * j + i
                parts = [part[i * (packed // 2):(i + 1) * (packed // 2)] for part in sides]
                if packed_pad > packed:
                    parts.append(jnp.zeros((packed_pad - packed, rs_cols), F32))
                rows_in = jnp.concatenate(parts, axis=0).astype(BF16)
                rs_buf[d, n - first] = own_sum(rs_dest(d, n), rs_chunk(d, n)) + mixed(mix_up[d, j], rows_in)
                rs_copy(d, n).start()

    def later_item(n):
        for d in range(2):
            value = own_sum(rs_dest(d, n), rs_chunk(d, n))
            rs_arrival(d, n).wait_recv()
            rs_buf[d, n - first] += value
            rs_copy(d, n).start()

    start_chains(0)

    @pl.when(core == 0)
    def _():
        from_sibling_o()

    for hop in range(half + 1):
        @pl.when(core == 0)
        def _():
            meta_from_sibling(hop)
            from_sibling(hop)

        @pl.when(core == 1)
        def _():
            for late, n in AG2_LATE[hop]:
                pass_on(late, n)

        place_hop(1, hop)
        if hop in (1, 2):
            @pl.when(core == 0)
            def _():
                second_pair(hop - 1)

    @pl.loop(0, n_slot)
    def _(slot):
        experts(slot, 1)

    start_chains(1)

    @pl.when(core == 1)
    def _():
        mix_first_hop()
        from_sibling_o()
        for j in range(2):
            second_pair(j)

    pl.loop(first + RS_CHUNKS, items)(later_item)

    for c in range(RS_CHUNKS):
        total_buf[c] = own_sum(z, c)
    for i in range(RS_CHUNKS):
        for d in range(2):
            rs_arrival(d, items + i).wait_recv()
        if i >= skip:
            for c in (i - skip, i):
                value = total_buf[c]
                for d in range(2):
                    value += rs_buf[d, items - first + ((c + skip) % RS_CHUNKS if d == 0 else c)]
                out_ref[:, c * rs_cols:(c + 1) * rs_cols] = value.astype(BF16)

    for d in range(2):
        for hop in range(1, half + 1):
            if meta_carried(d, hop):
                meta_copy(d, hop, 0).wait_send()
                meta_sib(d, hop, core).wait_send()
            for c in carried(d, hop):
                ag_copy(d, hop, c).wait_send()
                sib_copy(d, hop, c, core).wait_send()
    meta_sib(0, 0, core).wait_send()
    for c in range(AG_CHUNKS):
        sib_copy(0, 0, c, core).wait_send()

    @pl.loop(0, n_slot)
    def _(slot):
        o_copy(slot).wait_send()

    for batch in range(2):
        for d in range(2):
            for j in range(2):
                first_copy(batch, d, j).wait_send()

    @pl.loop(first, items)
    def _(n):
        for d in range(2):
            rs_copy(d, n).wait_send()


def solution(mesh):
    n_dev = mesh.shape["ep"]
    nz = n_dev // CORES
    half = nz // 2

    def group_layer(tokens, topk_idx, topk_w, w_up, w_down, slot_expert):
        n_tok, d_model = tokens.shape
        n_top = topk_idx.shape[1]
        n_slot = slot_expert.shape[1]
        n_exp = n_dev * (n_slot - 1)
        d_ff = w_up.shape[3]
        bound = slot_bound(n_tok, n_top, n_dev, n_slot)
        cap = round_up(bound, 16)
        k_pad = round_up(2 * n_slot * cap, 128)
        packed = 2 * round_up(n_slot * bound, 8)
        packed_pad = round_up(packed, 128)
        rs_cols = d_model // RS_CHUNKS
        skip = RS_CHUNKS // 2
        dma = pltpu.SemaphoreType.DMA
        any_space = pl.BlockSpec(memory_space=pl.ANY)
        vmem = pl.BlockSpec(memory_space=pltpu.VMEM)
        return pl.pallas_call(
            functools.partial(layer_kernel, nz, bound),
            out_shape=jax.ShapeDtypeStruct((n_tok, d_model), BF16),
            in_specs=[any_space] * 6,
            out_specs=vmem,
            scratch_shapes=[
                pltpu.VMEM((CORES, nz, n_tok, d_model), BF16),
                pltpu.VMEM((n_top, n_tok), jnp.int32),
                pltpu.SMEM(slot_expert.shape, jnp.int32),
                pltpu.VMEM(slot_expert.shape, jnp.int32),
                pltpu.VMEM((CORES, nz, 2 * n_top, n_tok), F32),
                pltpu.VMEM((n_slot, CORES, nz, cap, d_model), BF16),
                pltpu.VMEM((n_slot, nz, cap, d_model), BF16),
                pltpu.VMEM((W_DEPTH, d_model, d_ff), BF16),
                pltpu.VMEM((W_DEPTH, d_ff, d_model), BF16),
                pltpu.VMEM((2, half * RS_CHUNKS - skip, n_tok, rs_cols), F32),
                pltpu.VMEM((2, 2, 2, packed, rs_cols), BF16),
                pltpu.VMEM((2, 2, 2, packed, rs_cols), BF16),
                pltpu.VMEM((RS_CHUNKS, n_tok, rs_cols), F32),
                pltpu.VMEM((nz, 3 * n_tok, k_pad), BF16),
                pltpu.VMEM((2, 2, 3 * n_tok, packed_pad), BF16),
                pltpu.VMEM((k_pad, n_exp), BF16),
                pltpu.VMEM((k_pad, n_exp), F32),
                pltpu.VMEM((2, packed_pad, n_exp), BF16),
                pltpu.VMEM((2, packed_pad, n_exp), F32),
                pltpu.VMEM((packed_pad, k_pad), BF16),
                dma((5,)),
                dma((2, half, AG_CHUNKS)), dma((2, half, AG_CHUNKS)),
                dma((2, half + 1, AG_CHUNKS)), dma((2, half + 1, AG_CHUNKS)),
                dma((2, half)), dma((2, half)),
                dma((2, half + 1)), dma((2, half + 1)),
                dma((2, W_DEPTH)),
                dma((n_slot,)), dma((n_slot,)),
                dma((2, 2, 2)), dma((2, 2, 2)),
                dma((2, half * RS_CHUNKS)), dma((2, (half + 1) * RS_CHUNKS)),
            ],
            compiler_params=pltpu.CompilerParams(collective_id=0, has_side_effects=True,
                                                 vmem_limit_bytes=67043328),
        )(tokens, topk_idx.T, topk_w.T, slot_expert, w_up, w_down)

    row_spec = P(("dp", "ep"), None)
    weight_spec = P("ep", None, None, None)
    return jax.shard_map(group_layer, mesh=mesh,
                         in_specs=(row_spec, row_spec, row_spec, weight_spec, weight_spec, P(None, None)),
                         out_specs=row_spec, check_vma=False)
```

```python
import functools

import jax
import jax.numpy as jnp
from jax import lax
from jax.experimental import pallas as pl
from jax.experimental.pallas import tpu as pltpu
from jax.sharding import PartitionSpec as P

MESH = pl.DeviceIdType.MESH
F32 = jnp.float32
BF16 = jnp.bfloat16
CORES = 2
W_DEPTH = 4
AG_CHUNKS = 4
RS_CHUNKS = 4
AG2_LATE = (((3, 0), (3, 1)), ((3, 2), (3, 3)), ((4, 0), (4, 1)), (), ())
AG2_HOP = 3


def slot_bound(n_tok, n_top, n_dev, n_slot):
    base_load = (n_tok * n_top) // (n_dev * n_slot)
    return base_load + base_load // 2 + 1


def round_up(n, unit):
    return -(-n // unit) * unit


def split3(x):
    hi = x.astype(BF16)
    rest = x - hi.astype(F32)
    mid = rest.astype(BF16)
    low = (rest - mid.astype(F32)).astype(BF16)
    return hi, mid, low


def layer_kernel(nz, bound, tok_hbm, idx_hbm, gate_hbm, slot_hbm, up_hbm, down_hbm, out_ref,
                 toks, idx_own, slot_smem, slot_vmem, metas, x_buf, o_sib, up_buf, down_buf, rs_buf, first_out, first_in, total_buf,
                 mix, mix_up, pick, target, pick_up, target_up, pack,
                 in_sem, ag_send, ag_recv, sib_send, sib_recv, ms_send, ms_recv, mb_send, mb_recv,
                 w_sem, o_send, o_recv, first_send, first_recv, rs_send, rs_recv):
    half = nz // 2
    n_tok, d_model = tok_hbm.shape
    n_top = idx_hbm.shape[0]
    n_slot, cap = x_buf.shape[0], x_buf.shape[3]
    rows = n_slot * cap
    k_pad, n_exp = pick.shape
    packed, packed_pad = first_out.shape[3], pack.shape[0]
    ag_rows = n_tok // AG_CHUNKS
    rs_cols = d_model // RS_CHUNKS

    me = lax.axis_index("ep")
    z = me // CORES
    core = me % CORES
    other = 1 - core

    def ring(pos):
        return (pos + nz) % nz

    def device(pos, which):
        return {"ep": pos * CORES + which}

    def remote(src, dst, send, recv, dev):
        return pltpu.make_async_remote_copy(src_ref=src, dst_ref=dst, send_sem=send, recv_sem=recv,
                                            device_id=dev, device_id_type=MESH)

    def weight_copies(slot):
        buf = slot % W_DEPTH
        return (pltpu.make_async_copy(up_hbm.at[0, slot], up_buf.at[buf], w_sem.at[0, buf]),
                pltpu.make_async_copy(down_hbm.at[0, slot], down_buf.at[buf], w_sem.at[1, buf]))

    own_tok = pltpu.make_async_copy(tok_hbm, toks.at[core, z], in_sem.at[0])
    own_idx = pltpu.make_async_copy(idx_hbm, idx_own, in_sem.at[1])
    own_gate = pltpu.make_async_copy(gate_hbm, metas.at[core, z, n_top:], in_sem.at[2])
    tables = [pltpu.make_async_copy(slot_hbm, ref, in_sem.at[3 + n]) for n, ref in enumerate((slot_smem, slot_vmem))]
    own_tok.start()
    own_idx.start()
    own_gate.start()
    for copy in tables:
        copy.start()
    barrier = pltpu.get_barrier_semaphore()
    pl.semaphore_signal(barrier, inc=1, device_id=device(ring(z + 1), core), device_id_type=MESH)
    pl.semaphore_signal(barrier, inc=1, device_id=device(ring(z - 1), core), device_id_type=MESH)
    pl.semaphore_signal(barrier, inc=1, device_id=device(z, other), device_id_type=MESH)
    pl.semaphore_signal(barrier, inc=1, device_id=device(ring(z + 1), other), device_id_type=MESH)
    pl.semaphore_signal(barrier, inc=1, device_id=device(ring(z - 1), other), device_id_type=MESH)
    own_idx.wait()
    metas[core, z, :n_top, :] = idx_own[...].astype(F32)
    own_gate.wait()
    own_tok.wait()
    pl.semaphore_wait(barrier, 5)

    def ag_copy(d, hop, c):
        sign = 1 - 2 * d
        ref = toks.at[core, ring(z - sign * (hop - 1)), pl.ds(c * ag_rows, ag_rows)]
        return remote(ref, ref, ag_send.at[d, hop - 1, c], ag_recv.at[d, hop - 1, c], device(ring(z + sign), core))

    def ag_arrival(d, hop, c):
        sign = 1 - 2 * d
        ref = toks.at[core, ring(z - sign * hop), pl.ds(c * ag_rows, ag_rows)]
        return remote(ref, ref, ag_send.at[d, hop - 1, c], ag_recv.at[d, hop - 1, c], device(ring(z + sign), core))

    def sib_copy(d, hop, c, which):
        sign = 1 - 2 * d
        ref = toks.at[which, ring(z - sign * hop), pl.ds(c * ag_rows, ag_rows)]
        return remote(ref, ref, sib_send.at[d, hop, c], sib_recv.at[d, hop, c], device(z, other))

    def meta_copy(d, hop, back):
        sign = 1 - 2 * d
        ref = metas.at[core, ring(z - sign * (hop - 1 + back))]
        return remote(ref, ref, ms_send.at[d, hop - 1], ms_recv.at[d, hop - 1], device(ring(z + sign), core))

    def meta_sib(d, hop, which):
        sign = 1 - 2 * d
        ref = metas.at[which, ring(z - sign * hop)]
        return remote(ref, ref, mb_send.at[d, hop], mb_recv.at[d, hop], device(z, other))

    def chunk_order(d):
        return list(range(AG_CHUNKS)) if d == 0 else list(range(AG_CHUNKS))[::-1]

    def carried(d, hop):
        order = chunk_order(d)
        return order if hop < half else order[:AG_CHUNKS // 2]

    def meta_carried(d, hop):
        return hop < half or d == 0

    for d in range(2):
        meta_copy(d, 1, 0).start()
    meta_sib(0, 0, core).start()

    @pl.when(core == 0)
    def _():
        for c in range(AG_CHUNKS):
            for d in range(2):
                ag_copy(d, 1, chunk_order(d)[c]).start()
        for c in range(AG_CHUNKS):
            sib_copy(0, 0, c, core).start()

    for slot in range(W_DEPTH):
        for copy in weight_copies(slot):
            copy.start()

    lane = lax.broadcasted_iota(jnp.int32, (cap, n_exp), 1)
    row = lax.broadcasted_iota(jnp.int32, (cap, n_exp), 0).astype(F32)
    for copy in tables:
        copy.wait()
    table = slot_vmem[...]
    place = lax.broadcasted_iota(jnp.int32, table.shape, 0) * n_slot + lax.broadcasted_iota(jnp.int32, table.shape, 1)
    if k_pad > 2 * rows:
        pick[2 * rows:, :] = jnp.zeros((k_pad - 2 * rows, n_exp), BF16)
        target[2 * rows:, :] = jnp.full((k_pad - 2 * rows, n_exp), -1.0, F32)

    def slot_rows(pos):
        for w in range(2):
            dev = pos * CORES + (core if w == 0 else other)
            for s in range(n_slot):
                exp_id = slot_smem[dev, s]
                same = table == exp_id
                copies = jnp.sum(jnp.where(same, 1.0, 0.0))
                earlier = jnp.sum(jnp.where(same & (place < dev * n_slot + s), 1.0, 0.0))
                at = pl.ds(w * rows + s * cap, cap)
                pick[at, :] = jnp.where(lane == exp_id, 1.0, 0.0).astype(BF16)
                target[at, :] = row * copies + earlier

    column = lax.broadcasted_iota(jnp.int32, (packed_pad, k_pad), 1)
    side = jnp.where(column >= rows, 1, 0)
    in_side = column - side * rows
    in_slot = in_side % cap
    packed_row = side * (packed // 2) + (in_side // cap) * bound + in_slot
    used = (in_slot < bound) & (column < 2 * rows)
    pack[...] = jnp.where(used & (lax.broadcasted_iota(jnp.int32, (packed_pad, k_pad), 0) == packed_row),
                          1.0, 0.0).astype(BF16)
    for d in range(2):
        slot_rows(ring(z - (1 - 2 * d)))
        pick_up[d] = jnp.dot(pack[...], pick[...], preferred_element_type=F32).astype(BF16)
        target_up[d] = jnp.dot(pack[...], (target[...] + 1.0).astype(BF16), preferred_element_type=F32) - 1.0
    slot_rows(z)

    exp_iota = lax.broadcasted_iota(jnp.int32, (n_exp, n_tok), 0).astype(F32)

    def ranks(info):
        chosen = jnp.zeros((n_exp, n_tok), F32)
        for j in range(n_top):
            chosen = jnp.where(exp_iota == info[j:j + 1, :], 1.0, chosen)
        before = (lax.broadcasted_iota(jnp.int32, (n_tok, n_tok), 0)
                  < lax.broadcasted_iota(jnp.int32, (n_tok, n_tok), 1))
        rank = jnp.dot(chosen.astype(BF16), jnp.where(before, 1.0, 0.0).astype(BF16), preferred_element_type=F32)
        return jnp.where(chosen > 0.5, rank, -1.0).astype(BF16)

    def mixing(info, rank, picks, targets):
        gate = jnp.zeros((n_exp, n_tok), F32)
        for j in range(n_top):
            gate = jnp.where(exp_iota == info[j:j + 1, :], info[n_top + j:n_top + j + 1, :], gate)
        takes = jnp.dot(picks, rank, preferred_element_type=F32) == targets
        parts = [jnp.dot(picks, part, preferred_element_type=F32) for part in split3(gate)]
        return split3(jnp.where(takes, parts[0] + parts[1] + parts[2], 0.0).T)

    def mix_first_hop():
        @pl.loop(0, 4)
        def _(i):
            d, j = i // 2, i % 2
            info = metas[core, ring(z + (1 - 2 * d) * (half - 1 - j))]
            for n, part in enumerate(mixing(info, ranks(info), pick_up[d], target_up[d])):
                mix_up[d, j, n * n_tok:(n + 1) * n_tok, :] = part

    def place_rows(which, pos):
        info = metas[which, pos]
        rank = ranks(info)
        takes = jnp.dot(pick[:rows, :], rank, preferred_element_type=F32) == target[:rows, :]
        onehot = jnp.where(takes, 1.0, 0.0).astype(BF16)
        for c in range(RS_CHUNKS):
            cols = pl.ds(c * rs_cols, rs_cols)
            got = jnp.dot(onehot, toks[which, pos, :, cols], preferred_element_type=F32).astype(BF16)
            x_buf[:, which, pos, :, cols] = got.reshape(n_slot, cap, rs_cols)

        @pl.when(core == which)
        def _():
            for n, part in enumerate(mixing(info, rank, pick[...], target[...])):
                mix[pos, n * n_tok:(n + 1) * n_tok, :] = part

    def start_gather():
        for c in range(AG_CHUNKS):
            for d in range(2):
                ag_copy(d, 1, chunk_order(d)[c]).start()
        for c in range(AG_CHUNKS):
            sib_copy(0, 0, c, core).start()

    def pass_on(hop, n):
        for d in range(2):
            if n < len(carried(d, hop)):
                c = carried(d, hop)[n]
                ag_arrival(d, hop, c).wait_recv()
                if hop < half and c in carried(d, hop + 1):
                    ag_copy(d, hop + 1, c).start()
                sib_copy(d, hop, c, core).start()

    def from_sibling(hop):
        if hop == 0:
            for c in range(AG_CHUNKS):
                sib_copy(0, 0, c, other).wait_recv()
            return
        for d in range(2):
            for c in carried(d, hop):
                sib_copy(d, hop, c, other).wait_recv()

    def place_hop(which, hop):
        @pl.loop(0, 1 if hop in (0, half) else 2)
        def _(d):
            place_rows(which, ring(z - (1 - 2 * d) * hop))

    def meta_from_sibling(hop):
        for d in range(2):
            if (hop == 0 and d == 0) or (hop > 0 and meta_carried(d, hop)):
                meta_sib(d, hop, other).wait_recv()

    for hop in range(half + 1):
        if hop > 0:
            for d in range(2):
                if meta_carried(d, hop):
                    meta_copy(d, hop, 1).wait_recv()
                    if hop < half and meta_carried(d, hop + 1):
                        meta_copy(d, hop + 1, 0).start()
                    meta_sib(d, hop, core).start()

        @pl.when(core == 0)
        def _():
            if hop > 0:
                for n in range(len(carried(0, hop))):
                    pass_on(hop, n)

        @pl.when(core == 1)
        def _():
            meta_from_sibling(hop)
            from_sibling(hop)
            if hop == AG2_HOP:
                start_gather()

        place_hop(0, hop)
        if hop == half - 1:
            @pl.when(core == 0)
            def _():
                mix_first_hop()

    def o_copy(slot):
        return remote(x_buf.at[slot, other], o_sib.at[slot], o_send.at[slot], o_recv.at[slot], device(z, other))

    def experts(slot, batch):
        buf = slot % W_DEPTH

        @pl.when((batch == 0) | (slot < n_slot - W_DEPTH))
        def _():
            for copy in weight_copies(slot):
                copy.wait()

        x = x_buf[slot, batch].reshape(nz * cap, d_model)
        hidden = jax.nn.gelu(jnp.dot(x, up_buf[buf], preferred_element_type=F32), approximate=True).astype(BF16)
        for c in range(RS_CHUNKS):
            cols = pl.ds(c * rs_cols, rs_cols)
            o = jnp.dot(hidden, down_buf[buf, :, cols], preferred_element_type=F32).astype(BF16)
            x_buf[slot, batch, :, :, cols] = o.reshape(nz, cap, rs_cols)

        @pl.when(core != batch)
        def _():
            o_copy(slot).start()

        following = slot + W_DEPTH if batch == 0 else slot - W_DEPTH

        @pl.when((following >= 0) & (following < n_slot))
        def _():
            for copy in weight_copies(following):
                copy.start()

    @pl.loop(0, n_slot)
    def _(slot):
        experts(slot, 0)

        @pl.when((core == 1) & (slot < 2 * AG_CHUNKS))
        def _():
            hop, n = 1 + slot // AG_CHUNKS, slot % AG_CHUNKS
            for d in range(2):
                c = n if d == 0 else AG_CHUNKS - 1 - n
                ag_arrival(d, hop, c).wait_recv()
                ag_copy(d, hop + 1, c).start()
                sib_copy(d, hop, c, core).start()

    def from_sibling_o():
        @pl.loop(0, n_slot)
        def _(slot):
            o_copy(slot).wait_recv()

    def chip_rows(pos, c):
        cols = pl.ds(pl.multiple_of(c * rs_cols, rs_cols), rs_cols)
        parts = [x_buf[:, core, pos, :, cols].reshape(rows, rs_cols), o_sib[:, pos, :, cols].reshape(rows, rs_cols)]
        if k_pad > 2 * rows:
            parts.append(jnp.zeros((k_pad - 2 * rows, rs_cols), BF16))
        return jnp.concatenate(parts, axis=0)

    def mixed(weights, values):
        total = jnp.dot(weights, values, preferred_element_type=F32)
        return total[:n_tok] + total[n_tok:2 * n_tok] + total[2 * n_tok:]

    def own_sum(pos, c):
        return mixed(mix[pos], chip_rows(pos, c))

    skip = RS_CHUNKS // 2
    first = skip + RS_CHUNKS
    items = half * RS_CHUNKS

    def rs_chunk(d, n):
        c = n % RS_CHUNKS
        return (c + skip) % RS_CHUNKS if d == 0 else c

    def rs_dest(d, n):
        return ring(z + (1 - 2 * d) * (half - n // RS_CHUNKS))

    def first_copy(batch, d, j):
        side = jnp.where(core == batch, 0, 1)
        return remote(first_out.at[batch, d, j], first_in.at[side, d, j], first_send.at[batch, d, j],
                      first_recv.at[side, d, j], device(ring(z + (1 - 2 * d)), batch))

    def first_arrival(side, d, j):
        return remote(first_out.at[0, d, j], first_in.at[side, d, j], first_send.at[0, d, j],
                      first_recv.at[side, d, j], device(ring(z + (1 - 2 * d)), core))

    def rs_copy(d, n):
        return remote(rs_buf.at[d, n - first], rs_buf.at[d, n - first + RS_CHUNKS], rs_send.at[d, n],
                      rs_recv.at[d, n + RS_CHUNKS], device(ring(z + (1 - 2 * d)), core))

    def rs_arrival(d, n):
        return remote(rs_buf.at[d, n - first], rs_buf.at[d, n - first], rs_send.at[d, n], rs_recv.at[d, n],
                      device(ring(z + (1 - 2 * d)), core))

    def start_chains(batch):
        k_own = round_up(rows, 128)
        for j in range(2):
            for d in range(2):
                got = []
                for n in (skip + 2 * j, skip + 2 * j + 1):
                    cols = pl.ds(rs_chunk(d, n) * rs_cols, rs_cols)
                    parts = [x_buf[:, batch, rs_dest(d, n), :, cols].reshape(rows, rs_cols)]
                    if k_own > rows:
                        parts.append(jnp.zeros((k_own - rows, rs_cols), BF16))
                    got.append(jnp.dot(pack[:round_up(packed // 2, 16), :k_own], jnp.concatenate(parts, axis=0),
                                       preferred_element_type=F32)[:packed // 2])
                first_out[batch, d, j] = jnp.concatenate(got, axis=0).astype(BF16)
                first_copy(batch, d, j).start()

    def second_pair(j):
        for d in range(2):
            for side in range(2):
                first_arrival(side, d, j).wait_recv()
            sides = [first_in[side, d, j].astype(F32) for side in range(2)]
            for i in range(2):
                n = first + 2 * j + i
                parts = [part[i * (packed // 2):(i + 1) * (packed // 2)] for part in sides]
                if packed_pad > packed:
                    parts.append(jnp.zeros((packed_pad - packed, rs_cols), F32))
                rows_in = jnp.concatenate(parts, axis=0).astype(BF16)
                rs_buf[d, n - first] = own_sum(rs_dest(d, n), rs_chunk(d, n)) + mixed(mix_up[d, j], rows_in)
                rs_copy(d, n).start()

    def later_item(n):
        for d in range(2):
            value = own_sum(rs_dest(d, n), rs_chunk(d, n))
            rs_arrival(d, n).wait_recv()
            rs_buf[d, n - first] += value
            rs_copy(d, n).start()

    start_chains(0)

    @pl.when(core == 0)
    def _():
        from_sibling_o()

    for hop in range(half + 1):
        @pl.when(core == 0)
        def _():
            meta_from_sibling(hop)
            from_sibling(hop)

        @pl.when(core == 1)
        def _():
            for late, n in AG2_LATE[hop]:
                pass_on(late, n)

        place_hop(1, hop)
        if hop in (1, 2):
            @pl.when(core == 0)
            def _():
                second_pair(hop - 1)

    @pl.loop(0, n_slot)
    def _(i):
        experts(n_slot - 1 - i, 1)
        n = items - n_slot + i

        @pl.when((core == 0) & (n >= first + RS_CHUNKS))
        def _():
            later_item(n)

    start_chains(1)

    @pl.when(core == 1)
    def _():
        mix_first_hop()
        from_sibling_o()
        for j in range(2):
            second_pair(j)
        pl.loop(first + RS_CHUNKS, items)(later_item)

    for c in range(RS_CHUNKS):
        total_buf[c] = own_sum(z, c)
    for i in range(RS_CHUNKS):
        for d in range(2):
            rs_arrival(d, items + i).wait_recv()
        if i >= skip:
            for c in (i - skip, i):
                value = total_buf[c]
                for d in range(2):
                    value += rs_buf[d, items - first + ((c + skip) % RS_CHUNKS if d == 0 else c)]
                out_ref[:, c * rs_cols:(c + 1) * rs_cols] = value.astype(BF16)

    for d in range(2):
        for hop in range(1, half + 1):
            if meta_carried(d, hop):
                meta_copy(d, hop, 0).wait_send()
                meta_sib(d, hop, core).wait_send()
            for c in carried(d, hop):
                ag_copy(d, hop, c).wait_send()
                sib_copy(d, hop, c, core).wait_send()
    meta_sib(0, 0, core).wait_send()
    for c in range(AG_CHUNKS):
        sib_copy(0, 0, c, core).wait_send()

    @pl.loop(0, n_slot)
    def _(slot):
        o_copy(slot).wait_send()

    for batch in range(2):
        for d in range(2):
            for j in range(2):
                first_copy(batch, d, j).wait_send()

    @pl.loop(first, items)
    def _(n):
        for d in range(2):
            rs_copy(d, n).wait_send()


def solution(mesh):
    n_dev = mesh.shape["ep"]
    nz = n_dev // CORES
    half = nz // 2

    def group_layer(tokens, topk_idx, topk_w, w_up, w_down, slot_expert):
        n_tok, d_model = tokens.shape
        n_top = topk_idx.shape[1]
        n_slot = slot_expert.shape[1]
        n_exp = n_dev * (n_slot - 1)
        d_ff = w_up.shape[3]
        bound = slot_bound(n_tok, n_top, n_dev, n_slot)
        cap = round_up(bound, 16)
        k_pad = round_up(2 * n_slot * cap, 128)
        packed = 2 * round_up(n_slot * bound, 8)
        packed_pad = round_up(packed, 128)
        rs_cols = d_model // RS_CHUNKS
        skip = RS_CHUNKS // 2
        dma = pltpu.SemaphoreType.DMA
        any_space = pl.BlockSpec(memory_space=pl.ANY)
        vmem = pl.BlockSpec(memory_space=pltpu.VMEM)
        return pl.pallas_call(
            functools.partial(layer_kernel, nz, bound),
            out_shape=jax.ShapeDtypeStruct((n_tok, d_model), BF16),
            in_specs=[any_space] * 6,
            out_specs=vmem,
            scratch_shapes=[
                pltpu.VMEM((CORES, nz, n_tok, d_model), BF16),
                pltpu.VMEM((n_top, n_tok), jnp.int32),
                pltpu.SMEM(slot_expert.shape, jnp.int32),
                pltpu.VMEM(slot_expert.shape, jnp.int32),
                pltpu.VMEM((CORES, nz, 2 * n_top, n_tok), F32),
                pltpu.VMEM((n_slot, CORES, nz, cap, d_model), BF16),
                pltpu.VMEM((n_slot, nz, cap, d_model), BF16),
                pltpu.VMEM((W_DEPTH, d_model, d_ff), BF16),
                pltpu.VMEM((W_DEPTH, d_ff, d_model), BF16),
                pltpu.VMEM((2, half * RS_CHUNKS - skip, n_tok, rs_cols), F32),
                pltpu.VMEM((2, 2, 2, packed, rs_cols), BF16),
                pltpu.VMEM((2, 2, 2, packed, rs_cols), BF16),
                pltpu.VMEM((RS_CHUNKS, n_tok, rs_cols), F32),
                pltpu.VMEM((nz, 3 * n_tok, k_pad), BF16),
                pltpu.VMEM((2, 2, 3 * n_tok, packed_pad), BF16),
                pltpu.VMEM((k_pad, n_exp), BF16),
                pltpu.VMEM((k_pad, n_exp), F32),
                pltpu.VMEM((2, packed_pad, n_exp), BF16),
                pltpu.VMEM((2, packed_pad, n_exp), F32),
                pltpu.VMEM((packed_pad, k_pad), BF16),
                dma((5,)),
                dma((2, half, AG_CHUNKS)), dma((2, half, AG_CHUNKS)),
                dma((2, half + 1, AG_CHUNKS)), dma((2, half + 1, AG_CHUNKS)),
                dma((2, half)), dma((2, half)),
                dma((2, half + 1)), dma((2, half + 1)),
                dma((2, W_DEPTH)),
                dma((n_slot,)), dma((n_slot,)),
                dma((2, 2, 2)), dma((2, 2, 2)),
                dma((2, half * RS_CHUNKS)), dma((2, (half + 1) * RS_CHUNKS)),
            ],
            compiler_params=pltpu.CompilerParams(collective_id=0, has_side_effects=True,
                                                 vmem_limit_bytes=67043328),
        )(tokens, topk_idx.T, topk_w.T, slot_expert, w_up, w_down)

    row_spec = P(("dp", "ep"), None)
    weight_spec = P("ep", None, None, None)
    return jax.shard_map(group_layer, mesh=mesh,
                         in_specs=(row_spec, row_spec, row_spec, weight_spec, weight_spec, P(None, None)),
                         out_specs=row_spec, check_vma=False)
```

```python
import functools

import jax
import jax.numpy as jnp
from jax import lax
from jax.experimental import pallas as pl
from jax.experimental.pallas import tpu as pltpu
from jax.sharding import PartitionSpec as P

MESH = pl.DeviceIdType.MESH
F32 = jnp.float32
BF16 = jnp.bfloat16
CORES = 2
W_DEPTH = 4
AG_CHUNKS = 4
RS_CHUNKS = 4
AG2_LATE = (((3, 2), (3, 3)), ((4, 0), (4, 1)), (), (), ())
AG2_HOP = 3


def slot_bound(n_tok, n_top, n_dev, n_slot):
    base_load = (n_tok * n_top) // (n_dev * n_slot)
    return base_load + base_load // 2 + 1


def round_up(n, unit):
    return -(-n // unit) * unit


def split3(x):
    hi = x.astype(BF16)
    rest = x - hi.astype(F32)
    mid = rest.astype(BF16)
    low = (rest - mid.astype(F32)).astype(BF16)
    return hi, mid, low


def layer_kernel(nz, bound, tok_hbm, idx_hbm, gate_hbm, slot_hbm, up_hbm, down_hbm, out_ref,
                 toks, idx_own, slot_smem, slot_vmem, metas, x_buf, o_sib, up_buf, down_buf, rs_buf, first_out, first_in, total_buf,
                 mix, mix_up, pick, target, pick_up, target_up, pack,
                 in_sem, ag_send, ag_recv, sib_send, sib_recv, ms_send, ms_recv, mb_send, mb_recv,
                 w_sem, o_send, o_recv, first_send, first_recv, rs_send, rs_recv):
    half = nz // 2
    n_tok, d_model = tok_hbm.shape
    n_top = idx_hbm.shape[0]
    n_slot, cap = x_buf.shape[0], x_buf.shape[3]
    rows = n_slot * cap
    k_pad, n_exp = pick.shape
    packed, packed_pad = first_out.shape[3], pack.shape[0]
    ag_rows = n_tok // AG_CHUNKS
    rs_cols = d_model // RS_CHUNKS

    me = lax.axis_index("ep")
    z = me // CORES
    core = me % CORES
    other = 1 - core

    def ring(pos):
        return (pos + nz) % nz

    def device(pos, which):
        return {"ep": pos * CORES + which}

    def remote(src, dst, send, recv, dev):
        return pltpu.make_async_remote_copy(src_ref=src, dst_ref=dst, send_sem=send, recv_sem=recv,
                                            device_id=dev, device_id_type=MESH)

    def weight_copies(step):
        buf, slot = step % W_DEPTH, step % n_slot
        return (pltpu.make_async_copy(up_hbm.at[0, slot], up_buf.at[buf], w_sem.at[0, buf]),
                pltpu.make_async_copy(down_hbm.at[0, slot], down_buf.at[buf], w_sem.at[1, buf]))

    own_tok = pltpu.make_async_copy(tok_hbm, toks.at[core, z], in_sem.at[0])
    own_idx = pltpu.make_async_copy(idx_hbm, idx_own, in_sem.at[1])
    own_gate = pltpu.make_async_copy(gate_hbm, metas.at[core, z, n_top:], in_sem.at[2])
    tables = [pltpu.make_async_copy(slot_hbm, ref, in_sem.at[3 + n]) for n, ref in enumerate((slot_smem, slot_vmem))]
    own_tok.start()
    own_idx.start()
    own_gate.start()
    for copy in tables:
        copy.start()
    barrier = pltpu.get_barrier_semaphore()
    pl.semaphore_signal(barrier, inc=1, device_id=device(ring(z + 1), core), device_id_type=MESH)
    pl.semaphore_signal(barrier, inc=1, device_id=device(ring(z - 1), core), device_id_type=MESH)
    pl.semaphore_signal(barrier, inc=1, device_id=device(z, other), device_id_type=MESH)
    pl.semaphore_signal(barrier, inc=1, device_id=device(ring(z + 1), other), device_id_type=MESH)
    pl.semaphore_signal(barrier, inc=1, device_id=device(ring(z - 1), other), device_id_type=MESH)
    own_idx.wait()
    metas[core, z, :n_top, :] = idx_own[...].astype(F32)
    own_gate.wait()
    own_tok.wait()
    pl.semaphore_wait(barrier, 5)

    def ag_copy(d, hop, c):
        sign = 1 - 2 * d
        ref = toks.at[core, ring(z - sign * (hop - 1)), pl.ds(c * ag_rows, ag_rows)]
        return remote(ref, ref, ag_send.at[d, hop - 1, c], ag_recv.at[d, hop - 1, c], device(ring(z + sign), core))

    def ag_arrival(d, hop, c):
        sign = 1 - 2 * d
        ref = toks.at[core, ring(z - sign * hop), pl.ds(c * ag_rows, ag_rows)]
        return remote(ref, ref, ag_send.at[d, hop - 1, c], ag_recv.at[d, hop - 1, c], device(ring(z + sign), core))

    def sib_copy(d, hop, c, which):
        sign = 1 - 2 * d
        ref = toks.at[which, ring(z - sign * hop), pl.ds(c * ag_rows, ag_rows)]
        return remote(ref, ref, sib_send.at[d, hop, c], sib_recv.at[d, hop, c], device(z, other))

    def meta_copy(d, hop, back):
        sign = 1 - 2 * d
        ref = metas.at[core, ring(z - sign * (hop - 1 + back))]
        return remote(ref, ref, ms_send.at[d, hop - 1], ms_recv.at[d, hop - 1], device(ring(z + sign), core))

    def meta_sib(d, hop, which):
        sign = 1 - 2 * d
        ref = metas.at[which, ring(z - sign * hop)]
        return remote(ref, ref, mb_send.at[d, hop], mb_recv.at[d, hop], device(z, other))

    def chunk_order(d):
        return list(range(AG_CHUNKS)) if d == 0 else list(range(AG_CHUNKS))[::-1]

    def carried(d, hop):
        order = chunk_order(d)
        return order if hop < half else order[:AG_CHUNKS // 2]

    def meta_carried(d, hop):
        return hop < half or d == 0

    for d in range(2):
        meta_copy(d, 1, 0).start()
    meta_sib(0, 0, core).start()

    @pl.when(core == 0)
    def _():
        for c in range(AG_CHUNKS):
            for d in range(2):
                ag_copy(d, 1, chunk_order(d)[c]).start()
        for c in range(AG_CHUNKS):
            sib_copy(0, 0, c, core).start()

    for step in range(W_DEPTH):
        for copy in weight_copies(step):
            copy.start()

    lane = lax.broadcasted_iota(jnp.int32, (cap, n_exp), 1)
    row = lax.broadcasted_iota(jnp.int32, (cap, n_exp), 0).astype(F32)
    for copy in tables:
        copy.wait()
    table = slot_vmem[...]
    place = lax.broadcasted_iota(jnp.int32, table.shape, 0) * n_slot + lax.broadcasted_iota(jnp.int32, table.shape, 1)
    if k_pad > 2 * rows:
        pick[2 * rows:, :] = jnp.zeros((k_pad - 2 * rows, n_exp), BF16)
        target[2 * rows:, :] = jnp.full((k_pad - 2 * rows, n_exp), -1.0, F32)

    def slot_rows(pos):
        for w in range(2):
            dev = pos * CORES + (core if w == 0 else other)
            for s in range(n_slot):
                exp_id = slot_smem[dev, s]
                same = table == exp_id
                copies = jnp.sum(jnp.where(same, 1.0, 0.0))
                earlier = jnp.sum(jnp.where(same & (place < dev * n_slot + s), 1.0, 0.0))
                at = pl.ds(w * rows + s * cap, cap)
                pick[at, :] = jnp.where(lane == exp_id, 1.0, 0.0).astype(BF16)
                target[at, :] = row * copies + earlier

    column = lax.broadcasted_iota(jnp.int32, (packed_pad, k_pad), 1)
    side = jnp.where(column >= rows, 1, 0)
    in_side = column - side * rows
    in_slot = in_side % cap
    packed_row = side * (packed // 2) + (in_side // cap) * bound + in_slot
    used = (in_slot < bound) & (column < 2 * rows)
    pack[...] = jnp.where(used & (lax.broadcasted_iota(jnp.int32, (packed_pad, k_pad), 0) == packed_row),
                          1.0, 0.0).astype(BF16)
    for d in range(2):
        slot_rows(ring(z - (1 - 2 * d)))
        pick_up[d] = jnp.dot(pack[...], pick[...], preferred_element_type=F32).astype(BF16)
        target_up[d] = jnp.dot(pack[...], (target[...] + 1.0).astype(BF16), preferred_element_type=F32) - 1.0
    slot_rows(z)

    exp_iota = lax.broadcasted_iota(jnp.int32, (n_exp, n_tok), 0).astype(F32)

    def ranks(info):
        chosen = jnp.zeros((n_exp, n_tok), F32)
        for j in range(n_top):
            chosen = jnp.where(exp_iota == info[j:j + 1, :], 1.0, chosen)
        before = (lax.broadcasted_iota(jnp.int32, (n_tok, n_tok), 0)
                  < lax.broadcasted_iota(jnp.int32, (n_tok, n_tok), 1))
        rank = jnp.dot(chosen.astype(BF16), jnp.where(before, 1.0, 0.0).astype(BF16), preferred_element_type=F32)
        return jnp.where(chosen > 0.5, rank, -1.0).astype(BF16)

    def mixing(info, rank, picks, targets):
        gate = jnp.zeros((n_exp, n_tok), F32)
        for j in range(n_top):
            gate = jnp.where(exp_iota == info[j:j + 1, :], info[n_top + j:n_top + j + 1, :], gate)
        takes = jnp.dot(picks, rank, preferred_element_type=F32) == targets
        parts = [jnp.dot(picks, part, preferred_element_type=F32) for part in split3(gate)]
        return split3(jnp.where(takes, parts[0] + parts[1] + parts[2], 0.0).T)

    def mix_first_hop():
        @pl.loop(0, 4)
        def _(i):
            d, j = i // 2, i % 2
            info = metas[core, ring(z + (1 - 2 * d) * (half - 1 - j))]
            for n, part in enumerate(mixing(info, ranks(info), pick_up[d], target_up[d])):
                mix_up[d, j, n * n_tok:(n + 1) * n_tok, :] = part

    def place_rows(which, pos):
        info = metas[which, pos]
        rank = ranks(info)
        takes = jnp.dot(pick[:rows, :], rank, preferred_element_type=F32) == target[:rows, :]
        onehot = jnp.where(takes, 1.0, 0.0).astype(BF16)
        for c in range(RS_CHUNKS):
            cols = pl.ds(c * rs_cols, rs_cols)
            got = jnp.dot(onehot, toks[which, pos, :, cols], preferred_element_type=F32).astype(BF16)
            x_buf[:, which, pos, :, cols] = got.reshape(n_slot, cap, rs_cols)

        @pl.when(core == which)
        def _():
            for n, part in enumerate(mixing(info, rank, pick[...], target[...])):
                mix[pos, n * n_tok:(n + 1) * n_tok, :] = part

    def start_gather():
        for c in range(AG_CHUNKS):
            for d in range(2):
                ag_copy(d, 1, chunk_order(d)[c]).start()
        for c in range(AG_CHUNKS):
            sib_copy(0, 0, c, core).start()

    def pass_on(hop, n):
        for d in range(2):
            if n < len(carried(d, hop)):
                c = carried(d, hop)[n]
                ag_arrival(d, hop, c).wait_recv()
                if hop < half and c in carried(d, hop + 1):
                    ag_copy(d, hop + 1, c).start()
                sib_copy(d, hop, c, core).start()

    def from_sibling(hop):
        if hop == 0:
            for c in range(AG_CHUNKS):
                sib_copy(0, 0, c, other).wait_recv()
            return
        for d in range(2):
            for c in carried(d, hop):
                sib_copy(d, hop, c, other).wait_recv()

    def place_hop(which, hop):
        @pl.loop(0, 1 if hop in (0, half) else 2)
        def _(d):
            place_rows(which, ring(z - (1 - 2 * d) * hop))

    def meta_from_sibling(hop):
        for d in range(2):
            if (hop == 0 and d == 0) or (hop > 0 and meta_carried(d, hop)):
                meta_sib(d, hop, other).wait_recv()

    for hop in range(half + 1):
        if hop > 0:
            for d in range(2):
                if meta_carried(d, hop):
                    meta_copy(d, hop, 1).wait_recv()
                    if hop < half and meta_carried(d, hop + 1):
                        meta_copy(d, hop + 1, 0).start()
                    meta_sib(d, hop, core).start()

        @pl.when(core == 0)
        def _():
            if hop > 0:
                for n in range(len(carried(0, hop))):
                    pass_on(hop, n)

        @pl.when(core == 1)
        def _():
            meta_from_sibling(hop)
            from_sibling(hop)
            if hop == AG2_HOP:
                start_gather()

        place_hop(0, hop)
        if hop == half - 1:
            @pl.when(core == 0)
            def _():
                mix_first_hop()

    def o_copy(slot):
        return remote(x_buf.at[slot, other], o_sib.at[slot], o_send.at[slot], o_recv.at[slot], device(z, other))

    def experts(slot, batch):
        step = batch * n_slot + slot
        buf = step % W_DEPTH
        for copy in weight_copies(step):
            copy.wait()
        x = x_buf[slot, batch].reshape(nz * cap, d_model)
        hidden = jax.nn.gelu(jnp.dot(x, up_buf[buf], preferred_element_type=F32), approximate=True).astype(BF16)
        for c in range(RS_CHUNKS):
            cols = pl.ds(c * rs_cols, rs_cols)
            o = jnp.dot(hidden, down_buf[buf, :, cols], preferred_element_type=F32).astype(BF16)
            x_buf[slot, batch, :, :, cols] = o.reshape(nz, cap, rs_cols)

        @pl.when(core != batch)
        def _():
            o_copy(slot).start()

        @pl.when(step + W_DEPTH < 2 * n_slot)
        def _():
            for copy in weight_copies(step + W_DEPTH):
                copy.start()

    @pl.loop(0, n_slot)
    def _(slot):
        experts(slot, 0)

        @pl.when(core == 1)
        def _():
            hop, n = 1 + slot // AG_CHUNKS, slot % AG_CHUNKS
            for d in range(2):
                c = n if d == 0 else AG_CHUNKS - 1 - n
                ag_arrival(d, hop, c).wait_recv()
                ag_copy(d, hop + 1, c).start()
                sib_copy(d, hop, c, core).start()

    @pl.when(core == 1)
    def _():
        for n in range(n_slot - 2 * AG_CHUNKS, 2):
            pass_on(half - 1, n)

    def from_sibling_o():
        @pl.loop(0, n_slot)
        def _(slot):
            o_copy(slot).wait_recv()

    def chip_rows(pos, c):
        cols = pl.ds(pl.multiple_of(c * rs_cols, rs_cols), rs_cols)
        parts = [x_buf[:, core, pos, :, cols].reshape(rows, rs_cols), o_sib[:, pos, :, cols].reshape(rows, rs_cols)]
        if k_pad > 2 * rows:
            parts.append(jnp.zeros((k_pad - 2 * rows, rs_cols), BF16))
        return jnp.concatenate(parts, axis=0)

    def mixed(weights, values):
        total = jnp.dot(weights, values, preferred_element_type=F32)
        return total[:n_tok] + total[n_tok:2 * n_tok] + total[2 * n_tok:]

    def own_sum(pos, c):
        return mixed(mix[pos], chip_rows(pos, c))

    skip = RS_CHUNKS // 2
    first = skip + RS_CHUNKS
    items = half * RS_CHUNKS

    def rs_chunk(d, n):
        c = n % RS_CHUNKS
        return (c + skip) % RS_CHUNKS if d == 0 else c

    def rs_dest(d, n):
        return ring(z + (1 - 2 * d) * (half - n // RS_CHUNKS))

    def first_copy(batch, d, j):
        side = jnp.where(core == batch, 0, 1)
        return remote(first_out.at[batch, d, j], first_in.at[side, d, j], first_send.at[batch, d, j],
                      first_recv.at[side, d, j], device(ring(z + (1 - 2 * d)), batch))

    def first_arrival(side, d, j):
        return remote(first_out.at[0, d, j], first_in.at[side, d, j], first_send.at[0, d, j],
                      first_recv.at[side, d, j], device(ring(z + (1 - 2 * d)), core))

    def rs_copy(d, n):
        return remote(rs_buf.at[d, n - first], rs_buf.at[d, n - first + RS_CHUNKS], rs_send.at[d, n],
                      rs_recv.at[d, n + RS_CHUNKS], device(ring(z + (1 - 2 * d)), core))

    def rs_arrival(d, n):
        return remote(rs_buf.at[d, n - first], rs_buf.at[d, n - first], rs_send.at[d, n], rs_recv.at[d, n],
                      device(ring(z + (1 - 2 * d)), core))

    def start_chains(batch):
        k_own = round_up(rows, 128)
        for j in range(2):
            for d in range(2):
                got = []
                for n in (skip + 2 * j, skip + 2 * j + 1):
                    cols = pl.ds(rs_chunk(d, n) * rs_cols, rs_cols)
                    parts = [x_buf[:, batch, rs_dest(d, n), :, cols].reshape(rows, rs_cols)]
                    if k_own > rows:
                        parts.append(jnp.zeros((k_own - rows, rs_cols), BF16))
                    got.append(jnp.dot(pack[:round_up(packed // 2, 16), :k_own], jnp.concatenate(parts, axis=0),
                                       preferred_element_type=F32)[:packed // 2])
                first_out[batch, d, j] = jnp.concatenate(got, axis=0).astype(BF16)
                first_copy(batch, d, j).start()

    def second_pair(j):
        for d in range(2):
            for side in range(2):
                first_arrival(side, d, j).wait_recv()
            sides = [first_in[side, d, j].astype(F32) for side in range(2)]
            for i in range(2):
                n = first + 2 * j + i
                parts = [part[i * (packed // 2):(i + 1) * (packed // 2)] for part in sides]
                if packed_pad > packed:
                    parts.append(jnp.zeros((packed_pad - packed, rs_cols), F32))
                rows_in = jnp.concatenate(parts, axis=0).astype(BF16)
                rs_buf[d, n - first] = own_sum(rs_dest(d, n), rs_chunk(d, n)) + mixed(mix_up[d, j], rows_in)
                rs_copy(d, n).start()

    def later_item(n):
        for d in range(2):
            value = own_sum(rs_dest(d, n), rs_chunk(d, n))
            rs_arrival(d, n).wait_recv()
            rs_buf[d, n - first] += value
            rs_copy(d, n).start()

    start_chains(0)

    @pl.when(core == 0)
    def _():
        from_sibling_o()

    for hop in range(half + 1):
        @pl.when(core == 0)
        def _():
            meta_from_sibling(hop)
            from_sibling(hop)

        @pl.when(core == 1)
        def _():
            for late, n in AG2_LATE[hop]:
                pass_on(late, n)

        place_hop(1, hop)
        if hop in (1, 2):
            @pl.when(core == 0)
            def _():
                second_pair(hop - 1)

    @pl.loop(0, n_slot)
    def _(slot):
        experts(slot, 1)

        @pl.when((core == 0) & (slot < items - first - RS_CHUNKS))
        def _():
            later_item(first + RS_CHUNKS + slot)

    start_chains(1)

    @pl.when(core == 1)
    def _():
        mix_first_hop()
        from_sibling_o()
        for j in range(2):
            second_pair(j)
        pl.loop(first + RS_CHUNKS, items)(later_item)

    for c in range(RS_CHUNKS):
        total_buf[c] = own_sum(z, c)
    for i in range(RS_CHUNKS):
        for d in range(2):
            rs_arrival(d, items + i).wait_recv()
        if i >= skip:
            for c in (i - skip, i):
                value = total_buf[c]
                for d in range(2):
                    value += rs_buf[d, items - first + ((c + skip) % RS_CHUNKS if d == 0 else c)]
                out_ref[:, c * rs_cols:(c + 1) * rs_cols] = value.astype(BF16)

    for d in range(2):
        for hop in range(1, half + 1):
            if meta_carried(d, hop):
                meta_copy(d, hop, 0).wait_send()
                meta_sib(d, hop, core).wait_send()
            for c in carried(d, hop):
                ag_copy(d, hop, c).wait_send()
                sib_copy(d, hop, c, core).wait_send()
    meta_sib(0, 0, core).wait_send()
    for c in range(AG_CHUNKS):
        sib_copy(0, 0, c, core).wait_send()

    @pl.loop(0, n_slot)
    def _(slot):
        o_copy(slot).wait_send()

    for batch in range(2):
        for d in range(2):
            for j in range(2):
                first_copy(batch, d, j).wait_send()

    @pl.loop(first, items)
    def _(n):
        for d in range(2):
            rs_copy(d, n).wait_send()


def solution(mesh):
    n_dev = mesh.shape["ep"]
    nz = n_dev // CORES
    half = nz // 2

    def group_layer(tokens, topk_idx, topk_w, w_up, w_down, slot_expert):
        n_tok, d_model = tokens.shape
        n_top = topk_idx.shape[1]
        n_slot = slot_expert.shape[1]
        n_exp = n_dev * (n_slot - 1)
        d_ff = w_up.shape[3]
        bound = slot_bound(n_tok, n_top, n_dev, n_slot)
        cap = round_up(bound, 16)
        k_pad = round_up(2 * n_slot * cap, 128)
        packed = 2 * round_up(n_slot * bound, 8)
        packed_pad = round_up(packed, 128)
        rs_cols = d_model // RS_CHUNKS
        skip = RS_CHUNKS // 2
        dma = pltpu.SemaphoreType.DMA
        any_space = pl.BlockSpec(memory_space=pl.ANY)
        vmem = pl.BlockSpec(memory_space=pltpu.VMEM)
        return pl.pallas_call(
            functools.partial(layer_kernel, nz, bound),
            out_shape=jax.ShapeDtypeStruct((n_tok, d_model), BF16),
            in_specs=[any_space] * 6,
            out_specs=vmem,
            scratch_shapes=[
                pltpu.VMEM((CORES, nz, n_tok, d_model), BF16),
                pltpu.VMEM((n_top, n_tok), jnp.int32),
                pltpu.SMEM(slot_expert.shape, jnp.int32),
                pltpu.VMEM(slot_expert.shape, jnp.int32),
                pltpu.VMEM((CORES, nz, 2 * n_top, n_tok), F32),
                pltpu.VMEM((n_slot, CORES, nz, cap, d_model), BF16),
                pltpu.VMEM((n_slot, nz, cap, d_model), BF16),
                pltpu.VMEM((W_DEPTH, d_model, d_ff), BF16),
                pltpu.VMEM((W_DEPTH, d_ff, d_model), BF16),
                pltpu.VMEM((2, half * RS_CHUNKS - skip, n_tok, rs_cols), F32),
                pltpu.VMEM((2, 2, 2, packed, rs_cols), BF16),
                pltpu.VMEM((2, 2, 2, packed, rs_cols), BF16),
                pltpu.VMEM((RS_CHUNKS, n_tok, rs_cols), F32),
                pltpu.VMEM((nz, 3 * n_tok, k_pad), BF16),
                pltpu.VMEM((2, 2, 3 * n_tok, packed_pad), BF16),
                pltpu.VMEM((k_pad, n_exp), BF16),
                pltpu.VMEM((k_pad, n_exp), F32),
                pltpu.VMEM((2, packed_pad, n_exp), BF16),
                pltpu.VMEM((2, packed_pad, n_exp), F32),
                pltpu.VMEM((packed_pad, k_pad), BF16),
                dma((5,)),
                dma((2, half, AG_CHUNKS)), dma((2, half, AG_CHUNKS)),
                dma((2, half + 1, AG_CHUNKS)), dma((2, half + 1, AG_CHUNKS)),
                dma((2, half)), dma((2, half)),
                dma((2, half + 1)), dma((2, half + 1)),
                dma((2, W_DEPTH)),
                dma((n_slot,)), dma((n_slot,)),
                dma((2, 2, 2)), dma((2, 2, 2)),
                dma((2, half * RS_CHUNKS)), dma((2, (half + 1) * RS_CHUNKS)),
            ],
            compiler_params=pltpu.CompilerParams(collective_id=0, has_side_effects=True,
                                                 vmem_limit_bytes=67043328),
        )(tokens, topk_idx.T, topk_w.T, slot_expert, w_up, w_down)

    row_spec = P(("dp", "ep"), None)
    weight_spec = P("ep", None, None, None)
    return jax.shard_map(group_layer, mesh=mesh,
                         in_specs=(row_spec, row_spec, row_spec, weight_spec, weight_spec, P(None, None)),
                         out_specs=row_spec, check_vma=False)
```

```python
import functools

import jax
import jax.numpy as jnp
from jax import lax
from jax.experimental import pallas as pl
from jax.experimental.pallas import tpu as pltpu
from jax.sharding import PartitionSpec as P

MESH = pl.DeviceIdType.MESH
F32 = jnp.float32
BF16 = jnp.bfloat16
CORES = 2
W_DEPTH = 4
AG_CHUNKS = 4
RS_CHUNKS = 4
AG2_LATE = (((2, 3), (3, 0), (3, 1)), ((3, 2), (3, 3)), ((4, 0), (4, 1)), (), ())
AG2_HOP = 3


def slot_bound(n_tok, n_top, n_dev, n_slot):
    base_load = (n_tok * n_top) // (n_dev * n_slot)
    return base_load + base_load // 2 + 1


def round_up(n, unit):
    return -(-n // unit) * unit


def split3(x):
    hi = x.astype(BF16)
    rest = x - hi.astype(F32)
    mid = rest.astype(BF16)
    low = (rest - mid.astype(F32)).astype(BF16)
    return hi, mid, low


def layer_kernel(nz, bound, tok_hbm, idx_hbm, gate_hbm, slot_hbm, up_hbm, down_hbm, out_ref,
                 toks, idx_own, slot_smem, slot_vmem, metas, x_buf, o_sib, up_buf, down_buf, rs_buf, first_out, first_in, total_buf,
                 mix, mix_up, pick, target, pick_up, target_up, pack,
                 in_sem, ag_send, ag_recv, sib_send, sib_recv, ms_send, ms_recv, mb_send, mb_recv,
                 w_sem, o_send, o_recv, first_send, first_recv, rs_send, rs_recv):
    half = nz // 2
    n_tok, d_model = tok_hbm.shape
    n_top = idx_hbm.shape[0]
    n_slot, cap = x_buf.shape[0], x_buf.shape[3]
    rows = n_slot * cap
    k_pad, n_exp = pick.shape
    packed, packed_pad = first_out.shape[3], pack.shape[0]
    ag_rows = n_tok // AG_CHUNKS
    rs_cols = d_model // RS_CHUNKS

    me = lax.axis_index("ep")
    z = me // CORES
    core = me % CORES
    other = 1 - core

    def ring(pos):
        return (pos + nz) % nz

    def device(pos, which):
        return {"ep": pos * CORES + which}

    def remote(src, dst, send, recv, dev):
        return pltpu.make_async_remote_copy(src_ref=src, dst_ref=dst, send_sem=send, recv_sem=recv,
                                            device_id=dev, device_id_type=MESH)

    def weight_copies(step):
        buf, slot = step % W_DEPTH, step % n_slot
        return (pltpu.make_async_copy(up_hbm.at[0, slot], up_buf.at[buf], w_sem.at[0, buf]),
                pltpu.make_async_copy(down_hbm.at[0, slot], down_buf.at[buf], w_sem.at[1, buf]))

    own_tok = pltpu.make_async_copy(tok_hbm, toks.at[core, z], in_sem.at[0])
    own_idx = pltpu.make_async_copy(idx_hbm, idx_own, in_sem.at[1])
    own_gate = pltpu.make_async_copy(gate_hbm, metas.at[core, z, n_top:], in_sem.at[2])
    tables = [pltpu.make_async_copy(slot_hbm, ref, in_sem.at[3 + n]) for n, ref in enumerate((slot_smem, slot_vmem))]
    own_tok.start()
    own_idx.start()
    own_gate.start()
    for copy in tables:
        copy.start()
    barrier = pltpu.get_barrier_semaphore()
    pl.semaphore_signal(barrier, inc=1, device_id=device(ring(z + 1), core), device_id_type=MESH)
    pl.semaphore_signal(barrier, inc=1, device_id=device(ring(z - 1), core), device_id_type=MESH)
    pl.semaphore_signal(barrier, inc=1, device_id=device(z, other), device_id_type=MESH)
    pl.semaphore_signal(barrier, inc=1, device_id=device(ring(z + 1), other), device_id_type=MESH)
    pl.semaphore_signal(barrier, inc=1, device_id=device(ring(z - 1), other), device_id_type=MESH)
    own_idx.wait()
    metas[core, z, :n_top, :] = idx_own[...].astype(F32)
    own_gate.wait()
    own_tok.wait()
    pl.semaphore_wait(barrier, 5)

    def ag_copy(d, hop, c):
        sign = 1 - 2 * d
        ref = toks.at[core, ring(z - sign * (hop - 1)), pl.ds(c * ag_rows, ag_rows)]
        return remote(ref, ref, ag_send.at[d, hop - 1, c], ag_recv.at[d, hop - 1, c], device(ring(z + sign), core))

    def ag_arrival(d, hop, c):
        sign = 1 - 2 * d
        ref = toks.at[core, ring(z - sign * hop), pl.ds(c * ag_rows, ag_rows)]
        return remote(ref, ref, ag_send.at[d, hop - 1, c], ag_recv.at[d, hop - 1, c], device(ring(z + sign), core))

    def sib_copy(d, hop, c, which):
        sign = 1 - 2 * d
        ref = toks.at[which, ring(z - sign * hop), pl.ds(c * ag_rows, ag_rows)]
        return remote(ref, ref, sib_send.at[d, hop, c], sib_recv.at[d, hop, c], device(z, other))

    def meta_copy(d, hop, back):
        sign = 1 - 2 * d
        ref = metas.at[core, ring(z - sign * (hop - 1 + back))]
        return remote(ref, ref, ms_send.at[d, hop - 1], ms_recv.at[d, hop - 1], device(ring(z + sign), core))

    def meta_sib(d, hop, which):
        sign = 1 - 2 * d
        ref = metas.at[which, ring(z - sign * hop)]
        return remote(ref, ref, mb_send.at[d, hop], mb_recv.at[d, hop], device(z, other))

    def chunk_order(d):
        return list(range(AG_CHUNKS)) if d == 0 else list(range(AG_CHUNKS))[::-1]

    def carried(d, hop):
        order = chunk_order(d)
        return order if hop < half else order[:AG_CHUNKS // 2]

    def meta_carried(d, hop):
        return hop < half or d == 0

    for d in range(2):
        meta_copy(d, 1, 0).start()
    meta_sib(0, 0, core).start()

    @pl.when(core == 0)
    def _():
        for c in range(AG_CHUNKS):
            for d in range(2):
                ag_copy(d, 1, chunk_order(d)[c]).start()
        for c in range(AG_CHUNKS):
            sib_copy(0, 0, c, core).start()

    for step in range(W_DEPTH):
        for copy in weight_copies(step):
            copy.start()

    lane = lax.broadcasted_iota(jnp.int32, (cap, n_exp), 1)
    row = lax.broadcasted_iota(jnp.int32, (cap, n_exp), 0).astype(F32)
    for copy in tables:
        copy.wait()
    table = slot_vmem[...]
    place = lax.broadcasted_iota(jnp.int32, table.shape, 0) * n_slot + lax.broadcasted_iota(jnp.int32, table.shape, 1)
    if k_pad > 2 * rows:
        pick[2 * rows:, :] = jnp.zeros((k_pad - 2 * rows, n_exp), BF16)
        target[2 * rows:, :] = jnp.full((k_pad - 2 * rows, n_exp), -1.0, F32)

    def slot_rows(pos):
        for w in range(2):
            dev = pos * CORES + (core if w == 0 else other)
            for s in range(n_slot):
                exp_id = slot_smem[dev, s]
                same = table == exp_id
                copies = jnp.sum(jnp.where(same, 1.0, 0.0))
                earlier = jnp.sum(jnp.where(same & (place < dev * n_slot + s), 1.0, 0.0))
                at = pl.ds(w * rows + s * cap, cap)
                pick[at, :] = jnp.where(lane == exp_id, 1.0, 0.0).astype(BF16)
                target[at, :] = row * copies + earlier

    column = lax.broadcasted_iota(jnp.int32, (packed_pad, k_pad), 1)
    side = jnp.where(column >= rows, 1, 0)
    in_side = column - side * rows
    in_slot = in_side % cap
    packed_row = side * (packed // 2) + (in_side // cap) * bound + in_slot
    used = (in_slot < bound) & (column < 2 * rows)
    pack[...] = jnp.where(used & (lax.broadcasted_iota(jnp.int32, (packed_pad, k_pad), 0) == packed_row),
                          1.0, 0.0).astype(BF16)
    for d in range(2):
        slot_rows(ring(z - (1 - 2 * d)))
        pick_up[d] = jnp.dot(pack[...], pick[...], preferred_element_type=F32).astype(BF16)
        target_up[d] = jnp.dot(pack[...], (target[...] + 1.0).astype(BF16), preferred_element_type=F32) - 1.0
    slot_rows(z)

    exp_iota = lax.broadcasted_iota(jnp.int32, (n_exp, n_tok), 0).astype(F32)

    def ranks(info):
        chosen = jnp.zeros((n_exp, n_tok), F32)
        for j in range(n_top):
            chosen = jnp.where(exp_iota == info[j:j + 1, :], 1.0, chosen)
        before = (lax.broadcasted_iota(jnp.int32, (n_tok, n_tok), 0)
                  < lax.broadcasted_iota(jnp.int32, (n_tok, n_tok), 1))
        rank = jnp.dot(chosen.astype(BF16), jnp.where(before, 1.0, 0.0).astype(BF16), preferred_element_type=F32)
        return jnp.where(chosen > 0.5, rank, -1.0).astype(BF16)

    def mixing(info, rank, picks, targets):
        gate = jnp.zeros((n_exp, n_tok), F32)
        for j in range(n_top):
            gate = jnp.where(exp_iota == info[j:j + 1, :], info[n_top + j:n_top + j + 1, :], gate)
        takes = jnp.dot(picks, rank, preferred_element_type=F32) == targets
        parts = [jnp.dot(picks, part, preferred_element_type=F32) for part in split3(gate)]
        return split3(jnp.where(takes, parts[0] + parts[1] + parts[2], 0.0).T)

    def mix_first_hop():
        @pl.loop(0, 4)
        def _(i):
            d, j = i // 2, i % 2
            info = metas[core, ring(z + (1 - 2 * d) * (half - 1 - j))]
            for n, part in enumerate(mixing(info, ranks(info), pick_up[d], target_up[d])):
                mix_up[d, j, n * n_tok:(n + 1) * n_tok, :] = part

    def place_rows(which, pos):
        info = metas[which, pos]
        rank = ranks(info)
        takes = jnp.dot(pick[:rows, :], rank, preferred_element_type=F32) == target[:rows, :]
        onehot = jnp.where(takes, 1.0, 0.0).astype(BF16)
        for c in range(RS_CHUNKS):
            cols = pl.ds(c * rs_cols, rs_cols)
            got = jnp.dot(onehot, toks[which, pos, :, cols], preferred_element_type=F32).astype(BF16)
            x_buf[:, which, pos, :, cols] = got.reshape(n_slot, cap, rs_cols)

        @pl.when(core == which)
        def _():
            for n, part in enumerate(mixing(info, rank, pick[...], target[...])):
                mix[pos, n * n_tok:(n + 1) * n_tok, :] = part

    def start_gather():
        for c in range(AG_CHUNKS):
            for d in range(2):
                ag_copy(d, 1, chunk_order(d)[c]).start()
        for c in range(AG_CHUNKS):
            sib_copy(0, 0, c, core).start()

    def pass_on(hop, n):
        for d in range(2):
            if n < len(carried(d, hop)):
                c = carried(d, hop)[n]
                ag_arrival(d, hop, c).wait_recv()
                if hop < half and c in carried(d, hop + 1):
                    ag_copy(d, hop + 1, c).start()
                sib_copy(d, hop, c, core).start()

    def from_sibling(hop):
        if hop == 0:
            for c in range(AG_CHUNKS):
                sib_copy(0, 0, c, other).wait_recv()
            return
        for d in range(2):
            for c in carried(d, hop):
                sib_copy(d, hop, c, other).wait_recv()

    def place_hop(which, hop):
        @pl.loop(0, 1 if hop in (0, half) else 2)
        def _(d):
            place_rows(which, ring(z - (1 - 2 * d) * hop))

    def meta_from_sibling(hop):
        for d in range(2):
            if (hop == 0 and d == 0) or (hop > 0 and meta_carried(d, hop)):
                meta_sib(d, hop, other).wait_recv()

    for hop in range(half + 1):
        if hop > 0:
            for d in range(2):
                if meta_carried(d, hop):
                    meta_copy(d, hop, 1).wait_recv()
                    if hop < half and meta_carried(d, hop + 1):
                        meta_copy(d, hop + 1, 0).start()
                    meta_sib(d, hop, core).start()

        @pl.when(core == 0)
        def _():
            if hop > 0:
                for n in range(len(carried(0, hop))):
                    pass_on(hop, n)

        @pl.when(core == 1)
        def _():
            meta_from_sibling(hop)
            from_sibling(hop)
            if hop == AG2_HOP:
                start_gather()

        place_hop(0, hop)
        if hop == half - 1:
            @pl.when(core == 0)
            def _():
                mix_first_hop()

    def o_copy(slot):
        return remote(x_buf.at[slot, other], o_sib.at[slot], o_send.at[slot], o_recv.at[slot], device(z, other))

    def experts(slot, batch):
        step = batch * n_slot + slot
        buf = step % W_DEPTH
        for copy in weight_copies(step):
            copy.wait()
        x = x_buf[slot, batch].reshape(nz * cap, d_model)
        hidden = jax.nn.gelu(jnp.dot(x, up_buf[buf], preferred_element_type=F32), approximate=True).astype(BF16)
        for c in range(RS_CHUNKS):
            cols = pl.ds(c * rs_cols, rs_cols)
            o = jnp.dot(hidden, down_buf[buf, :, cols], preferred_element_type=F32).astype(BF16)
            x_buf[slot, batch, :, :, cols] = o.reshape(nz, cap, rs_cols)

        @pl.when(core != batch)
        def _():
            o_copy(slot).start()

        @pl.when(step + W_DEPTH < 2 * n_slot)
        def _():
            for copy in weight_copies(step + W_DEPTH):
                copy.start()

    @pl.loop(0, n_slot)
    def _(slot):
        experts(slot, 0)

        @pl.when((core == 1) & (slot >= 1) & (slot < 2 * AG_CHUNKS))
        def _():
            hop, n = 1 + (slot - 1) // AG_CHUNKS, (slot - 1) % AG_CHUNKS
            for d in range(2):
                c = n if d == 0 else AG_CHUNKS - 1 - n
                ag_arrival(d, hop, c).wait_recv()
                ag_copy(d, hop + 1, c).start()
                sib_copy(d, hop, c, core).start()

    def from_sibling_o():
        @pl.loop(0, n_slot)
        def _(slot):
            o_copy(slot).wait_recv()

    def chip_rows(pos, c):
        cols = pl.ds(pl.multiple_of(c * rs_cols, rs_cols), rs_cols)
        parts = [x_buf[:, core, pos, :, cols].reshape(rows, rs_cols), o_sib[:, pos, :, cols].reshape(rows, rs_cols)]
        if k_pad > 2 * rows:
            parts.append(jnp.zeros((k_pad - 2 * rows, rs_cols), BF16))
        return jnp.concatenate(parts, axis=0)

    def mixed(weights, values):
        total = jnp.dot(weights, values, preferred_element_type=F32)
        return total[:n_tok] + total[n_tok:2 * n_tok] + total[2 * n_tok:]

    def own_sum(pos, c):
        return mixed(mix[pos], chip_rows(pos, c))

    skip = RS_CHUNKS // 2
    first = skip + RS_CHUNKS
    items = half * RS_CHUNKS

    def rs_chunk(d, n):
        c = n % RS_CHUNKS
        return (c + skip) % RS_CHUNKS if d == 0 else c

    def rs_dest(d, n):
        return ring(z + (1 - 2 * d) * (half - n // RS_CHUNKS))

    def first_copy(batch, d, j):
        side = jnp.where(core == batch, 0, 1)
        return remote(first_out.at[batch, d, j], first_in.at[side, d, j], first_send.at[batch, d, j],
                      first_recv.at[side, d, j], device(ring(z + (1 - 2 * d)), batch))

    def first_arrival(side, d, j):
        return remote(first_out.at[0, d, j], first_in.at[side, d, j], first_send.at[0, d, j],
                      first_recv.at[side, d, j], device(ring(z + (1 - 2 * d)), core))

    def rs_copy(d, n):
        return remote(rs_buf.at[d, n - first], rs_buf.at[d, n - first + RS_CHUNKS], rs_send.at[d, n],
                      rs_recv.at[d, n + RS_CHUNKS], device(ring(z + (1 - 2 * d)), core))

    def rs_arrival(d, n):
        return remote(rs_buf.at[d, n - first], rs_buf.at[d, n - first], rs_send.at[d, n], rs_recv.at[d, n],
                      device(ring(z + (1 - 2 * d)), core))

    def start_chains(batch):
        k_own = round_up(rows, 128)
        for j in range(2):
            for d in range(2):
                got = []
                for n in (skip + 2 * j, skip + 2 * j + 1):
                    cols = pl.ds(rs_chunk(d, n) * rs_cols, rs_cols)
                    parts = [x_buf[:, batch, rs_dest(d, n), :, cols].reshape(rows, rs_cols)]
                    if k_own > rows:
                        parts.append(jnp.zeros((k_own - rows, rs_cols), BF16))
                    got.append(jnp.dot(pack[:round_up(packed // 2, 16), :k_own], jnp.concatenate(parts, axis=0),
                                       preferred_element_type=F32)[:packed // 2])
                first_out[batch, d, j] = jnp.concatenate(got, axis=0).astype(BF16)
                first_copy(batch, d, j).start()

    def second_pair(j):
        for d in range(2):
            for side in range(2):
                first_arrival(side, d, j).wait_recv()
            sides = [first_in[side, d, j].astype(F32) for side in range(2)]
            for i in range(2):
                n = first + 2 * j + i
                parts = [part[i * (packed // 2):(i + 1) * (packed // 2)] for part in sides]
                if packed_pad > packed:
                    parts.append(jnp.zeros((packed_pad - packed, rs_cols), F32))
                rows_in = jnp.concatenate(parts, axis=0).astype(BF16)
                rs_buf[d, n - first] = own_sum(rs_dest(d, n), rs_chunk(d, n)) + mixed(mix_up[d, j], rows_in)
                rs_copy(d, n).start()

    def later_item(n):
        for d in range(2):
            value = own_sum(rs_dest(d, n), rs_chunk(d, n))
            rs_arrival(d, n).wait_recv()
            rs_buf[d, n - first] += value
            rs_copy(d, n).start()

    start_chains(0)

    @pl.when(core == 0)
    def _():
        from_sibling_o()

    for hop in range(half + 1):
        @pl.when(core == 0)
        def _():
            meta_from_sibling(hop)
            from_sibling(hop)

        @pl.when(core == 1)
        def _():
            for late, n in AG2_LATE[hop]:
                pass_on(late, n)

        place_hop(1, hop)
        if hop in (1, 2):
            @pl.when(core == 0)
            def _():
                second_pair(hop - 1)

    @pl.loop(0, n_slot)
    def _(slot):
        experts(slot, 1)

        @pl.when((core == 0) & (slot < items - first - RS_CHUNKS))
        def _():
            later_item(first + RS_CHUNKS + slot)

    start_chains(1)

    @pl.when(core == 1)
    def _():
        mix_first_hop()
        from_sibling_o()
        for j in range(2):
            second_pair(j)
        pl.loop(first + RS_CHUNKS, items)(later_item)

    for c in range(RS_CHUNKS):
        total_buf[c] = own_sum(z, c)
    for i in range(RS_CHUNKS):
        for d in range(2):
            rs_arrival(d, items + i).wait_recv()
        if i >= skip:
            for c in (i - skip, i):
                value = total_buf[c]
                for d in range(2):
                    value += rs_buf[d, items - first + ((c + skip) % RS_CHUNKS if d == 0 else c)]
                out_ref[:, c * rs_cols:(c + 1) * rs_cols] = value.astype(BF16)

    for d in range(2):
        for hop in range(1, half + 1):
            if meta_carried(d, hop):
                meta_copy(d, hop, 0).wait_send()
                meta_sib(d, hop, core).wait_send()
            for c in carried(d, hop):
                ag_copy(d, hop, c).wait_send()
                sib_copy(d, hop, c, core).wait_send()
    meta_sib(0, 0, core).wait_send()
    for c in range(AG_CHUNKS):
        sib_copy(0, 0, c, core).wait_send()

    @pl.loop(0, n_slot)
    def _(slot):
        o_copy(slot).wait_send()

    for batch in range(2):
        for d in range(2):
            for j in range(2):
                first_copy(batch, d, j).wait_send()

    @pl.loop(first, items)
    def _(n):
        for d in range(2):
            rs_copy(d, n).wait_send()


def solution(mesh):
    n_dev = mesh.shape["ep"]
    nz = n_dev // CORES
    half = nz // 2

    def group_layer(tokens, topk_idx, topk_w, w_up, w_down, slot_expert):
        n_tok, d_model = tokens.shape
        n_top = topk_idx.shape[1]
        n_slot = slot_expert.shape[1]
        n_exp = n_dev * (n_slot - 1)
        d_ff = w_up.shape[3]
        bound = slot_bound(n_tok, n_top, n_dev, n_slot)
        cap = round_up(bound, 16)
        k_pad = round_up(2 * n_slot * cap, 128)
        packed = 2 * round_up(n_slot * bound, 8)
        packed_pad = round_up(packed, 128)
        rs_cols = d_model // RS_CHUNKS
        skip = RS_CHUNKS // 2
        dma = pltpu.SemaphoreType.DMA
        any_space = pl.BlockSpec(memory_space=pl.ANY)
        vmem = pl.BlockSpec(memory_space=pltpu.VMEM)
        return pl.pallas_call(
            functools.partial(layer_kernel, nz, bound),
            out_shape=jax.ShapeDtypeStruct((n_tok, d_model), BF16),
            in_specs=[any_space] * 6,
            out_specs=vmem,
            scratch_shapes=[
                pltpu.VMEM((CORES, nz, n_tok, d_model), BF16),
                pltpu.VMEM((n_top, n_tok), jnp.int32),
                pltpu.SMEM(slot_expert.shape, jnp.int32),
                pltpu.VMEM(slot_expert.shape, jnp.int32),
                pltpu.VMEM((CORES, nz, 2 * n_top, n_tok), F32),
                pltpu.VMEM((n_slot, CORES, nz, cap, d_model), BF16),
                pltpu.VMEM((n_slot, nz, cap, d_model), BF16),
                pltpu.VMEM((W_DEPTH, d_model, d_ff), BF16),
                pltpu.VMEM((W_DEPTH, d_ff, d_model), BF16),
                pltpu.VMEM((2, half * RS_CHUNKS - skip, n_tok, rs_cols), F32),
                pltpu.VMEM((2, 2, 2, packed, rs_cols), BF16),
                pltpu.VMEM((2, 2, 2, packed, rs_cols), BF16),
                pltpu.VMEM((RS_CHUNKS, n_tok, rs_cols), F32),
                pltpu.VMEM((nz, 3 * n_tok, k_pad), BF16),
                pltpu.VMEM((2, 2, 3 * n_tok, packed_pad), BF16),
                pltpu.VMEM((k_pad, n_exp), BF16),
                pltpu.VMEM((k_pad, n_exp), F32),
                pltpu.VMEM((2, packed_pad, n_exp), BF16),
                pltpu.VMEM((2, packed_pad, n_exp), F32),
                pltpu.VMEM((packed_pad, k_pad), BF16),
                dma((5,)),
                dma((2, half, AG_CHUNKS)), dma((2, half, AG_CHUNKS)),
                dma((2, half + 1, AG_CHUNKS)), dma((2, half + 1, AG_CHUNKS)),
                dma((2, half)), dma((2, half)),
                dma((2, half + 1)), dma((2, half + 1)),
                dma((2, W_DEPTH)),
                dma((n_slot,)), dma((n_slot,)),
                dma((2, 2, 2)), dma((2, 2, 2)),
                dma((2, half * RS_CHUNKS)), dma((2, (half + 1) * RS_CHUNKS)),
            ],
            compiler_params=pltpu.CompilerParams(collective_id=0, has_side_effects=True,
                                                 vmem_limit_bytes=67043328),
        )(tokens, topk_idx.T, topk_w.T, slot_expert, w_up, w_down)

    row_spec = P(("dp", "ep"), None)
    weight_spec = P("ep", None, None, None)
    return jax.shard_map(group_layer, mesh=mesh,
                         in_specs=(row_spec, row_spec, row_spec, weight_spec, weight_spec, P(None, None)),
                         out_specs=row_spec, check_vma=False)
```
